32 devices in a mesh: dp: 8 (over z, y), mp: 4 (over x, core).
Axes of the slice: x: 2, y: 2, z: 4, core: 2. Of those that a mesh axis runs over, the one named last changes fastest.
Arguments:
- tokens: bfloat16 [32768, 768], P(('dp', 'mp')), may hold values from -6 to 6
- cotangent: bfloat16 [32768, 768], P(('dp', 'mp')), may hold values from -6 to 6
- prompts: float32 [50, 768], replicated, may hold values from -6 to 6
- segments: int32 [32768], P(('dp', 'mp')), may hold values from 0 to 6, as said below
- prompt_slot_index: int32 [32768], P(('dp', 'mp')), may hold values from 0 to 50, as said below
- norm_gain: float32 [2, 768], replicated, may hold values from 0.5 to 1.5
- norm_shift: float32 [2, 768], replicated, may hold values from -2 to 2
- attn_qkv: bfloat16 [3, 768, 768], P(None, ('dp', 'mp')), may hold values from -0.21875 to 0.21875
- attn_bias: float32 [3, 768], replicated, may hold values from -2 to 2
- attn_out: bfloat16 [768, 768], P(('dp', 'mp')), may hold values from -0.625 to 0.625
- mlp_weight: bfloat16 [2, 768, 3072], P(None, 'dp', 'mp'), may hold values from -0.21875 to 0.21875
- mlp_bias_up: float32 [3072], replicated, may hold values from -2 to 2
- mlp_bias_down: float32 [768], replicated, may hold values from -2 to 2
Outputs:
- block_output: bfloat16 [32768, 768], P(('dp', 'mp'))
- input_grad: float32 [32768, 768], P(('dp', 'mp'))
- prompt_grad: float32 [50, 768], replicated
- gain_grad: float32 [2, 768], replicated
- shift_grad: float32 [2, 768], replicated
- qkv_grad: float32 [3, 768, 768], P(None, ('dp', 'mp'))
- attn_bias_grad: float32 [3, 768], replicated
- attn_out_grad: float32 [768, 768], P(('dp', 'mp'))
- mlp_grad: float32 [2, 768, 3072], P(None, 'dp', 'mp')
- up_bias_grad: float32 [3072], replicated
- down_bias_grad: float32 [768], replicated
The draws below stay inside these ranges and needn't reach their ends.
Inputs may be any that keep to these rules, and one draw needn't show every extreme that they name: Every packed row holds images of one size: from the row's start, as many whole segments of 151, of 247 or of 627 tokens as fit, numbered from 0, then one segment of the remaining tokens. Row 0 holds the smallest images. `prompt_slot_index`: in each image segment, tokens 1 to 50 carry slots 0 to 49; all other tokens carry 50.
All inputs are finite; a program needn't handle non-finite values.
Results may differ from the reference program's by a relative error of at most 0.014.
Values may be sent and summed in bfloat16 or wider, within the bound.
No kernel may reach another device: no remote copies, remote signals or barrier semaphores. Data moves between devices by JAX's collectives and lax.ppermute only.
A program may use at most 256 MiB of HBM per device.

```python
import jax
import jax.numpy as jnp
from jax import lax

MODEL_WIDTH = 768
HEADS = 12
HEAD_SIZE = 64
FF = 3072
NPROMPT = 50
PATCH_S = 100
PATCH_M = 196
PATCH_L = 576
PACKED_ROW_LENGTH = 1024
TOKEN_TOTAL = 32768


def row_layout(key):
    row_count_total = TOKEN_TOTAL // PACKED_ROW_LENGTH
    groups = jax.random.randint(jax.random.fold_in(key, 11), (row_count_total,), 0, 3)
    groups = groups.at[0].set(0)
    spans = NPROMPT + 1 + jnp.array([PATCH_S, PATCH_M, PATCH_L], jnp.int32)
    row_extent = spans[groups]
    picture_list = PACKED_ROW_LENGTH // row_extent
    token_positions = jnp.arange(PACKED_ROW_LENGTH, dtype=jnp.int32)
    segment_ids = token_positions[None, :] // row_extent[:, None]
    within = token_positions[None, :] - segment_ids * row_extent[:, None]
    is_prompt = (segment_ids < picture_list[:, None]) & (within >= 1) & (within <= NPROMPT)
    slot_ids = jnp.where(is_prompt, within - 1, NPROMPT)
    return (segment_ids.reshape(-1).astype(jnp.int32), slot_ids.reshape(-1).astype(jnp.int32))


def draw_segments(key, part):
    return row_layout(key)[0]


def draw_prompt_slot_index(key, part):
    return row_layout(key)[1]


def block_levels(key, shape, cuts, least, high):
    level, own = 1.0, jax.random.fold_in(key, 6)
    for dim, shards_of in cuts:
        draws = jnp.exp(jax.random.uniform(jax.random.fold_in(own, dim), (shards_of,), jnp.float32, least / len(cuts), high / len(cuts)))
        level = level * jnp.repeat(draws, shape[dim] // shards_of).reshape([-1 if axis == dim else 1 for axis in range(len(shape))])
    return level


def bell_draw(key, shape, width, most, cuts=(), kind=jnp.bfloat16):
    level = block_levels(key, shape, cuts, -0.22, 0.18) if cuts else 1.0
    entries = jax.random.normal(key, shape, jnp.float32) * width * level
    return jnp.minimum(jnp.maximum(entries, -most), most).astype(kind)


def setup_inputs(seed: int = 0) -> dict:
    key_of = jax.random.split(jax.random.key(seed), 14)
    return {
        "tokens": bell_draw(key_of[0], (TOKEN_TOTAL, MODEL_WIDTH), 1.0, 6.0, ((0, 32),)),
        "cotangent": bell_draw(key_of[1], (TOKEN_TOTAL, MODEL_WIDTH), 1.0, 6.0, ((0, 32),)),
        "prompts": bell_draw(key_of[2], (NPROMPT, MODEL_WIDTH), 1.0, 6.0, (), jnp.float32),
        "segments": draw_segments(jax.random.fold_in(key_of[13], 71), 0),
        "prompt_slot_index": draw_prompt_slot_index(jax.random.fold_in(key_of[13], 71), 0),
        "norm_gain": jnp.clip(1.0 + 0.1 * jax.random.normal(key_of[5], (2, MODEL_WIDTH), jnp.float32), 0.5, 1.5),
        "norm_shift": bell_draw(key_of[6], (2, MODEL_WIDTH), 0.3, 2.0, (), jnp.float32),
        "attn_qkv": bell_draw(key_of[7], (3, MODEL_WIDTH, MODEL_WIDTH), MODEL_WIDTH ** -0.5, 0.21875, ((1, 32),)),
        "attn_bias": bell_draw(key_of[8], (3, MODEL_WIDTH), 0.3, 2.0, (), jnp.float32),
        "attn_out": bell_draw(key_of[9], (MODEL_WIDTH, MODEL_WIDTH), (MODEL_WIDTH // 8) ** -0.5, 0.625, ((0, 32),)),
        "mlp_weight": bell_draw(key_of[10], (2, MODEL_WIDTH, FF), MODEL_WIDTH ** -0.5, 0.21875, ((1, 8), (2, 4))),
        "mlp_bias_up": bell_draw(key_of[11], (FF,), 0.3, 2.0, (), jnp.float32),
        "mlp_bias_down": bell_draw(key_of[12], (MODEL_WIDTH,), 0.3, 2.0, (), jnp.float32),
    }


EPS = 1e-06
HIGHEST = lax.Precision.HIGHEST
MASKED = -1e+30

@jax.custom_vjp
def low(v):
    return lax.optimization_barrier(v.astype(jnp.bfloat16)).astype(jnp.float32)

@jax.custom_vjp
def low_back(v):
    return v

def low_keep(v):
    return (low(v), None)

def low_pass(kept, grad):
    return (grad,)

def back_keep(v):
    return (v, None)

def back_low(kept, grad):
    return (low(grad),)
low.defvjp(low_keep, low_pass)
low_back.defvjp(back_keep, back_low)

def rounded(value_list):
    return low_back(low(value_list))

def matmul(left, right):
    return jnp.dot(left, right, precision=HIGHEST)

def layer_norm(value_list, gain_row, shift_row):
    centre = lax.optimization_barrier(jnp.mean(value_list, axis=-1, keepdims=True))
    centred = value_list - centre
    spread = lax.optimization_barrier(jnp.mean(centred * centred, axis=-1, keepdims=True))
    return centred * lax.rsqrt(spread + EPS) * gain_row + shift_row

def attend_row(queries, key_rows, value_rows, seg_row):
    length = queries.shape[0]
    query_heads = queries.reshape(length, HEADS, HEAD_SIZE)
    key_heads = key_rows.reshape(length, HEADS, HEAD_SIZE)
    value_heads = value_rows.reshape(length, HEADS, HEAD_SIZE)
    scores = jnp.einsum('qhd,khd->hqk', query_heads, key_heads, precision=HIGHEST) * HEAD_SIZE ** (-0.5)
    scores = low_back(scores)
    allowed = seg_row[:, None] == seg_row[None, :]
    scores = jnp.where(allowed[None], scores, MASKED)
    row_peak = lax.optimization_barrier(jnp.max(scores, axis=-1, keepdims=True))
    raised = jnp.exp(scores - row_peak)
    weights = low(raised / lax.optimization_barrier(jnp.sum(raised, axis=-1, keepdims=True)))
    mixed = jnp.einsum('hqk,khd->qhd', weights, value_heads, precision=HIGHEST)
    return mixed.reshape(length, MODEL_WIDTH)

def reference(tokens, cotangent, prompts, segments, prompt_slot_index, norm_gain, norm_shift, attn_qkv, attn_bias, attn_out, mlp_weight, mlp_bias_up, mlp_bias_down):
    row_count_total = TOKEN_TOTAL // PACKED_ROW_LENGTH
    segment_row_list = segments.reshape(row_count_total, PACKED_ROW_LENGTH)
    slot_row_list = prompt_slot_index.reshape(row_count_total, PACKED_ROW_LENGTH)

    def forward(input_list, prompt_table, gains, shifts, qkv, biases, out_weight, mlp, bias_up, bias_down):
        table = jnp.concatenate([prompt_table, jnp.zeros((1, MODEL_WIDTH), jnp.float32)], 0)

        def single_row(packed):
            row_inputs, seg_row, slot_row = packed
            onehot = (slot_row[:, None] == jnp.arange(NPROMPT + 1, dtype=jnp.int32)[None, :]).astype(jnp.float32)
            start = jnp.where((slot_row < NPROMPT)[:, None], matmul(onehot, table), row_inputs)
            normed_one = low(layer_norm(start, gains[0], shifts[0]))
            queries = rounded(matmul(normed_one, qkv[0]) + biases[0])
            key_rows = rounded(matmul(normed_one, qkv[1]))
            value_rows = rounded(matmul(normed_one, qkv[2]) + biases[1])
            mixed = rounded(attend_row(queries, key_rows, value_rows, seg_row))
            middle = start + low_back(matmul(mixed, out_weight) + biases[2])
            normed_two = low(layer_norm(middle, gains[1], shifts[1]))
            before = low_back(matmul(normed_two, mlp[0]) + bias_up)
            hidden = low(jax.nn.gelu(before, approximate=False))
            return middle + low_back(matmul(hidden, mlp[1].T) + bias_down)
        return lax.map(jax.checkpoint(single_row), (input_list.reshape(row_count_total, PACKED_ROW_LENGTH, MODEL_WIDTH), segment_row_list, slot_row_list))
    result, backward_pull = jax.vjp(forward, tokens.astype(jnp.float32), prompts, norm_gain, norm_shift, attn_qkv.astype(jnp.float32), attn_bias, attn_out.astype(jnp.float32), mlp_weight.astype(jnp.float32), mlp_bias_up, mlp_bias_down)
    gradient_list = backward_pull(cotangent.astype(jnp.float32).reshape(row_count_total, PACKED_ROW_LENGTH, MODEL_WIDTH))
    return (result.reshape(TOKEN_TOTAL, MODEL_WIDTH).astype(jnp.bfloat16), gradient_list[0].reshape(TOKEN_TOTAL, MODEL_WIDTH), gradient_list[1], gradient_list[2], gradient_list[3], gradient_list[4], gradient_list[5], gradient_list[6], gradient_list[7], gradient_list[8], gradient_list[9])
```

```python
from functools import partial

import jax
import jax.numpy as jnp
from jax import lax
from jax.experimental import pallas as pl
from jax.experimental.pallas import tpu as pltpu
from jax.sharding import PartitionSpec as P

NPROMPT = 50
ROW = 1024
SPANS = (151, 247, 627)
EPS = 1e-06
HIGHEST = lax.Precision.HIGHEST
BIG = 1e30
B16 = jnp.bfloat16
F32 = jnp.float32
AXES = ("dp", "mp")
TILE = 256
NT = (((1,), (1,)), ((), ()))
TN = (((0,), (0,)), ((), ()))
VMEM_LIMIT = 60 * 1024 * 1024


def layer_norm(value_list, gain_row, shift_row):
    centre = jnp.mean(value_list, axis=-1, keepdims=True)
    centred = value_list - centre
    spread = jnp.mean(centred * centred, axis=-1, keepdims=True)
    return centred * lax.rsqrt(spread + EPS) * gain_row + shift_row


def key_window(first, count):
    low, high = ROW, 0
    for span in SPANS:
        whole = ROW // span
        for row in (first, first + count - 1):
            seg = min(row // span, whole)
            low = min(low, seg * span)
            high = max(high, ROW if seg == whole else (seg + 1) * span)
    return low // 128 * 128, -(-high // 128) * 128


def dotf(a, b, dims=None):
    if dims is None:
        return jnp.dot(a, b, preferred_element_type=F32)
    return lax.dot_general(a, b, dims, preferred_element_type=F32)


def px(x, k):
    return lax.ppermute(x, AXES, [(i, i ^ k) for i in range(32)])


def gather_pieces(piece):
    zs = jnp.stack([piece] + [px(piece, 8 * k) for k in range(1, 4)])
    qs = [zs] + [px(zs, 2 * k) for k in range(1, 4)]
    return qs + [px(q, 1) for q in qs]


def reduce_pieces(own, other):
    got = px(other, 1)
    parts = [own[k].astype(F32) + got[k].astype(F32) for k in range(4)]
    moved = [px(parts[k].astype(B16), 2 * k).astype(F32) for k in range(1, 4)]
    col = (parts[0] + moved[0]) + (moved[1] + moved[2])
    last = [px(col[z].astype(B16), 8 * z).astype(F32) for z in range(1, 4)]
    return (col[0] + last[0]) + (last[1] + last[2])


def all_reduce(x):
    x = x + px(x, 1)
    x = (x + px(x, 2)) + (px(x, 4) + px(x, 6))
    return (x + px(x, 8)) + (px(x, 16) + px(x, 24))


def pair_halves(weight, core):
    half = weight.shape[2] // 2
    mine = lax.dynamic_slice_in_dim(weight, core * half, half, 2)
    theirs = lax.dynamic_slice_in_dim(weight, (1 - core) * half, half, 2)
    got = px(theirs, 1)
    return jnp.where(
        core == 0, jnp.concatenate([mine, got], 1), jnp.concatenate([got, mine], 1)
    )


def assemble_kernel(meta, *refs):
    pieces, out, sems = refs[:8], refs[8], refs[9]
    chip, core = meta[0] // 2, meta[0] % 2
    copies = []
    for b in range(2):
        for xy in range(4):
            for z in range(4):
                rows = pl.multiple_of(48 * jnp.bitwise_xor(chip, xy + 4 * z), 16)
                cols = pl.multiple_of(384 * jnp.bitwise_xor(core, b), 128)
                copies.append(
                    pltpu.make_async_copy(
                        pieces[4 * b + xy].at[z],
                        out.at[:, pl.ds(rows, 48), pl.ds(cols, 384)],
                        sems.at[16 * b + 4 * xy + z],
                    )
                )
    for copy in copies:
        copy.start()
    for copy in copies:
        copy.wait()


def assemble(meta, pieces, name):
    count = pieces[0].shape[1]
    return pl.pallas_call(
        assemble_kernel,
        name=name,
        out_shape=jax.ShapeDtypeStruct((count, 768, 768), B16),
        in_specs=[pl.BlockSpec(memory_space=pltpu.SMEM)]
        + [pl.BlockSpec(memory_space=pl.ANY)] * 8,
        out_specs=pl.BlockSpec(memory_space=pltpu.VMEM),
        scratch_shapes=[pltpu.SemaphoreType.DMA((32,))],
    )(meta, *pieces)


def reorder_kernel(meta, g_ref, own_ref, other_ref):
    core = meta[0] % 2
    own_ref[0, 0] = g_ref[:, 0, pl.ds(pl.multiple_of(24 * core, 8), 24), :].astype(B16)
    other_ref[0, 0] = g_ref[:, 0, pl.ds(pl.multiple_of(24 * (1 - core), 8), 24), :].astype(B16)


def reorder(meta, grads, name):
    count = grads.shape[0]
    shape = jax.ShapeDtypeStruct((4, 4, count, 24, 768), B16)
    out_spec = pl.BlockSpec((1, 1, count, 24, 768), lambda i, j, meta: (i, j, 0, 0, 0))
    return pl.pallas_call(
        reorder_kernel,
        name=name,
        out_shape=(shape, shape),
        grid_spec=pltpu.PrefetchScalarGridSpec(
            num_scalar_prefetch=1,
            grid=(4, 4),
            in_specs=[
                pl.BlockSpec(
                    (count, 1, 48, 768),
                    lambda i, j, meta: (0, jnp.bitwise_xor(meta[0] // 2, i + 4 * j), 0, 0),
                )
            ],
            out_specs=[out_spec, out_spec],
        ),
    )(meta, grads.reshape(count, 16, 48, 768))


def three_parts(x):
    high = x.astype(B16).astype(F32)
    mid = (x - high).astype(B16).astype(F32)
    return high, mid, (x - high) - mid


def attention_forward_kernel(qf_ref, kf_ref, q_ref, k_ref, v_ref, mixed_ref, lse_ref):
    half = lax.broadcasted_iota(jnp.int32, (1, 128), 1) < 64
    q = q_ref[...] * jnp.asarray(0.125, B16)
    k, v = k_ref[...], v_ref[...]
    qf, kf = qf_ref[...], kf_ref[...]
    one = jnp.ones((), B16)
    sides = []
    for e in range(2):
        own = half if e == 0 else ~half
        sides.append((jnp.where(own, q, qf), jnp.where(own, k, kf), jnp.where(own, v, one)))
    for first in range(0, ROW, TILE):
        low, high = key_window(first, TILE)
        outs, peaks = [], []
        for qe, ke, ve in sides:
            s = dotf(qe[first : first + TILE], ke[low:high], NT)
            peak = jnp.max(s, axis=-1, keepdims=True)
            p = jnp.exp(s - peak).astype(B16)
            outs.append(dotf(p, ve[low:high]))
            peaks.append(peak)
        data = jnp.where(half, outs[0], outs[1])
        total = pltpu.roll(jnp.where(half, outs[1], outs[0]), 64, 1)
        mixed_ref[first : first + TILE, :] = (data / total).astype(B16)
        lse_ref[first : first + TILE, :] = jnp.where(half, peaks[0], peaks[1]) + jnp.log(total)


def attention_forward(qf, kf, qkv, pairs):
    rows = qkv.shape[0]
    full = pl.BlockSpec((ROW, 128), lambda r, p: (r, 0))

    def block(c):
        return pl.BlockSpec((ROW, 128), lambda r, p: (r, c * pairs + p))

    out = pl.BlockSpec((ROW, 128), lambda r, p: (r, p))
    return pl.pallas_call(
        attention_forward_kernel,
        name="attention_forward",
        grid=(rows // ROW, pairs),
        in_specs=[full, full, block(0), block(1), block(2)],
        out_specs=[out, out],
        out_shape=(
            jax.ShapeDtypeStruct((rows, 128 * pairs), B16),
            jax.ShapeDtypeStruct((rows, 128 * pairs), F32),
        ),
        compiler_params=pltpu.CompilerParams(vmem_limit_bytes=VMEM_LIMIT),
    )(qf, kf, qkv, qkv, qkv)


def attention_backward_kernel(
    qf_ref, kf_ref, q_ref, k_ref, v_ref, g_ref, mixed_ref, lse_ref, dq_ref, dk_ref, dv_ref, dk_acc, dv_acc
):
    lane = lax.broadcasted_iota(jnp.int32, (1, 128), 1)
    half = lane < 64
    spot = lane % 64
    q = q_ref[...] * jnp.asarray(0.125, B16)
    k, v, g = k_ref[...], v_ref[...], g_ref[...]
    qf, kf = qf_ref[...].astype(F32), kf_ref[...]
    prod = g.astype(F32) * mixed_ref[...].astype(F32)
    d0 = jnp.sum(jnp.where(half, prod, 0.0), axis=-1, keepdims=True)
    d1 = jnp.sum(jnp.where(half, 0.0, prod), axis=-1, keepdims=True)
    delta = jnp.where(half, d1, d0)
    lse = pltpu.roll(lse_ref[...], 64, 1)

    def spread(base, x):
        a, b, c = three_parts(-x)
        return jnp.where(spot == 7, a, jnp.where(spot == 8, b, jnp.where(spot == 9, c, base))).astype(B16)

    q_extra = spread(qf, lse)
    g_extra = spread(jnp.zeros_like(qf), delta)
    v_extra = jnp.where((spot >= 7) & (spot <= 9), 1.0, 0.0).astype(B16)
    dk_acc[...] = jnp.zeros_like(dk_acc)
    dv_acc[...] = jnp.zeros_like(dv_acc)
    sides = []
    for e in range(2):
        own = half if e == 0 else ~half
        sides.append(
            (
                jnp.where(own, q, q_extra),
                jnp.where(own, k, kf),
                jnp.where(own, g, g_extra),
                jnp.where(own, v, v_extra),
            )
        )
    for first in range(0, ROW, TILE):
        low, high = key_window(first, TILE)
        dqs, dks, dvs = [], [], []
        for qe, ke, ge, ve in sides:
            s = dotf(qe[first : first + TILE], ke[low:high], NT)
            p = jnp.exp(s)
            d = dotf(ge[first : first + TILE], ve[low:high], NT)
            ds = (p * d).astype(B16)
            dqs.append(dotf(ds, k[low:high]))
            dks.append(dotf(ds, q[first : first + TILE], TN))
            dvs.append(dotf(p.astype(B16), g[first : first + TILE], TN))
        dq_ref[first : first + TILE, :] = (jnp.where(half, dqs[0], dqs[1]) * 0.125).astype(B16)
        dk_acc[low:high, :] += jnp.where(half, dks[0], dks[1])
        dv_acc[low:high, :] += jnp.where(half, dvs[0], dvs[1])
    dk_ref[...] = dk_acc[...].astype(B16)
    dv_ref[...] = dv_acc[...].astype(B16)


def attention_backward(qf, kf, qkv, grad, mixed, lse, pairs):
    rows = qkv.shape[0]
    full = pl.BlockSpec((ROW, 128), lambda r, p: (r, 0))

    def block(c):
        return pl.BlockSpec((ROW, 128), lambda r, p: (r, c * pairs + p))

    out = pl.BlockSpec((ROW, 128), lambda r, p: (r, p))
    shape = jax.ShapeDtypeStruct((rows, 128 * pairs), B16)
    return pl.pallas_call(
        attention_backward_kernel,
        name="attention_backward",
        grid=(rows // ROW, pairs),
        in_specs=[full, full, block(0), block(1), block(2), out, out, out],
        out_specs=[out, out, out],
        out_shape=(shape, shape, shape),
        scratch_shapes=[pltpu.VMEM((ROW, 128), F32), pltpu.VMEM((ROW, 128), F32)],
        compiler_params=pltpu.CompilerParams(vmem_limit_bytes=VMEM_LIMIT),
    )(qf, kf, qkv, qkv, qkv, grad, mixed, lse)


SUB = 256
PER = 768 // SUB


def mlp_kernel(fast, *refs):
    meta, n_ref, c_ref, b_ref = refs[:4]
    count = 8 if fast else 1
    pieces, refs = refs[4 : 4 + count], refs[4 + count :]
    branch_ref, gn_ref, db_ref, own_ref, other_ref = refs[:5]
    w, nt, ct, dw, wsem, dsem = refs[5:]
    t = pl.program_id(0)
    jr, sub = t // PER, t % PER
    me_mp, me_dp = meta[0] % 4, meta[0] // 4

    def loads(j):
        if not fast:
            return [pltpu.make_async_copy(pieces[0].at[:, :, pl.ds(768 * j, 768)], w.at[j], wsem.at[j, 0])]
        out = []
        for dr in range(8):
            rows = pl.multiple_of(96 * jnp.bitwise_xor(me_dp, dr), 32)
            source = pieces[4 * (j & 1) + (j >> 1) + 2 * (dr & 1)].at[dr >> 1]
            out.append(pltpu.make_async_copy(source, w.at[j, :, pl.ds(rows, 96), :], wsem.at[j, dr]))
        return out

    def stores(j):
        if not fast:
            return [pltpu.make_async_copy(dw.at[j], own_ref.at[j], dsem.at[j, 0])]
        out = []
        for dr in range(8):
            target = (other_ref if j & 1 else own_ref).at[(j >> 1) + 2 * (dr & 1), dr >> 1]
            out.append(pltpu.make_async_copy(dw.at[j, dr], target, dsem.at[j, dr]))
        return out

    @pl.when(t == 0)
    def _():
        for j in range(4):
            for copy in loads(j):
                copy.start()
        nt[...] = n_ref[...].T
        ct[...] = c_ref[...].T
        branch_ref[...] = jnp.zeros_like(branch_ref)
        gn_ref[...] = jnp.zeros_like(gn_ref)

    for j in range(4):

        @pl.when(t == PER * j)
        def _():
            for copy in loads(j):
                copy.wait()

    spot = jnp.bitwise_xor(me_mp, jr) if fast else jr
    cols = pl.ds(pl.multiple_of(sub * SUB, SUB), SUB)
    w1 = w[jr, 0, :, cols]
    w2 = w[jr, 1, :, cols]
    u = dotf(n_ref[...], w1) + b_ref[spot, :, cols]
    cdf = 0.5 * (1.0 + lax.erf(u * 0.7071067811865476))
    hidden = (u * cdf).astype(B16)
    slope = cdf + u * (0.3989422804014327 * jnp.exp(-0.5 * u * u))
    gb32 = dotf(c_ref[...], w2) * slope
    gb = gb32.astype(B16)
    db_ref[spot, :, cols] = jnp.sum(gb.astype(F32), axis=0, keepdims=True)
    branch_ref[...] += dotf(hidden, w2, NT)
    gn_ref[...] += dotf(gb, w1, NT)
    dw1 = dotf(nt[...], gb).astype(B16)
    dw2 = dotf(ct[...], hidden).astype(B16)
    for a in range(8):
        dr = jnp.bitwise_xor(me_dp, a) if fast else a
        dw[jr, dr, 0, :, cols] = dw1[96 * a : 96 * a + 96]
        dw[jr, dr, 1, :, cols] = dw2[96 * a : 96 * a + 96]

    for j in range(4):

        @pl.when(t == PER * j + PER - 1)
        def _():
            for copy in stores(j):
                copy.start()

    @pl.when(t == 4 * PER - 1)
    def _():
        for j in range(4):
            for copy in stores(j):
                copy.wait()


def mlp(meta, normed, cot, bias, pieces):
    fast = len(pieces) == 8
    tokens = normed.shape[0]
    vmem = pl.BlockSpec(memory_space=pltpu.VMEM)
    anys = pl.BlockSpec(memory_space=pl.ANY)
    if fast:
        shape = jax.ShapeDtypeStruct((4, 4, 2, 96, 768), B16)
    else:
        shape = jax.ShapeDtypeStruct((4, 8, 2, 96, 768), B16)
    return pl.pallas_call(
        partial(mlp_kernel, fast),
        name="mlp",
        grid=(4 * PER,),
        in_specs=[pl.BlockSpec(memory_space=pltpu.SMEM), vmem, vmem, vmem] + [anys] * len(pieces),
        out_specs=[vmem, vmem, vmem, anys, anys],
        out_shape=(
            jax.ShapeDtypeStruct((tokens, 768), F32),
            jax.ShapeDtypeStruct((tokens, 768), F32),
            jax.ShapeDtypeStruct((4, 1, 768), F32),
            shape,
            shape,
        ),
        scratch_shapes=[
            pltpu.VMEM((4, 2, 768, 768), B16),
            pltpu.VMEM((768, tokens), B16),
            pltpu.VMEM((768, tokens), B16),
            pltpu.VMEM((4, 8, 2, 96, 768), B16),
            pltpu.SemaphoreType.DMA((4, 8)),
            pltpu.SemaphoreType.DMA((4, 8)),
        ],
        compiler_params=pltpu.CompilerParams(vmem_limit_bytes=VMEM_LIMIT),
    )(meta, normed, cot, bias.reshape(4, 1, 768), *pieces)


def local(
    fast,
    tokens,
    cotangent,
    prompts,
    segments,
    prompt_slot_index,
    norm_gain,
    norm_shift,
    attn_qkv,
    attn_bias,
    attn_out,
    mlp_weight,
    mlp_bias_up,
    mlp_bias_down,
):
    width = tokens.shape[1]
    pairs = width // 128
    device = lax.axis_index("dp") * lax.axis_size("mp") + lax.axis_index("mp")
    meta = jnp.reshape(device, (1,)).astype(jnp.int32)
    if fast:
        core = device % 2
        qkv_pieces = gather_pieces(pair_halves(attn_qkv, core))
        qkv_all = assemble(meta, qkv_pieces, "assemble_qkv")
        attn_out_tied, mlp_tied, _ = lax.optimization_barrier((attn_out, mlp_weight, qkv_pieces[3]))
        out_pieces = gather_pieces(pair_halves(attn_out_tied[None], core))
        out_all = assemble(meta, out_pieces, "assemble_out")[0]
        mlp_tied, _ = lax.optimization_barrier((mlp_tied, out_pieces[3]))
        mlp_pieces = gather_pieces(mlp_tied)
    else:
        qkv_all = lax.all_gather(attn_qkv, AXES, axis=1, tiled=True)
        out_all = lax.all_gather(attn_out, AXES, axis=0, tiled=True)
        mlp_all = lax.all_gather(mlp_weight, "dp", axis=1, tiled=True)
        mlp_pieces = [lax.all_gather(mlp_all, "mp", axis=2, tiled=True)]

    table = jnp.concatenate([prompts, jnp.zeros((1, width), F32)], 0)
    onehot = (prompt_slot_index[:, None] == jnp.arange(NPROMPT + 1, dtype=jnp.int32)[None, :]).astype(F32)
    is_prompt = (prompt_slot_index < NPROMPT)[:, None]
    start = jnp.where(is_prompt, jnp.dot(onehot, table, precision=HIGHEST), tokens.astype(F32))
    normed_one = layer_norm(start, norm_gain[0], norm_shift[0]).astype(B16)
    lane = jnp.arange(128, dtype=jnp.int32)[None, :] % 64
    same = (segments[:, None] == lane) & (lane < 7)
    qf = same.astype(B16)
    kf = jnp.where(lane < 7, jnp.where(same, 0.0, -BIG), jnp.where(lane < 10, 1.0, 0.0)).astype(B16)

    bias_row = jnp.concatenate([attn_bias[0], jnp.zeros_like(attn_bias[0]), attn_bias[1]])
    qkv = jnp.concatenate([dotf(normed_one, qkv_all[c]) for c in range(3)], 1) + bias_row
    qkv = qkv.astype(B16)
    mixed, lse = attention_forward(qf, kf, qkv, pairs)
    middle = start + dotf(mixed, out_all) + attn_bias[2]
    normed_two = layer_norm(middle, norm_gain[1], norm_shift[1]).astype(B16)
    grad_output = cotangent.astype(F32)
    grad_down = jnp.sum(grad_output, axis=0)
    branch, grad_normed_two, grad_up, own_mlp, other_mlp = mlp(
        meta, normed_two, cotangent, mlp_bias_up, mlp_pieces
    )
    output = middle + branch + mlp_bias_down
    norm_out_two, pull_two = jax.vjp(layer_norm, middle, norm_gain[1], norm_shift[1])
    grad_from_two, grad_gain_two, grad_shift_two = pull_two(grad_normed_two)
    grad_middle = grad_output + grad_from_two
    grad_branch = grad_middle.astype(B16)
    grad_bias_out = jnp.sum(grad_branch.astype(F32), axis=0)
    grad_out_weight = dotf(mixed, grad_branch, TN)
    grad_mixed = dotf(grad_branch, out_all, NT).astype(B16)
    dq, dk, dv = attention_backward(qf, kf, qkv, grad_mixed, mixed, lse, pairs)
    grad_qkv = jnp.stack([dotf(normed_one, x, TN) for x in (dq, dk, dv)])
    grad_attn_bias = jnp.stack([jnp.sum(dq.astype(F32), axis=0), jnp.sum(dv.astype(F32), axis=0), grad_bias_out])
    grad_normed_one = sum(dotf(x, qkv_all[c], NT) for c, x in enumerate((dq, dk, dv)))
    norm_out_one, pull_one = jax.vjp(layer_norm, start, norm_gain[0], norm_shift[0])
    grad_from_one, grad_gain_one, grad_shift_one = pull_one(grad_normed_one)
    grad_start = grad_middle + grad_from_one
    input_grad = jnp.where(is_prompt, 0.0, grad_start)
    grad_prompts = jnp.dot(onehot.T, grad_start, precision=HIGHEST)[:NPROMPT]
    small = jnp.concatenate(
        [
            grad_prompts,
            grad_gain_one[None],
            grad_gain_two[None],
            grad_shift_one[None],
            grad_shift_two[None],
            grad_attn_bias,
            grad_down[None],
            grad_up.reshape(4, width),
        ]
    )
    if fast:
        mlp_grad = reduce_pieces(own_mlp, other_mlp)
        out_grad = reduce_pieces(*reorder(meta, grad_out_weight[None], "reorder_out"))[0]
        qkv_grad = reduce_pieces(*reorder(meta, grad_qkv, "reorder_qkv"))
        small = all_reduce(small)
    else:
        mlp_grad = own_mlp.transpose(2, 1, 3, 0, 4).reshape(2, 768, 3072)
        mlp_grad = lax.psum_scatter(mlp_grad, "dp", scatter_dimension=1, tiled=True)
        mlp_grad = lax.psum_scatter(mlp_grad, "mp", scatter_dimension=2, tiled=True).astype(F32)
        qkv_grad = lax.psum_scatter(grad_qkv, AXES, scatter_dimension=1, tiled=True)
        out_grad = lax.psum_scatter(grad_out_weight, AXES, scatter_dimension=0, tiled=True)
        small = lax.psum(small, AXES)
    at = NPROMPT
    return (
        output.astype(B16),
        input_grad,
        small[:at],
        small[at : at + 2],
        small[at + 2 : at + 4],
        qkv_grad,
        small[at + 4 : at + 7],
        out_grad,
        mlp_grad,
        small[at + 8 :].reshape(-1),
        small[at + 7],
    )


def solution(mesh):
    fast = dict(mesh.shape) == {"dp": 8, "mp": 4}
    return jax.shard_map(
        partial(local, fast),
        mesh=mesh,
        in_specs=(
            P(AXES, None),
            P(AXES, None),
            P(),
            P(AXES),
            P(AXES),
            P(),
            P(),
            P(None, AXES, None),
            P(),
            P(AXES, None),
            P(None, "dp", "mp"),
            P(),
            P(),
        ),
        out_specs=(
            P(AXES, None),
            P(AXES, None),
            P(),
            P(),
            P(),
            P(None, AXES, None),
            P(),
            P(AXES, None),
            P(None, "dp", "mp"),
            P(),
            P(),
        ),
        check_vma=False,
    )
```

```python
from functools import partial

import jax
import jax.numpy as jnp
from jax import lax
from jax.experimental import pallas as pl
from jax.experimental.pallas import tpu as pltpu
from jax.sharding import PartitionSpec as P

NPROMPT = 50
ROW = 1024
SPANS = (151, 247, 627)
EPS = 1e-06
HIGHEST = lax.Precision.HIGHEST
BIG = 1e30
B16 = jnp.bfloat16
F32 = jnp.float32
AXES = ("dp", "mp")
TILE = 256
NT = (((1,), (1,)), ((), ()))
TN = (((0,), (0,)), ((), ()))
VMEM_LIMIT = 60 * 1024 * 1024


def layer_norm(value_list, gain_row, shift_row):
    centre = jnp.mean(value_list, axis=-1, keepdims=True)
    centred = value_list - centre
    spread = jnp.mean(centred * centred, axis=-1, keepdims=True)
    return centred * lax.rsqrt(spread + EPS) * gain_row + shift_row


def key_window(first, count):
    low, high = ROW, 0
    for span in SPANS:
        whole = ROW // span
        for row in (first, first + count - 1):
            seg = min(row // span, whole)
            low = min(low, seg * span)
            high = max(high, ROW if seg == whole else (seg + 1) * span)
    return low // 128 * 128, -(-high // 128) * 128


def dotf(a, b, dims=None):
    if dims is None:
        return jnp.dot(a, b, preferred_element_type=F32)
    return lax.dot_general(a, b, dims, preferred_element_type=F32)


def px(x, k):
    return lax.ppermute(x, AXES, [(i, i ^ k) for i in range(32)])


def tie(*trees):
    return lax.optimization_barrier(trees)


def stack_kernel(*refs):
    for i, ref in enumerate(refs[:-1]):
        refs[-1][i] = ref[...]


def stack(parts, name):
    vmem = pl.BlockSpec(memory_space=pltpu.VMEM)
    return pl.pallas_call(
        stack_kernel,
        name=name,
        out_shape=jax.ShapeDtypeStruct((len(parts),) + parts[0].shape, parts[0].dtype),
        in_specs=[vmem] * len(parts),
        out_specs=vmem,
    )(*parts)


def z_stage(piece):
    return stack([piece] + [px(piece, 8 * k) for k in range(1, 4)], "stack_z")


def xy_stage(parts):
    return [parts] + [px(parts, 2 * k) for k in range(1, 4)]


def split_kernel(meta, qkv_ref, out_ref, mine_ref, theirs_ref):
    core = meta[0] % 2
    for ref, half in ((mine_ref, core), (theirs_ref, 1 - core)):
        cols = pl.ds(pl.multiple_of(384 * half, 128), 384)
        ref[0:3] = qkv_ref[:, :, cols]
        ref[3] = out_ref[:, cols]


def join_kernel(meta, mine_ref, got_ref, out_ref):
    for core in range(2):

        @pl.when(meta[0] % 2 == core)
        def _():
            out_ref[...] = jnp.concatenate([mine_ref[...], got_ref[...]][:: 1 - 2 * core], 1)


def pair_rows(meta, qkv, out):
    vmem = pl.BlockSpec(memory_space=pltpu.VMEM)
    smem = pl.BlockSpec(memory_space=pltpu.SMEM)
    half = jax.ShapeDtypeStruct((4, 24, 384), B16)
    mine, theirs = pl.pallas_call(
        split_kernel, name="split", out_shape=(half, half), in_specs=[smem, vmem, vmem], out_specs=(vmem, vmem)
    )(meta, qkv, out)
    return pl.pallas_call(
        join_kernel,
        name="join",
        out_shape=jax.ShapeDtypeStruct((4, 48, 384), B16),
        in_specs=[smem, vmem, vmem],
        out_specs=vmem,
    )(meta, mine, px(theirs, 1))


def assemble_kernel(meta, *refs):
    pieces, out, sems = refs[:4], refs[4], refs[5]
    copies = []
    for xy in range(4):
        for z in range(4):
            rows = pl.multiple_of(48 * jnp.bitwise_xor(meta[0] // 2, xy + 4 * z), 16)
            copies.append(
                pltpu.make_async_copy(pieces[xy].at[z], out.at[:, pl.ds(rows, 48), :], sems.at[4 * xy + z])
            )
    for copy in copies:
        copy.start()
    for copy in copies:
        copy.wait()


def assemble(meta, pieces, name):
    return pl.pallas_call(
        assemble_kernel,
        name=name,
        out_shape=jax.ShapeDtypeStruct((4, 768, 384), B16),
        in_specs=[pl.BlockSpec(memory_space=pltpu.SMEM)] + [pl.BlockSpec(memory_space=pl.ANY)] * 4,
        out_specs=pl.BlockSpec(memory_space=pltpu.VMEM),
        scratch_shapes=[pltpu.SemaphoreType.DMA((16,))],
    )(meta, *pieces)


def project_kernel(side, meta, x_ref, w_ref, b_ref, *refs):
    half = jnp.bitwise_xor(meta[0] % 2, side)
    cols = pl.ds(pl.multiple_of(384 * half, 128), 384)
    for c in range(3):
        y = dotf(x_ref[...], w_ref[c]) + b_ref[c, :, cols]
        refs[-1][:, 384 * c : 384 * c + 384] = y.astype(B16)


def project(meta, x, weight, bias, side, held):
    rows = x.shape[0]
    vmem = pl.BlockSpec(memory_space=pltpu.VMEM)
    return pl.pallas_call(
        partial(project_kernel, side),
        name="project",
        grid=(rows // TILE,),
        out_shape=jax.ShapeDtypeStruct((rows, 2304), B16),
        in_specs=[
            pl.BlockSpec(memory_space=pltpu.SMEM),
            pl.BlockSpec((TILE, 768), lambda i: (i, 0)),
            pl.BlockSpec((3, 768, 384), lambda i: (0, 0, 0), pipeline_mode=pl.Buffered(1)),
            vmem,
        ]
        + [pl.BlockSpec(memory_space=pl.ANY)] * len(held),
        out_specs=pl.BlockSpec((TILE, 1152), lambda i: (i, side)),
        input_output_aliases={4 + i: i for i in range(len(held))},
        compiler_params=pltpu.CompilerParams(vmem_limit_bytes=VMEM_LIMIT),
    )(meta, x, weight, bias, *held)


def embed_kernel(tokens_ref, slots_ref, segs_ref, table_ref, p_ref, start_ref, normed_ref, hot_ref, qf_ref, kf_ref):
    lane = lax.broadcasted_iota(jnp.int32, (TILE, 128), 1)
    slots, segs = slots_ref[...], segs_ref[...]
    is_prompt = slots < NPROMPT
    hot = jnp.where((lane == slots) & is_prompt, 1.0, 0.0).astype(B16)
    hot_ref[...] = hot
    rows = None
    for part in three_parts(table_ref[...]):
        term = dotf(hot, part.astype(B16))
        rows = term if rows is None else rows + term
    start = jnp.where(is_prompt, rows, tokens_ref[...].astype(F32))
    start_ref[...] = start
    normed_ref[...] = (centred(start)[0] * p_ref[0:1] + p_ref[1:2]).astype(B16)
    spot = lane % 64
    same = (spot == segs) & (spot < 7)
    qf_ref[...] = jnp.where(same, 1.0, 0.0).astype(B16)
    kf = jnp.where(spot < 7, jnp.where(same, 0.0, -BIG), jnp.where(spot < 10, 1.0, 0.0))
    kf_ref[...] = kf.astype(B16)


def embed(tokens, slots, segs, table, params):
    rows = tokens.shape[0]

    def block(width):
        return pl.BlockSpec((TILE, width), lambda i: (i, 0))

    vmem = pl.BlockSpec(memory_space=pltpu.VMEM)
    lanes = jax.ShapeDtypeStruct((rows, 128), B16)
    return pl.pallas_call(
        embed_kernel,
        name="embed",
        grid=(rows // TILE,),
        in_specs=[block(768), block(1), block(1), vmem, vmem],
        out_specs=[block(768), block(768), block(128), block(128), block(128)],
        out_shape=(
            jax.ShapeDtypeStruct((rows, 768), F32),
            jax.ShapeDtypeStruct((rows, 768), B16),
            lanes,
            lanes,
            lanes,
        ),
    )(tokens, slots[:, None], segs[:, None], table, params)


def gather_sums_kernel(own_ref, got_ref, own_out_ref, got_out_ref, keep_ref, *sends):
    for k in range(4):
        for z in range(4):
            for m in range(4):
                if m < 3:
                    x = add_parts(own_ref[k, z, m], got_ref[k, z, m])
                else:
                    x = add_parts(own_out_ref[k, z, 0], got_out_ref[k, z, 0])
                if k:
                    sends[k - 1][z, m] = x.astype(B16)
                else:
                    keep_ref[z, m] = x


def gather_sums(own, got, own_out, got_out):
    vmem = pl.BlockSpec(memory_space=pltpu.VMEM)
    send = jax.ShapeDtypeStruct((4, 4, 24, 768), B16)
    return pl.pallas_call(
        gather_sums_kernel,
        name="gather_sums",
        in_specs=[vmem] * 4,
        out_specs=[vmem] * 4,
        out_shape=(jax.ShapeDtypeStruct((4, 4, 24, 768), F32), send, send, send),
        compiler_params=pltpu.CompilerParams(vmem_limit_bytes=VMEM_LIMIT),
    )(own, got, own_out, got_out)


def four(values):
    return (values[0] + values[1]) + (values[2] + values[3])


def plane_sums_kernel(keep_ref, *refs):
    moved, (col_ref, *sends) = refs[:3], refs[3:]
    for z in range(4):
        for m in range(4):
            x = four([keep_ref[z, m]] + [ref[z, m].astype(F32) for ref in moved])
            if z:
                sends[z - 1][m] = x.astype(B16)
            else:
                col_ref[m] = x


def plane_sums(keep, moved):
    vmem = pl.BlockSpec(memory_space=pltpu.VMEM)
    send = jax.ShapeDtypeStruct((4, 24, 768), B16)
    return pl.pallas_call(
        plane_sums_kernel,
        name="plane_sums",
        in_specs=[vmem] * 4,
        out_specs=[vmem] * 4,
        out_shape=(jax.ShapeDtypeStruct((4, 24, 768), F32), send, send, send),
        compiler_params=pltpu.CompilerParams(vmem_limit_bytes=VMEM_LIMIT),
    )(keep, *moved)


def line_sums_kernel(col_ref, *refs):
    last, (qkv_ref, out_ref) = refs[:3], refs[3:]
    for m in range(4):
        x = four([col_ref[m]] + [ref[m].astype(F32) for ref in last])
        if m < 3:
            qkv_ref[m] = x
        else:
            out_ref[...] = x


def line_sums(col, last):
    vmem = pl.BlockSpec(memory_space=pltpu.VMEM)
    return pl.pallas_call(
        line_sums_kernel,
        name="line_sums",
        in_specs=[vmem] * 4,
        out_specs=[vmem] * 2,
        out_shape=(jax.ShapeDtypeStruct((3, 24, 768), F32), jax.ShapeDtypeStruct((24, 768), F32)),
    )(col, *last)


def centred(x):
    mean = jnp.mean(x, axis=-1, keepdims=True)
    x = x - mean
    rate = lax.rsqrt(jnp.mean(x * x, axis=-1, keepdims=True) + EPS)
    return x * rate, rate


def out_kernel(meta, x_ref, start_ref, own_ref, other_ref, p_ref, middle_ref, normed_ref, w_ref):
    core = meta[0] % 2

    @pl.when(pl.program_id(0) == 0)
    def _():
        for ref, half in ((own_ref, core), (other_ref, 1 - core)):
            w_ref[:, pl.ds(pl.multiple_of(384 * half, 128), 384)] = ref[3]

    middle = start_ref[...] + dotf(x_ref[...], w_ref[...]) + p_ref[0:1]
    middle_ref[...] = middle
    normed_ref[...] = (centred(middle)[0] * p_ref[1:2] + p_ref[2:3]).astype(B16)


def out_projection(meta, mixed, start, own, other, params):
    rows = mixed.shape[0]
    block = pl.BlockSpec((TILE, 768), lambda i: (i, 0))
    vmem = pl.BlockSpec(memory_space=pltpu.VMEM)
    return pl.pallas_call(
        out_kernel,
        name="out_projection",
        grid=(rows // TILE,),
        in_specs=[pl.BlockSpec(memory_space=pltpu.SMEM), block, block, vmem, vmem, vmem],
        out_specs=[block, block, vmem],
        out_shape=(
            jax.ShapeDtypeStruct((rows, 768), F32),
            jax.ShapeDtypeStruct((rows, 768), B16),
            jax.ShapeDtypeStruct((768, 768), B16),
        ),
        compiler_params=pltpu.CompilerParams(vmem_limit_bytes=VMEM_LIMIT),
    )(meta, mixed, start, own, other, params)


def norm_backward(normal, rate, grad, gain):
    u = grad * gain
    return rate * (u - jnp.mean(u, axis=-1, keepdims=True) - normal * jnp.mean(u * normal, axis=-1, keepdims=True))


def row_sum(x):
    return jnp.sum(x, axis=0, keepdims=True)


def put_parts(meta, acc, own_ref, other_ref, m):
    chip, core = meta[0] // 2, meta[0] % 2
    for z in range(4):
        for xy in range(4):
            row = 48 * jnp.bitwise_xor(chip, xy + 4 * z)
            own_ref[xy, z, m] = acc[pl.ds(pl.multiple_of(row + 24 * core, 8), 24), :].astype(B16)
            other_ref[xy, z, m] = acc[pl.ds(pl.multiple_of(row + 24 * (1 - core), 8), 24), :].astype(B16)


def turn_kernel(
    meta, middle_ref, branch_ref, grad_ref, cot_ref, mixed_ref, w_ref, p_ref,
    output_ref, gmiddle_ref, gmixed_ref, own_ref, other_ref, sums_ref, acc,
):
    i = pl.program_id(0)

    @pl.when(i == 0)
    def _():
        sums_ref[...] = jnp.zeros_like(sums_ref)
        acc[...] = jnp.zeros_like(acc)

    middle, grad = middle_ref[...], grad_ref[...]
    cot = cot_ref[...].astype(F32)
    output_ref[...] = (middle + branch_ref[...] + p_ref[1:2]).astype(B16)
    normal, rate = centred(middle)
    gmiddle = cot + norm_backward(normal, rate, grad, p_ref[0:1])
    gmiddle_ref[...] = gmiddle
    low = gmiddle.astype(B16)
    for row, x in enumerate((normal * grad, grad, low.astype(F32), cot)):
        sums_ref[row : row + 1, :] += row_sum(x)
    gmixed_ref[...] = dotf(low, w_ref[...], NT).astype(B16)
    acc[...] += dotf(mixed_ref[...], low, TN)

    @pl.when(i == pl.num_programs(0) - 1)
    def _():
        put_parts(meta, acc, own_ref, other_ref, 0)


def turn(meta, middle, branch, grad, cot, mixed, weight, params):
    rows = middle.shape[0]
    block = pl.BlockSpec((TILE, 768), lambda i: (i, 0))
    vmem = pl.BlockSpec(memory_space=pltpu.VMEM)
    parts = jax.ShapeDtypeStruct((4, 4, 1, 24, 768), B16)
    return pl.pallas_call(
        turn_kernel,
        name="turn",
        grid=(rows // TILE,),
        in_specs=[pl.BlockSpec(memory_space=pltpu.SMEM)] + [block] * 5 + [vmem, vmem],
        out_specs=[block, block, block, vmem, vmem, vmem],
        out_shape=(
            jax.ShapeDtypeStruct((rows, 768), B16),
            jax.ShapeDtypeStruct((rows, 768), F32),
            jax.ShapeDtypeStruct((rows, 768), B16),
            parts,
            parts,
            jax.ShapeDtypeStruct((8, 768), F32),
        ),
        scratch_shapes=[pltpu.VMEM((768, 768), F32)],
        compiler_params=pltpu.CompilerParams(vmem_limit_bytes=VMEM_LIMIT),
    )(meta, middle, branch, grad, cot, mixed, weight, params)


def tail_kernel(meta, start_ref, gmiddle_ref, slots_ref, p_ref, *refs):
    weights, grads = refs[:2], refs[2:5]
    input_ref, prompt_ref, sums_ref = refs[5:]
    core = meta[0] % 2

    @pl.when(pl.program_id(0) == 0)
    def _():
        prompt_ref[...] = jnp.zeros_like(prompt_ref)
        sums_ref[...] = jnp.zeros_like(sums_ref)

    total = None
    for c in range(3):
        for side in range(2):
            half = jnp.bitwise_xor(core, side)
            left = grads[c][:, pl.ds(pl.multiple_of(384 * half, 128), 384)]
            term = dotf(left, weights[side][c], NT)
            total = term if total is None else total + term
    normal, rate = centred(start_ref[...])
    for row, x in enumerate((normal * total, total, grads[0][...].astype(F32), grads[2][...].astype(F32))):
        sums_ref[row : row + 1, :] += row_sum(x)
    gstart = gmiddle_ref[...] + norm_backward(normal, rate, total, p_ref[0:1])
    slots = slots_ref[...]
    is_prompt = jnp.sum(slots.astype(F32), axis=-1, keepdims=True) > 0.5
    input_ref[...] = jnp.where(is_prompt, 0.0, gstart)
    for part in three_parts(gstart):
        prompt_ref[...] += dotf(slots, part.astype(B16), TN)


def tail_step(meta, start, gmiddle, slots, params, weights, grads):
    rows = start.shape[0]

    def block(width):
        return pl.BlockSpec((TILE, width), lambda i: (i, 0))

    vmem = pl.BlockSpec(memory_space=pltpu.VMEM)
    return pl.pallas_call(
        tail_kernel,
        name="tail_step",
        grid=(rows // TILE,),
        in_specs=[pl.BlockSpec(memory_space=pltpu.SMEM), block(768), block(768), block(128), vmem, vmem, vmem]
        + [block(768)] * 3,
        out_specs=[block(768), vmem, vmem],
        out_shape=(
            jax.ShapeDtypeStruct((rows, 768), F32),
            jax.ShapeDtypeStruct((128, 768), F32),
            jax.ShapeDtypeStruct((8, 768), F32),
        ),
        compiler_params=pltpu.CompilerParams(vmem_limit_bytes=VMEM_LIMIT),
    )(meta, start, gmiddle, slots, params, *weights, *grads)


def weight_grad_kernel(count, meta, left_ref, *refs):
    rights, own_ref, other_ref, acc = refs[:count], refs[count], refs[count + 1], refs[count + 2]
    for m in range(count):
        acc[...] = dotf(left_ref[...], rights[m][...], TN)
        put_parts(meta, acc, own_ref, other_ref, m)


def weight_grad(meta, left, rights, name):
    count, width = len(rights), rights[0].shape[1]
    shape = jax.ShapeDtypeStruct((4, 4, count, 24, width), B16)
    vmem = pl.BlockSpec(memory_space=pltpu.VMEM)
    return pl.pallas_call(
        partial(weight_grad_kernel, count),
        name=name,
        out_shape=(shape, shape),
        in_specs=[pl.BlockSpec(memory_space=pltpu.SMEM)] + [vmem] * (count + 1),
        out_specs=(vmem, vmem),
        scratch_shapes=[pltpu.VMEM((left.shape[1], width), F32)],
        compiler_params=pltpu.CompilerParams(vmem_limit_bytes=VMEM_LIMIT),
    )(meta, left, *rights)


def pack_small(small):
    low = small[:NPROMPT].astype(B16)
    rest = small[NPROMPT:]
    high = rest.astype(B16)
    return jnp.concatenate([low, high, (rest - high.astype(F32)).astype(B16), jnp.zeros((6, small.shape[1]), B16)])


def open_small(packed):
    wide = packed.astype(F32)
    at = NPROMPT + 12
    return jnp.concatenate([wide[:NPROMPT], wide[NPROMPT:at] + wide[at : at + 12]])


def add_parts(own, got):
    return own.astype(F32) + got.astype(F32)


def three_parts(x):
    high = x.astype(B16).astype(F32)
    mid = (x - high).astype(B16).astype(F32)
    return high, mid, (x - high) - mid


def attention_forward_kernel(qf_ref, kf_ref, q_ref, k_ref, v_ref, mixed_ref, lse_ref):
    half = lax.broadcasted_iota(jnp.int32, (1, 128), 1) < 64
    q = q_ref[...] * jnp.asarray(0.125, B16)
    k, v = k_ref[...], v_ref[...]
    qf, kf = qf_ref[...], kf_ref[...]
    one = jnp.ones((), B16)
    sides = []
    for e in range(2):
        own = half if e == 0 else ~half
        sides.append((jnp.where(own, q, qf), jnp.where(own, k, kf), jnp.where(own, v, one)))
    for first in range(0, ROW, TILE):
        low, high = key_window(first, TILE)
        outs, peaks = [], []
        for qe, ke, ve in sides:
            s = dotf(qe[first : first + TILE], ke[low:high], NT)
            peak = jnp.max(s, axis=-1, keepdims=True)
            p = jnp.exp(s - peak).astype(B16)
            outs.append(dotf(p, ve[low:high]))
            peaks.append(peak)
        data = jnp.where(half, outs[0], outs[1])
        total = pltpu.roll(jnp.where(half, outs[1], outs[0]), 64, 1)
        mixed_ref[first : first + TILE, :] = (data / total).astype(B16)
        lse_ref[first : first + TILE, :] = jnp.where(half, peaks[0], peaks[1]) + jnp.log(total)


def pair_specs(rows):
    full = pl.BlockSpec((ROW, 128), lambda r, s, p, meta: (r, 0))
    blocks = [pl.BlockSpec((ROW, 128), lambda r, s, p, meta, c=c: (r, 9 * s + 3 * c + p)) for c in range(3)]
    whole = pl.BlockSpec((ROW, 128), lambda r, s, p, meta: (r, 3 * jnp.bitwise_xor(meta[0] % 2, s) + p))
    return (rows // ROW, 2, 3), full, blocks, whole


def attention_forward(meta, qf, kf, qkv):
    rows = qkv.shape[0]
    grid, full, blocks, whole = pair_specs(rows)

    def kernel(meta, *refs):
        attention_forward_kernel(*refs)

    return pl.pallas_call(
        kernel,
        name="attention_forward",
        grid_spec=pltpu.PrefetchScalarGridSpec(
            num_scalar_prefetch=1, grid=grid, in_specs=[full, full] + blocks, out_specs=[whole, whole]
        ),
        out_shape=(
            jax.ShapeDtypeStruct((rows, 768), B16),
            jax.ShapeDtypeStruct((rows, 768), F32),
        ),
        compiler_params=pltpu.CompilerParams(vmem_limit_bytes=VMEM_LIMIT),
    )(meta, qf, kf, qkv, qkv, qkv)


def attention_backward_kernel(
    qf_ref, kf_ref, q_ref, k_ref, v_ref, g_ref, mixed_ref, lse_ref, dq_ref, dk_ref, dv_ref, dk_acc, dv_acc
):
    lane = lax.broadcasted_iota(jnp.int32, (1, 128), 1)
    half = lane < 64
    spot = lane % 64
    q = q_ref[...] * jnp.asarray(0.125, B16)
    k, v, g = k_ref[...], v_ref[...], g_ref[...]
    qf, kf = qf_ref[...].astype(F32), kf_ref[...]
    prod = g.astype(F32) * mixed_ref[...].astype(F32)
    d0 = jnp.sum(jnp.where(half, prod, 0.0), axis=-1, keepdims=True)
    d1 = jnp.sum(jnp.where(half, 0.0, prod), axis=-1, keepdims=True)
    delta = jnp.where(half, d1, d0)
    lse = pltpu.roll(lse_ref[...], 64, 1)

    def spread(base, x):
        a, b, c = three_parts(-x)
        return jnp.where(spot == 7, a, jnp.where(spot == 8, b, jnp.where(spot == 9, c, base))).astype(B16)

    q_extra = spread(qf, lse)
    g_extra = spread(jnp.zeros_like(qf), delta)
    v_extra = jnp.where((spot >= 7) & (spot <= 9), 1.0, 0.0).astype(B16)
    dk_acc[...] = jnp.zeros_like(dk_acc)
    dv_acc[...] = jnp.zeros_like(dv_acc)
    sides = []
    for e in range(2):
        own = half if e == 0 else ~half
        sides.append(
            (
                jnp.where(own, q, q_extra),
                jnp.where(own, k, kf),
                jnp.where(own, g, g_extra),
                jnp.where(own, v, v_extra),
            )
        )
    for first in range(0, ROW, TILE):
        low, high = key_window(first, TILE)
        dqs, dks, dvs = [], [], []
        for qe, ke, ge, ve in sides:
            s = dotf(qe[first : first + TILE], ke[low:high], NT)
            p = jnp.exp(s)
            d = dotf(ge[first : first + TILE], ve[low:high], NT)
            ds = (p * d).astype(B16)
            dqs.append(dotf(ds, k[low:high]))
            dks.append(dotf(ds, q[first : first + TILE], TN))
            dvs.append(dotf(p.astype(B16), g[first : first + TILE], TN))
        dq_ref[first : first + TILE, :] = (jnp.where(half, dqs[0], dqs[1]) * 0.125).astype(B16)
        dk_acc[low:high, :] += jnp.where(half, dks[0], dks[1])
        dv_acc[low:high, :] += jnp.where(half, dvs[0], dvs[1])
    dk_ref[...] = dk_acc[...].astype(B16)
    dv_ref[...] = dv_acc[...].astype(B16)


def attention_backward(meta, qf, kf, qkv, grad, mixed, lse):
    rows = qkv.shape[0]
    grid, full, blocks, whole = pair_specs(rows)
    shape = jax.ShapeDtypeStruct((rows, 768), B16)

    def kernel(meta, *refs):
        attention_backward_kernel(*refs)

    return pl.pallas_call(
        kernel,
        name="attention_backward",
        grid_spec=pltpu.PrefetchScalarGridSpec(
            num_scalar_prefetch=1,
            grid=grid,
            in_specs=[full, full] + blocks + [whole] * 3,
            out_specs=[whole] * 3,
            scratch_shapes=[pltpu.VMEM((ROW, 128), F32), pltpu.VMEM((ROW, 128), F32)],
        ),
        out_shape=(shape, shape, shape),
        compiler_params=pltpu.CompilerParams(vmem_limit_bytes=VMEM_LIMIT),
    )(meta, qf, kf, qkv, qkv, qkv, grad, mixed, lse)


SUB = 256
PER = 768 // SUB


def mlp_kernel(fast, base, *refs):
    meta, n_ref, c_ref, b_ref = refs[:4]
    count = 4 if fast else 1
    pieces, refs = refs[4 : 4 + count], refs[4 + count :]
    if base:
        held, refs = refs[:2], refs[2:]
    branch_ref, gn_ref, db_ref, own_ref, other_ref = refs[:5]
    w, nt, ct, dw, wsem, dsem = refs[5:]
    t = pl.program_id(0)
    jl, sub = t // PER, t % PER
    me_mp, me_dp = meta[0] % 4, meta[0] // 4

    def loads(j):
        if not fast:
            source = pieces[0].at[:, :, pl.ds(768 * (base + j), 768)]
            return [pltpu.make_async_copy(source, w.at[j], wsem.at[j, 0])]
        out = []
        for dr in range(8):
            rows = pl.multiple_of(96 * jnp.bitwise_xor(me_dp, dr), 32)
            source = pieces[2 * j + (dr & 1)].at[dr >> 1]
            out.append(pltpu.make_async_copy(source, w.at[j, :, pl.ds(rows, 96), :], wsem.at[j, dr]))
        return out

    def stores(j):
        out = []
        for dr in range(8):
            target = (other_ref if j else own_ref).at[dr & 1, dr >> 1]
            out.append(pltpu.make_async_copy(dw.at[j, dr], target, dsem.at[j, dr]))
        return out

    @pl.when(t == 0)
    def _():
        for j in range(2):
            for copy in loads(j):
                copy.start()
        nt[...] = n_ref[...].T
        ct[...] = c_ref[...].T
        if base:
            branch_ref[...] = held[0][...]
            gn_ref[...] = held[1][...]
        else:
            branch_ref[...] = jnp.zeros_like(branch_ref)
            gn_ref[...] = jnp.zeros_like(gn_ref)

    for j in range(2):

        @pl.when(t == PER * j)
        def _():
            for copy in loads(j):
                copy.wait()

    spot = jnp.bitwise_xor(me_mp, base + jl) if fast else base + jl
    cols = pl.ds(pl.multiple_of(sub * SUB, SUB), SUB)
    w1 = w[jl, 0, :, cols]
    w2 = w[jl, 1, :, cols]
    u = dotf(n_ref[...], w1) + b_ref[spot, :, cols]
    cdf = 0.5 * (1.0 + lax.erf(u * 0.7071067811865476))
    hidden = (u * cdf).astype(B16)
    slope = cdf + u * (0.3989422804014327 * jnp.exp(-0.5 * u * u))
    gb = (dotf(c_ref[...], w2) * slope).astype(B16)
    db_ref[jl, :, cols] = jnp.sum(gb.astype(F32), axis=0, keepdims=True)
    branch_ref[...] += dotf(hidden, w2, NT)
    gn_ref[...] += dotf(gb, w1, NT)
    dw1 = dotf(nt[...], gb).astype(B16)
    dw2 = dotf(ct[...], hidden).astype(B16)
    for a in range(8):
        dr = jnp.bitwise_xor(me_dp, a) if fast else a
        dw[jl, dr, 0, :, cols] = dw1[96 * a : 96 * a + 96]
        dw[jl, dr, 1, :, cols] = dw2[96 * a : 96 * a + 96]

    for j in range(2):

        @pl.when(t == PER * j + PER - 1)
        def _():
            for copy in stores(j):
                copy.start()

    @pl.when(t == 2 * PER - 1)
    def _():
        for j in range(2):
            for copy in stores(j):
                copy.wait()


def mlp(meta, normed, cot, bias, pieces, base, held):
    fast = len(pieces) == 4
    tokens = normed.shape[0]
    vmem = pl.BlockSpec(memory_space=pltpu.VMEM)
    anys = pl.BlockSpec(memory_space=pl.ANY)
    shape = jax.ShapeDtypeStruct((2, 4, 2, 96, 768), B16)
    at = 4 + len(pieces)
    return pl.pallas_call(
        partial(mlp_kernel, fast, base),
        name="mlp",
        grid=(2 * PER,),
        in_specs=[pl.BlockSpec(memory_space=pltpu.SMEM), vmem, vmem, vmem]
        + [anys] * len(pieces)
        + [vmem] * len(held),
        out_specs=[vmem, vmem, vmem, anys, anys],
        out_shape=(
            jax.ShapeDtypeStruct((tokens, 768), F32),
            jax.ShapeDtypeStruct((tokens, 768), F32),
            jax.ShapeDtypeStruct((2, 1, 768), F32),
            shape,
            shape,
        ),
        scratch_shapes=[
            pltpu.VMEM((2, 2, 768, 768), B16),
            pltpu.VMEM((768, tokens), B16),
            pltpu.VMEM((768, tokens), B16),
            pltpu.VMEM((2, 8, 2, 96, 768), B16),
            pltpu.SemaphoreType.DMA((2, 8)),
            pltpu.SemaphoreType.DMA((2, 8)),
        ],
        compiler_params=pltpu.CompilerParams(vmem_limit_bytes=VMEM_LIMIT),
    )(meta, normed, cot, bias.reshape(4, 1, 768), *pieces, *held)


def local(
    fast,
    tokens,
    cotangent,
    prompts,
    segments,
    prompt_slot_index,
    norm_gain,
    norm_shift,
    attn_qkv,
    attn_bias,
    attn_out,
    mlp_weight,
    mlp_bias_up,
    mlp_bias_down,
):
    width = tokens.shape[1]
    device = lax.axis_index("dp") * lax.axis_size("mp") + lax.axis_index("mp")
    meta = jnp.reshape(device, (1,)).astype(jnp.int32)
    core = device % 2
    if fast:
        piece = pair_rows(meta, attn_qkv, attn_out)
        piece, tokens, prompts, segments, prompt_slot_index = tie(
            piece, tokens, prompts, segments, prompt_slot_index
        )
        held = z_stage(piece)
    table = jnp.concatenate([prompts, jnp.zeros((128 - NPROMPT, width), F32)], 0)
    start, normed_one, onehot, qf, kf = embed(
        tokens, prompt_slot_index, segments, table, jnp.stack([norm_gain[0], norm_shift[0]])
    )
    bias = jnp.stack([attn_bias[0], jnp.zeros_like(attn_bias[0]), attn_bias[1]])[:, None]
    out_params = jnp.stack([attn_bias[2], norm_gain[1], norm_shift[1]])

    if fast:
        held, mlp_piece, x = tie(held, mlp_weight, (normed_one, start, qf, kf, onehot))
        mlp_z = [mlp_piece] + [px(mlp_piece, 8 * k) for k in range(1, 4)]
        quad, mlp_z, x = tie(xy_stage(held), mlp_z, x)
        own = assemble(meta, quad, "assemble")
        own, mlp_z = tie(own, mlp_z)
        other = px(own, 1)
        stack_mlp = stack(mlp_z, "stack_z")
        normed_one, start, qf, kf, onehot = x
        qkv = project(meta, normed_one, own, bias, 0, ())
        other, stack_mlp, qkv = tie(other, stack_mlp, qkv)
        mlp_x, mlp_y = px(stack_mlp, 2), px(stack_mlp, 4)
        stack_mlp_other = px(stack_mlp, 1)
    else:
        qkv_all = lax.all_gather(attn_qkv, AXES, axis=1, tiled=True)
        out_all = lax.all_gather(attn_out, AXES, axis=0, tiled=True)
        mlp_all = lax.all_gather(mlp_weight, "dp", axis=1, tiled=True)
        mlp_all = lax.all_gather(mlp_all, "mp", axis=2, tiled=True)
        four_all = jnp.concatenate([qkv_all, out_all[None]])
        own = lax.dynamic_slice_in_dim(four_all, 384 * core, 384, 2)
        other = lax.dynamic_slice_in_dim(four_all, 384 * (1 - core), 384, 2)
        qkv = project(meta, normed_one, own, bias, 0, ())
    qkv = project(meta, normed_one, other, bias, 1, (qkv,))
    mixed, lse = attention_forward(meta, qf, kf, qkv)
    if fast:
        mlp_y, mlp_x, stack_mlp, mixed = tie(mlp_y, mlp_x, (stack_mlp, stack_mlp_other), mixed)
        mlp_y_other, mlp_x_other, mlp_xy = px(mlp_y, 1), px(mlp_x, 1), px(stack_mlp[0], 6)
    middle, normed_two, out_weight = out_projection(meta, mixed, start, own, other, out_params)
    if fast:
        mlp_y_other, normed_two = tie(mlp_y_other, normed_two)
        pieces_a = [stack_mlp[0], mlp_y, stack_mlp[1], mlp_y_other]
        branch, grad_two, up_a, own_a, other_a = mlp(meta, normed_two, cotangent, mlp_bias_up, pieces_a, 0, ())
        mlp_x, mlp_xy, other_a, branch, grad_two = tie(
            (mlp_x, mlp_x_other), mlp_xy, other_a, branch, grad_two
        )
        pieces_b = [mlp_x[0], mlp_xy, mlp_x[1], px(mlp_xy, 1)]
        got_a = px(other_a, 1)
        branch, grad_two, up_b, own_b, other_b = mlp(
            meta, normed_two, cotangent, mlp_bias_up, pieces_b, 2, (branch, grad_two)
        )
        other_b, got_a, grad_two, branch = tie(other_b, got_a, grad_two, branch)
        got_b = px(other_b, 1)
        up_rows = jnp.concatenate([up_a[:, 0], up_b[:, 0]])
        spots = jnp.bitwise_xor(jnp.arange(4), device % 4)
        grad_up = (jnp.arange(4)[:, None] == spots[None, :]).astype(F32)
        grad_up = jnp.sum(grad_up[:, :, None] * up_rows[None], axis=1)
    else:
        branch, grad_two, up_a, own_a, other_a = mlp(meta, normed_two, cotangent, mlp_bias_up, [mlp_all], 0, ())
        branch, grad_two, up_b, own_b, other_b = mlp(
            meta, normed_two, cotangent, mlp_bias_up, [mlp_all], 2, (branch, grad_two)
        )
        grad_up = jnp.concatenate([up_a[:, 0], up_b[:, 0]])
    turn_params = jnp.stack([norm_gain[1], mlp_bias_down])
    output, grad_middle, grad_mixed, own_out, other_out, sums_two = turn(
        meta, middle, branch, grad_two, cotangent, mixed, out_weight, turn_params
    )
    if fast:
        got_b, grad_mixed, other_out = tie(got_b, grad_mixed, other_out)
        sum_a = add_parts(own_a, got_a)
        sum_b = add_parts(own_b, got_b)
        send_x = sum_b[:, :, 0].astype(B16)
        send_y = jnp.stack([sum_a[1, :, 1], sum_b[1, :, 1]]).astype(B16)
        send_x, send_y, grad_mixed, other_out = tie(send_x, send_y, grad_mixed, other_out)
        got_x, got_y, got_out = px(send_x, 2), px(send_y, 4), px(other_out, 1)
    grads = attention_backward(meta, qf, kf, qkv, grad_mixed, mixed, lse)
    if fast:
        got_x, got_y, got_out, grads, grad_middle = tie(got_x, got_y, got_out, grads, grad_middle)
        first = add_parts(sum_a[:, :, 0], got_x)
        second = [add_parts(sum_a[0, :, 1], got_y[0]), add_parts(sum_b[0, :, 1], got_y[1])]
        send_x, send_y, grads = tie(second[1].astype(B16), first[1].astype(B16), grads)
        got_x, got_y = px(send_x, 2), px(send_y, 4)
        own_w, other_w = weight_grad(meta, normed_one, grads, "weight_grad_qkv")
        other_w, got_x, got_y, grads, grad_middle = tie(other_w, got_x, got_y, grads, grad_middle)
        got_w = px(other_w, 1)
        col = [add_parts(first[0], got_y), add_parts(second[0], got_x)]
        col_send = [jnp.stack([c[i].astype(B16) for c in col]) for i in range(1, 4)]
        got_w, col_send, grads = tie(got_w, col_send, grads)
        keep, *sends = gather_sums(own_w, got_w, own_out, got_out)
        sends, col_send, grads, grad_middle = tie(sends, col_send, grads, grad_middle)
        moved = [px(x, 2 * i + 2) for i, x in enumerate(sends)]
        last_mlp = [px(x, 8 * i + 8) for i, x in enumerate(col_send)]
    input_grad, prompt_sums, sums_one = tail_step(
        meta, start, grad_middle, onehot, norm_gain[0:1], (own, other), grads
    )

    small = jnp.concatenate(
        [
            prompt_sums[:NPROMPT],
            sums_one[0:1],
            sums_two[0:1],
            sums_one[1:2],
            sums_two[1:2],
            sums_one[2:4],
            sums_two[2:4],
            grad_up,
        ]
    )
    if fast:
        packed = pack_small(small)
        packed = pack_small(open_small(packed) + open_small(px(packed, 1)))
        packed = pack_small(open_small(packed) + open_small(px(packed, 2)))
        packed = pack_small(open_small(packed) + open_small(px(packed, 4)))
        moved, packed = tie(moved, packed)
        col_attn, *last = plane_sums(keep, moved)
        last = [px(x, 8 * i + 8) for i, x in enumerate(last)]
        small = four([open_small(x) for x in [packed] + [px(packed, 8 * i) for i in range(1, 4)]])
        mine = jnp.stack([c[0] for c in col])
        mlp_grad = four([mine] + [x.astype(F32) for x in last_mlp])
        qkv_grad, out_grad = line_sums(col_attn, last)
    else:
        mlp_grad = jnp.stack([own_a, other_a, own_b, other_b]).transpose(3, 2, 1, 4, 0, 5)
        mlp_grad = mlp_grad.reshape(2, 768, 3072)
        mlp_grad = lax.psum_scatter(mlp_grad, "dp", scatter_dimension=1, tiled=True)
        mlp_grad = lax.psum_scatter(mlp_grad, "mp", scatter_dimension=2, tiled=True).astype(F32)
        grad_out_weight = dotf(mixed, grad_middle.astype(B16), TN)
        grad_qkv = jnp.stack([dotf(normed_one, g, TN) for g in grads])
        qkv_grad = lax.psum_scatter(grad_qkv, AXES, scatter_dimension=1, tiled=True)
        out_grad = lax.psum_scatter(grad_out_weight, AXES, scatter_dimension=0, tiled=True)
        small = lax.psum(small, AXES)
    at = NPROMPT
    return (
        output.astype(B16),
        input_grad,
        small[:at],
        small[at : at + 2],
        small[at + 2 : at + 4],
        qkv_grad,
        small[at + 4 : at + 7],
        out_grad,
        mlp_grad,
        small[at + 8 :].reshape(-1),
        small[at + 7],
    )


def solution(mesh):
    fast = dict(mesh.shape) == {"dp": 8, "mp": 4}
    return jax.shard_map(
        partial(local, fast),
        mesh=mesh,
        in_specs=(
            P(AXES, None),
            P(AXES, None),
            P(),
            P(AXES),
            P(AXES),
            P(),
            P(),
            P(None, AXES, None),
            P(),
            P(AXES, None),
            P(None, "dp", "mp"),
            P(),
            P(),
        ),
        out_specs=(
            P(AXES, None),
            P(AXES, None),
            P(),
            P(),
            P(),
            P(None, AXES, None),
            P(),
            P(AXES, None),
            P(None, "dp", "mp"),
            P(),
            P(),
        ),
        check_vma=False,
    )
```

```python
from functools import partial

import jax
import jax.numpy as jnp
from jax import lax
from jax.experimental import pallas as pl
from jax.experimental.pallas import tpu as pltpu
from jax.sharding import PartitionSpec as P

NPROMPT = 50
ROW = 1024
SPANS = (151, 247, 627)
EPS = 1e-06
HIGHEST = lax.Precision.HIGHEST
BIG = 1e30
B16 = jnp.bfloat16
F32 = jnp.float32
AXES = ("dp", "mp")
TILE = 256
STEP = 512
QROWS = 512
NT = (((1,), (1,)), ((), ()))
TN = (((0,), (0,)), ((), ()))
VMEM_LIMIT = 60 * 1024 * 1024


def layer_norm(value_list, gain_row, shift_row):
    centre = jnp.mean(value_list, axis=-1, keepdims=True)
    centred = value_list - centre
    spread = jnp.mean(centred * centred, axis=-1, keepdims=True)
    return centred * lax.rsqrt(spread + EPS) * gain_row + shift_row


def key_window(first, count):
    low, high = ROW, 0
    for span in SPANS:
        whole = ROW // span
        for row in (first, first + count - 1):
            seg = min(row // span, whole)
            low = min(low, seg * span)
            high = max(high, ROW if seg == whole else (seg + 1) * span)
    return low // 128 * 128, -(-high // 128) * 128


def dotf(a, b, dims=None):
    if dims is None:
        return jnp.dot(a, b, preferred_element_type=F32)
    return lax.dot_general(a, b, dims, preferred_element_type=F32)


def px(x, k):
    return lax.ppermute(x, AXES, [(i, i ^ k) for i in range(32)])


def tie(*trees):
    return lax.optimization_barrier(trees)


def stack_kernel(*refs):
    for i, ref in enumerate(refs[:-1]):
        refs[-1][i] = ref[...]


def stack(parts, name):
    vmem = pl.BlockSpec(memory_space=pltpu.VMEM)
    return pl.pallas_call(
        stack_kernel,
        name=name,
        out_shape=jax.ShapeDtypeStruct((len(parts),) + parts[0].shape, parts[0].dtype),
        in_specs=[vmem] * len(parts),
        out_specs=vmem,
    )(*parts)


def z_stage(piece):
    return stack([piece] + [px(piece, 8 * k) for k in range(1, 4)], "stack_z")


def stack_pair_kernel(*refs):
    for i, ref in enumerate(refs[:-2]):
        for c in range(2):
            refs[c - 2][i] = ref[c]


def stack_pair(parts):
    vmem = pl.BlockSpec(memory_space=pltpu.VMEM)
    shape = jax.ShapeDtypeStruct((len(parts),) + parts[0].shape[1:], parts[0].dtype)
    return pl.pallas_call(
        stack_pair_kernel,
        name="stack_pair",
        out_shape=(shape, shape),
        in_specs=[vmem] * len(parts),
        out_specs=(vmem, vmem),
    )(*parts)


def xy_stage(parts):
    return [parts] + [px(parts, 2 * k) for k in range(1, 4)]


def split_kernel(meta, qkv_ref, out_ref, mine_ref, theirs_ref):
    core = meta[0] % 2
    for ref, half in ((mine_ref, core), (theirs_ref, 1 - core)):
        cols = pl.ds(pl.multiple_of(384 * half, 128), 384)
        ref[0:3] = qkv_ref[:, :, cols]
        ref[3] = out_ref[:, cols]


def join_kernel(meta, mine_ref, got_ref, out_ref):
    for core in range(2):

        @pl.when(meta[0] % 2 == core)
        def _():
            out_ref[...] = jnp.concatenate([mine_ref[...], got_ref[...]][:: 1 - 2 * core], 1)


def pair_rows(meta, qkv, out):
    vmem = pl.BlockSpec(memory_space=pltpu.VMEM)
    smem = pl.BlockSpec(memory_space=pltpu.SMEM)
    half = jax.ShapeDtypeStruct((4, 24, 384), B16)
    mine, theirs = pl.pallas_call(
        split_kernel, name="split", out_shape=(half, half), in_specs=[smem, vmem, vmem], out_specs=(vmem, vmem)
    )(meta, qkv, out)
    return pl.pallas_call(
        join_kernel,
        name="join",
        out_shape=jax.ShapeDtypeStruct((4, 48, 384), B16),
        in_specs=[smem, vmem, vmem],
        out_specs=vmem,
    )(meta, mine, px(theirs, 1))


def assemble_kernel(meta, *refs):
    pieces, out, sems = refs[:4], refs[4], refs[5]
    copies = []
    for xy in range(4):
        for z in range(4):
            rows = pl.multiple_of(48 * jnp.bitwise_xor(meta[0] // 2, xy + 4 * z), 16)
            copies.append(
                pltpu.make_async_copy(pieces[xy].at[z], out.at[:, pl.ds(rows, 48), :], sems.at[4 * xy + z])
            )
    for copy in copies:
        copy.start()
    for copy in copies:
        copy.wait()


def assemble(meta, pieces, name):
    return pl.pallas_call(
        assemble_kernel,
        name=name,
        out_shape=jax.ShapeDtypeStruct((4, 768, 384), B16),
        in_specs=[pl.BlockSpec(memory_space=pltpu.SMEM)] + [pl.BlockSpec(memory_space=pl.ANY)] * 4,
        out_specs=pl.BlockSpec(memory_space=pltpu.VMEM),
        scratch_shapes=[pltpu.SemaphoreType.DMA((16,))],
    )(meta, *pieces)


def project_kernel(side, meta, x_ref, w_ref, b_ref, *refs):
    half = jnp.bitwise_xor(meta[0] % 2, side)
    cols = pl.ds(pl.multiple_of(384 * half, 128), 384)
    y = dotf(x_ref[...], w_ref[0]) + b_ref[pl.program_id(0), :, cols]
    refs[-1][...] = y.astype(B16)


def project(meta, x, weight, bias, side, held):
    rows = x.shape[0]
    vmem = pl.BlockSpec(memory_space=pltpu.VMEM)
    return pl.pallas_call(
        partial(project_kernel, side),
        name="project",
        grid=(3,),
        out_shape=jax.ShapeDtypeStruct((rows, 2304), B16),
        in_specs=[
            pl.BlockSpec(memory_space=pltpu.SMEM),
            vmem,
            pl.BlockSpec((1, 768, 384), lambda c: (c, 0, 0)),
            vmem,
        ]
        + [pl.BlockSpec(memory_space=pl.ANY)] * len(held),
        out_specs=pl.BlockSpec((rows, 384), lambda c: (0, 3 * side + c)),
        input_output_aliases={4 + i: i for i in range(len(held))},
        compiler_params=pltpu.CompilerParams(vmem_limit_bytes=VMEM_LIMIT),
    )(meta, x, weight, bias, *held)


def embed_kernel(tokens_ref, slots_ref, segs_ref, table_ref, p_ref, start_ref, normed_ref, hot_ref, qf_ref, kf_ref):
    lane = lax.broadcasted_iota(jnp.int32, (TILE, 128), 1)
    slots, segs = slots_ref[...], segs_ref[...]
    is_prompt = slots < NPROMPT
    hot = jnp.where((lane == slots) & is_prompt, 1.0, 0.0).astype(B16)
    hot_ref[...] = hot
    rows = None
    for part in three_parts(table_ref[...]):
        term = dotf(hot, part.astype(B16))
        rows = term if rows is None else rows + term
    start = jnp.where(is_prompt, rows, tokens_ref[...].astype(F32))
    start_ref[...] = start
    normed_ref[...] = (centred(start)[0] * p_ref[0:1] + p_ref[1:2]).astype(B16)
    spot = lane % 64
    same = (spot == segs) & (spot < 7)
    qf_ref[...] = jnp.where(same, 1.0, 0.0).astype(B16)
    kf = jnp.where(spot < 7, jnp.where(same, 0.0, -BIG), jnp.where(spot < 10, 1.0, 0.0))
    kf_ref[...] = kf.astype(B16)


def embed(tokens, slots, segs, table, params):
    rows = tokens.shape[0]

    def block(width):
        return pl.BlockSpec((TILE, width), lambda i: (i, 0))

    vmem = pl.BlockSpec(memory_space=pltpu.VMEM)
    lanes = jax.ShapeDtypeStruct((rows, 128), B16)
    return pl.pallas_call(
        embed_kernel,
        name="embed",
        grid=(rows // TILE,),
        in_specs=[block(768), block(1), block(1), vmem, vmem],
        out_specs=[block(768), block(768), block(128), block(128), block(128)],
        out_shape=(
            jax.ShapeDtypeStruct((rows, 768), F32),
            jax.ShapeDtypeStruct((rows, 768), B16),
            lanes,
            lanes,
            lanes,
        ),
    )(tokens, slots[:, None], segs[:, None], table, params)


def gather_sums_kernel(own_ref, got_ref, own_out_ref, got_out_ref, keep_ref, *sends):
    for k in range(4):
        for z in range(4):
            for m in range(4):
                if m < 3:
                    x = add_parts(own_ref[k, z, m], got_ref[k, z, m])
                else:
                    x = add_parts(own_out_ref[k, z, 0], got_out_ref[k, z, 0])
                if k:
                    sends[k - 1][z, m] = x.astype(B16)
                else:
                    keep_ref[z, m] = x


def gather_sums(own, got, own_out, got_out):
    vmem = pl.BlockSpec(memory_space=pltpu.VMEM)
    send = jax.ShapeDtypeStruct((4, 4, 24, 768), B16)
    return pl.pallas_call(
        gather_sums_kernel,
        name="gather_sums",
        in_specs=[vmem] * 4,
        out_specs=[vmem] * 4,
        out_shape=(jax.ShapeDtypeStruct((4, 4, 24, 768), F32), send, send, send),
        compiler_params=pltpu.CompilerParams(vmem_limit_bytes=VMEM_LIMIT),
    )(own, got, own_out, got_out)


def four(values):
    return (values[0] + values[1]) + (values[2] + values[3])


def plane_sums_kernel(keep_ref, *refs):
    moved, (col_ref, *sends) = refs[:3], refs[3:]
    for z in range(4):
        for m in range(4):
            x = four([keep_ref[z, m]] + [ref[z, m].astype(F32) for ref in moved])
            if z:
                sends[z - 1][m] = x.astype(B16)
            else:
                col_ref[m] = x


def plane_sums(keep, moved):
    vmem = pl.BlockSpec(memory_space=pltpu.VMEM)
    send = jax.ShapeDtypeStruct((4, 24, 768), B16)
    return pl.pallas_call(
        plane_sums_kernel,
        name="plane_sums",
        in_specs=[vmem] * 4,
        out_specs=[vmem] * 4,
        out_shape=(jax.ShapeDtypeStruct((4, 24, 768), F32), send, send, send),
        compiler_params=pltpu.CompilerParams(vmem_limit_bytes=VMEM_LIMIT),
    )(keep, *moved)


def line_sums_kernel(col_ref, *refs):
    last, (qkv_ref, out_ref) = refs[:3], refs[3:]
    for m in range(4):
        x = four([col_ref[m]] + [ref[m].astype(F32) for ref in last])
        if m < 3:
            qkv_ref[m] = x
        else:
            out_ref[...] = x


def line_sums(col, last):
    vmem = pl.BlockSpec(memory_space=pltpu.VMEM)
    return pl.pallas_call(
        line_sums_kernel,
        name="line_sums",
        in_specs=[vmem] * 4,
        out_specs=[vmem] * 2,
        out_shape=(jax.ShapeDtypeStruct((3, 24, 768), F32), jax.ShapeDtypeStruct((24, 768), F32)),
    )(col, *last)


def centred(x):
    mean = jnp.mean(x, axis=-1, keepdims=True)
    x = x - mean
    rate = lax.rsqrt(jnp.mean(x * x, axis=-1, keepdims=True) + EPS)
    return x * rate, rate


def out_kernel(meta, x_ref, start_ref, own_ref, other_ref, p_ref, middle_ref, normed_ref, w_ref):
    core = meta[0] % 2

    @pl.when(pl.program_id(0) == 0)
    def _():
        for ref, half in ((own_ref, core), (other_ref, 1 - core)):
            w_ref[:, pl.ds(pl.multiple_of(384 * half, 128), 384)] = ref[3]

    middle = start_ref[...] + dotf(x_ref[...], w_ref[...]) + p_ref[0:1]
    middle_ref[...] = middle
    normed_ref[...] = (centred(middle)[0] * p_ref[1:2] + p_ref[2:3]).astype(B16)


def out_projection(meta, mixed, start, own, other, params):
    rows = mixed.shape[0]
    block = pl.BlockSpec((STEP, 768), lambda i: (i, 0))
    vmem = pl.BlockSpec(memory_space=pltpu.VMEM)
    return pl.pallas_call(
        out_kernel,
        name="out_projection",
        grid=(rows // STEP,),
        in_specs=[pl.BlockSpec(memory_space=pltpu.SMEM), block, block, vmem, vmem, vmem],
        out_specs=[block, block, vmem],
        out_shape=(
            jax.ShapeDtypeStruct((rows, 768), F32),
            jax.ShapeDtypeStruct((rows, 768), B16),
            jax.ShapeDtypeStruct((768, 768), B16),
        ),
        compiler_params=pltpu.CompilerParams(vmem_limit_bytes=VMEM_LIMIT),
    )(meta, mixed, start, own, other, params)


def norm_backward(normal, rate, grad, gain):
    u = grad * gain
    return rate * (u - jnp.mean(u, axis=-1, keepdims=True) - normal * jnp.mean(u * normal, axis=-1, keepdims=True))


def row_sum(x):
    return jnp.sum(x, axis=0, keepdims=True)


def put_parts(meta, acc, own_ref, other_ref, m):
    chip, core = meta[0] // 2, meta[0] % 2
    for z in range(4):
        for xy in range(4):
            row = 48 * jnp.bitwise_xor(chip, xy + 4 * z)
            own_ref[xy, z, m] = acc[pl.ds(pl.multiple_of(row + 24 * core, 8), 24), :].astype(B16)
            other_ref[xy, z, m] = acc[pl.ds(pl.multiple_of(row + 24 * (1 - core), 8), 24), :].astype(B16)


def turn_kernel(
    meta, middle_ref, branch_ref, grad_ref, cot_ref, mixed_ref, w_ref, p_ref,
    output_ref, gmiddle_ref, gmixed_ref, own_ref, other_ref, sums_ref, acc,
):
    i = pl.program_id(0)

    @pl.when(i == 0)
    def _():
        sums_ref[...] = jnp.zeros_like(sums_ref)
        acc[...] = jnp.zeros_like(acc)

    middle, grad = middle_ref[...], grad_ref[...]
    cot = cot_ref[...].astype(F32)
    output_ref[...] = (middle + branch_ref[...] + p_ref[1:2]).astype(B16)
    normal, rate = centred(middle)
    gmiddle = cot + norm_backward(normal, rate, grad, p_ref[0:1])
    gmiddle_ref[...] = gmiddle
    low = gmiddle.astype(B16)
    for row, x in enumerate((normal * grad, grad, low.astype(F32), cot)):
        sums_ref[row : row + 1, :] += row_sum(x)
    gmixed_ref[...] = dotf(low, w_ref[...], NT).astype(B16)
    acc[...] += dotf(mixed_ref[...], low, TN)

    @pl.when(i == pl.num_programs(0) - 1)
    def _():
        put_parts(meta, acc, own_ref, other_ref, 0)


def turn(meta, middle, branch, grad, cot, mixed, weight, params):
    rows = middle.shape[0]
    block = pl.BlockSpec((STEP, 768), lambda i: (i, 0))
    vmem = pl.BlockSpec(memory_space=pltpu.VMEM)
    parts = jax.ShapeDtypeStruct((4, 4, 1, 24, 768), B16)
    return pl.pallas_call(
        turn_kernel,
        name="turn",
        grid=(rows // STEP,),
        in_specs=[pl.BlockSpec(memory_space=pltpu.SMEM)] + [block] * 5 + [vmem, vmem],
        out_specs=[block, block, block, vmem, vmem, vmem],
        out_shape=(
            jax.ShapeDtypeStruct((rows, 768), B16),
            jax.ShapeDtypeStruct((rows, 768), F32),
            jax.ShapeDtypeStruct((rows, 768), B16),
            parts,
            parts,
            jax.ShapeDtypeStruct((8, 768), F32),
        ),
        scratch_shapes=[pltpu.VMEM((768, 768), F32)],
        compiler_params=pltpu.CompilerParams(vmem_limit_bytes=VMEM_LIMIT),
    )(meta, middle, branch, grad, cot, mixed, weight, params)


def tail_kernel(meta, start_ref, gmiddle_ref, slots_ref, p_ref, turn_ref, up_ref, *refs):
    weights, grads = refs[:2], refs[2:5]
    input_ref, packed_ref, prompt_ref, sums_ref = refs[5:]
    core = meta[0] % 2

    @pl.when(pl.program_id(0) == 0)
    def _():
        prompt_ref[...] = jnp.zeros_like(prompt_ref)
        sums_ref[...] = jnp.zeros_like(sums_ref)

    total = None
    for c in range(3):
        for side in range(2):
            half = jnp.bitwise_xor(core, side)
            left = grads[c][:, pl.ds(pl.multiple_of(384 * half, 128), 384)]
            term = dotf(left, weights[side][c], NT)
            total = term if total is None else total + term
    normal, rate = centred(start_ref[...])
    rows = ((0, normal * total), (2, total), (4, grads[0][...].astype(F32)), (5, grads[2][...].astype(F32)))
    for row, x in rows:
        sums_ref[row : row + 1, :] += row_sum(x)
    gstart = gmiddle_ref[...] + norm_backward(normal, rate, total, p_ref[0:1])
    slots = slots_ref[...]
    is_prompt = jnp.sum(slots.astype(F32), axis=-1, keepdims=True) > 0.5
    input_ref[...] = jnp.where(is_prompt, 0.0, gstart)
    for part in three_parts(gstart):
        prompt_ref[...] += dotf(slots, part.astype(B16), TN)

    @pl.when(pl.program_id(0) == pl.num_programs(0) - 1)
    def _():
        for row, source in ((1, 0), (3, 1), (6, 2), (7, 3)):
            sums_ref[row : row + 1, :] = turn_ref[source : source + 1, :]
        for row in range(4):
            sums_ref[8 + row : 9 + row, :] = up_ref[row]
        packed_ref[0:64, :] = prompt_ref[0:64, :].astype(B16)
        high, low = split_rows(sums_ref[...])
        packed_ref[64:80, :] = high
        packed_ref[80:96, :] = low


def tail_step(meta, start, gmiddle, slots, params, sums_two, up, weights, grads):
    rows = start.shape[0]

    def block(width):
        return pl.BlockSpec((STEP, width), lambda i: (i, 0))

    vmem = pl.BlockSpec(memory_space=pltpu.VMEM)
    return pl.pallas_call(
        tail_kernel,
        name="tail_step",
        grid=(rows // STEP,),
        in_specs=[pl.BlockSpec(memory_space=pltpu.SMEM), block(768), block(768), block(128)]
        + [vmem] * 3
        + [pl.BlockSpec((3, 768, 384), lambda i: (0, 0, 0))] * 2
        + [block(768)] * 3,
        out_specs=[block(768), vmem],
        out_shape=(
            jax.ShapeDtypeStruct((rows, 768), F32),
            jax.ShapeDtypeStruct((96, 768), B16),
        ),
        scratch_shapes=[pltpu.VMEM((128, 768), F32), pltpu.VMEM((16, 768), F32)],
        compiler_params=pltpu.CompilerParams(vmem_limit_bytes=VMEM_LIMIT),
    )(meta, start, gmiddle, slots, params, sums_two, up, *weights, *grads)


def weight_grad_kernel(count, meta, left_ref, *refs):
    rights, own_ref, other_ref, acc = refs[:count], refs[count], refs[count + 1], refs[count + 2]
    for m in range(count):
        acc[...] = dotf(left_ref[...], rights[m][...], TN)
        put_parts(meta, acc, own_ref, other_ref, m)


def weight_grad(meta, left, rights, name):
    count, width = len(rights), rights[0].shape[1]
    shape = jax.ShapeDtypeStruct((4, 4, count, 24, width), B16)
    vmem = pl.BlockSpec(memory_space=pltpu.VMEM)
    return pl.pallas_call(
        partial(weight_grad_kernel, count),
        name=name,
        out_shape=(shape, shape),
        in_specs=[pl.BlockSpec(memory_space=pltpu.SMEM)] + [vmem] * (count + 1),
        out_specs=(vmem, vmem),
        scratch_shapes=[pltpu.VMEM((left.shape[1], width), F32)],
        compiler_params=pltpu.CompilerParams(vmem_limit_bytes=VMEM_LIMIT),
    )(meta, left, *rights)


def split_rows(rest):
    high = rest.astype(B16)
    return high, (rest - high.astype(F32)).astype(B16)


def add_small(x, y):
    x, y = x.astype(F32), y.astype(F32)
    return jnp.concatenate([x[:64] + y[:64], (x[64:80] + x[80:]) + (y[64:80] + y[80:])])


def pack_small(x):
    return jnp.concatenate([x[:64].astype(B16), *split_rows(x[64:])])


def exchange_small(x, k):
    return add_small(x, px(x, k))


def add_parts(own, got):
    return own.astype(F32) + got.astype(F32)


def three_parts(x):
    high = x.astype(B16).astype(F32)
    mid = (x - high).astype(B16).astype(F32)
    return high, mid, (x - high) - mid


def attention_forward_kernel(qf_ref, kf_ref, q_ref, k_ref, v_ref, mixed_ref, lse_ref):
    half = lax.broadcasted_iota(jnp.int32, (1, 128), 1) < 64
    q = q_ref[...] * jnp.asarray(0.125, B16)
    k, v = k_ref[...], v_ref[...]
    qf, kf = qf_ref[...], kf_ref[...]
    one = jnp.ones((), B16)
    sides = []
    for e in range(2):
        own = half if e == 0 else ~half
        sides.append((jnp.where(own, q, qf), jnp.where(own, k, kf), jnp.where(own, v, one)))
    for first in range(0, ROW, QROWS):
        low, high = key_window(first, QROWS)
        outs, peaks = [], []
        for qe, ke, ve in sides:
            s = dotf(qe[first : first + QROWS], ke[low:high], NT)
            peak = jnp.max(s, axis=-1, keepdims=True)
            p = jnp.exp(s - peak).astype(B16)
            outs.append(dotf(p, ve[low:high]))
            peaks.append(peak)
        data = jnp.where(half, outs[0], outs[1])
        total = pltpu.roll(jnp.where(half, outs[1], outs[0]), 64, 1)
        mixed_ref[first : first + QROWS, :] = (data / total).astype(B16)
        lse_ref[first : first + QROWS, :] = jnp.where(half, peaks[0], peaks[1]) + jnp.log(total)


def pair_specs(rows):
    full = pl.BlockSpec((ROW, 128), lambda r, s, p, meta: (r, 0))
    blocks = [pl.BlockSpec((ROW, 128), lambda r, s, p, meta, c=c: (r, 9 * s + 3 * c + p)) for c in range(3)]
    whole = pl.BlockSpec((ROW, 128), lambda r, s, p, meta: (r, 3 * jnp.bitwise_xor(meta[0] % 2, s) + p))
    return (rows // ROW, 2, 3), full, blocks, whole


def attention_forward(meta, qf, kf, qkv):
    rows = qkv.shape[0]
    grid, full, blocks, whole = pair_specs(rows)

    def kernel(meta, *refs):
        attention_forward_kernel(*refs)

    return pl.pallas_call(
        kernel,
        name="attention_forward",
        grid_spec=pltpu.PrefetchScalarGridSpec(
            num_scalar_prefetch=1, grid=grid, in_specs=[full, full] + blocks, out_specs=[whole, whole]
        ),
        out_shape=(
            jax.ShapeDtypeStruct((rows, 768), B16),
            jax.ShapeDtypeStruct((rows, 768), F32),
        ),
        compiler_params=pltpu.CompilerParams(vmem_limit_bytes=VMEM_LIMIT),
    )(meta, qf, kf, qkv, qkv, qkv)


def attention_backward_kernel(
    qf_ref, kf_ref, q_ref, k_ref, v_ref, g_ref, mixed_ref, lse_ref, dq_ref, dk_ref, dv_ref, dk_acc, dv_acc
):
    lane = lax.broadcasted_iota(jnp.int32, (1, 128), 1)
    half = lane < 64
    spot = lane % 64
    q = q_ref[...] * jnp.asarray(0.125, B16)
    k, v, g = k_ref[...], v_ref[...], g_ref[...]
    qf, kf = qf_ref[...].astype(F32), kf_ref[...]
    prod = g.astype(F32) * mixed_ref[...].astype(F32)
    d0 = jnp.sum(jnp.where(half, prod, 0.0), axis=-1, keepdims=True)
    d1 = jnp.sum(jnp.where(half, 0.0, prod), axis=-1, keepdims=True)
    delta = jnp.where(half, d1, d0)
    lse = pltpu.roll(lse_ref[...], 64, 1)

    def spread(base, x):
        a, b, c = three_parts(-x)
        return jnp.where(spot == 7, a, jnp.where(spot == 8, b, jnp.where(spot == 9, c, base))).astype(B16)

    q_extra = spread(qf, lse)
    g_extra = spread(jnp.zeros_like(qf), delta)
    v_extra = jnp.where((spot >= 7) & (spot <= 9), 1.0, 0.0).astype(B16)
    dk_acc[...] = jnp.zeros_like(dk_acc)
    dv_acc[...] = jnp.zeros_like(dv_acc)
    sides = []
    for e in range(2):
        own = half if e == 0 else ~half
        sides.append(
            (
                jnp.where(own, q, q_extra),
                jnp.where(own, k, kf),
                jnp.where(own, g, g_extra),
                jnp.where(own, v, v_extra),
            )
        )
    for first in range(0, ROW, TILE):
        low, high = key_window(first, TILE)
        dqs, dks, dvs = [], [], []
        for qe, ke, ge, ve in sides:
            s = dotf(qe[first : first + TILE], ke[low:high], NT)
            p = jnp.exp(s)
            d = dotf(ge[first : first + TILE], ve[low:high], NT)
            ds = (p * d).astype(B16)
            dqs.append(dotf(ds, k[low:high]))
            dks.append(dotf(ds, q[first : first + TILE], TN))
            dvs.append(dotf(p.astype(B16), g[first : first + TILE], TN))
        dq_ref[first : first + TILE, :] = (jnp.where(half, dqs[0], dqs[1]) * 0.125).astype(B16)
        dk_acc[low:high, :] += jnp.where(half, dks[0], dks[1])
        dv_acc[low:high, :] += jnp.where(half, dvs[0], dvs[1])
    dk_ref[...] = dk_acc[...].astype(B16)
    dv_ref[...] = dv_acc[...].astype(B16)


def attention_backward(meta, qf, kf, qkv, grad, mixed, lse):
    rows = qkv.shape[0]
    grid, full, blocks, whole = pair_specs(rows)
    shape = jax.ShapeDtypeStruct((rows, 768), B16)

    def kernel(meta, *refs):
        attention_backward_kernel(*refs)

    return pl.pallas_call(
        kernel,
        name="attention_backward",
        grid_spec=pltpu.PrefetchScalarGridSpec(
            num_scalar_prefetch=1,
            grid=grid,
            in_specs=[full, full] + blocks + [whole] * 3,
            out_specs=[whole] * 3,
            scratch_shapes=[pltpu.VMEM((ROW, 128), F32), pltpu.VMEM((ROW, 128), F32)],
        ),
        out_shape=(shape, shape, shape),
        compiler_params=pltpu.CompilerParams(vmem_limit_bytes=VMEM_LIMIT),
    )(meta, qf, kf, qkv, qkv, qkv, grad, mixed, lse)


SUB = 256
PER = 768 // SUB


def mlp_kernel(fast, *refs):
    meta, n_ref, c_ref, b_ref = refs[:4]
    count = 16 if fast else 1
    pieces, refs = refs[4 : 4 + count], refs[4 + count :]
    branch_ref, gn_ref, db_ref, own_ref, other_ref = refs[:5]
    w, nt, ct, dw, wsem, dsem = refs[5:]
    t = pl.program_id(0)
    jr, sub = t // PER, t % PER
    me_mp, me_dp = meta[0] % 4, meta[0] // 4

    def loads(j):
        if not fast:
            source = pieces[0].at[:, :, pl.ds(768 * j, 768)]
            return [pltpu.make_async_copy(source, w.at[j], wsem.at[j, 0, 0])]
        out = []
        for dr in range(8):
            rows = pl.multiple_of(96 * jnp.bitwise_xor(me_dp, dr), 32)
            for c in range(2):
                source = pieces[8 * (j & 1) + 4 * c + (j >> 1) + 2 * (dr & 1)].at[dr >> 1]
                out.append(pltpu.make_async_copy(source, w.at[j, c, pl.ds(rows, 96), :], wsem.at[j, dr, c]))
        return out

    def stores(j):
        if not fast:
            return [pltpu.make_async_copy(dw.at[j], own_ref.at[j], dsem.at[j, 0, 0])]
        out = []
        for dr in range(8):
            x, y = j >> 1, dr & 1
            for c, spot in enumerate((2 * x + y, 2 * y + x)):
                target = (other_ref if j & 1 else own_ref).at[c, spot, dr >> 1]
                out.append(pltpu.make_async_copy(dw.at[j, dr, c], target, dsem.at[j, dr, c]))
        return out

    @pl.when(t == 0)
    def _():
        for j in range(4):
            for copy in loads(j):
                copy.start()
        nt[...] = n_ref[...].T
        ct[...] = c_ref[...].T
        branch_ref[...] = jnp.zeros_like(branch_ref)
        gn_ref[...] = jnp.zeros_like(gn_ref)

    for j in range(4):

        @pl.when(t == PER * j)
        def _():
            for copy in loads(j):
                copy.wait()

    spot = jnp.bitwise_xor(me_mp, jr) if fast else jr
    cols = pl.ds(pl.multiple_of(sub * SUB, SUB), SUB)
    w1 = w[jr, 0, :, cols]
    w2 = w[jr, 1, :, cols]
    u = dotf(n_ref[...], w1) + b_ref[spot, :, cols]
    cdf = 0.5 * (1.0 + lax.erf(u * 0.7071067811865476))
    hidden = (u * cdf).astype(B16)
    slope = cdf + u * (0.3989422804014327 * jnp.exp(-0.5 * u * u))
    gb = (dotf(c_ref[...], w2) * slope).astype(B16)
    db_ref[spot, :, cols] = jnp.sum(gb.astype(F32), axis=0, keepdims=True)
    branch_ref[...] += dotf(hidden, w2, NT)
    gn_ref[...] += dotf(gb, w1, NT)
    dw1 = dotf(nt[...], gb).astype(B16)
    dw2 = dotf(ct[...], hidden).astype(B16)
    for a in range(8):
        dr = jnp.bitwise_xor(me_dp, a) if fast else a
        dw[jr, dr, 0, :, cols] = dw1[96 * a : 96 * a + 96]
        dw[jr, dr, 1, :, cols] = dw2[96 * a : 96 * a + 96]

    for j in range(4):

        @pl.when(t == PER * j + PER - 1)
        def _():
            for copy in stores(j):
                copy.start()

    @pl.when(t == 4 * PER - 1)
    def _():
        for j in range(4):
            for copy in stores(j):
                copy.wait()


def mlp(meta, normed, cot, bias, pieces):
    fast = len(pieces) == 16
    tokens = normed.shape[0]
    vmem = pl.BlockSpec(memory_space=pltpu.VMEM)
    anys = pl.BlockSpec(memory_space=pl.ANY)
    shape = jax.ShapeDtypeStruct((2, 4, 4, 96, 768) if fast else (4, 8, 2, 96, 768), B16)
    return pl.pallas_call(
        partial(mlp_kernel, fast),
        name="mlp",
        grid=(4 * PER,),
        in_specs=[pl.BlockSpec(memory_space=pltpu.SMEM), vmem, vmem, vmem] + [anys] * len(pieces),
        out_specs=[vmem, vmem, vmem, anys, anys],
        out_shape=(
            jax.ShapeDtypeStruct((tokens, 768), F32),
            jax.ShapeDtypeStruct((tokens, 768), F32),
            jax.ShapeDtypeStruct((4, 1, 768), F32),
            shape,
            shape,
        ),
        scratch_shapes=[
            pltpu.VMEM((4, 2, 768, 768), B16),
            pltpu.VMEM((768, tokens), B16),
            pltpu.VMEM((768, tokens), B16),
            pltpu.VMEM((4, 8, 2, 96, 768), B16),
            pltpu.SemaphoreType.DMA((4, 8, 2)),
            pltpu.SemaphoreType.DMA((4, 8, 2)),
        ],
        compiler_params=pltpu.CompilerParams(vmem_limit_bytes=VMEM_LIMIT),
    )(meta, normed, cot, bias.reshape(4, 1, 768), *pieces)


def local(
    fast,
    tokens,
    cotangent,
    prompts,
    segments,
    prompt_slot_index,
    norm_gain,
    norm_shift,
    attn_qkv,
    attn_bias,
    attn_out,
    mlp_weight,
    mlp_bias_up,
    mlp_bias_down,
):
    width = tokens.shape[1]
    device = lax.axis_index("dp") * lax.axis_size("mp") + lax.axis_index("mp")
    meta = jnp.reshape(device, (1,)).astype(jnp.int32)
    core = device % 2
    if fast:
        piece = pair_rows(meta, attn_qkv, attn_out)
        held = z_stage(piece)
        held, mlp_piece, tokens, prompts, segments, prompt_slot_index = tie(
            held, mlp_weight, tokens, prompts, segments, prompt_slot_index
        )
    table = jnp.concatenate([prompts, jnp.zeros((128 - NPROMPT, width), F32)], 0)
    start, normed_one, onehot, qf, kf = embed(
        tokens, prompt_slot_index, segments, table, jnp.stack([norm_gain[0], norm_shift[0]])
    )
    bias = jnp.stack([attn_bias[0], jnp.zeros_like(attn_bias[0]), attn_bias[1]])[:, None]
    out_params = jnp.stack([attn_bias[2], norm_gain[1], norm_shift[1]])

    if fast:
        x = (normed_one, start, qf, kf, onehot)
        mlp_z = [mlp_piece] + [px(mlp_piece, 8 * k) for k in range(1, 4)]
        quad, mlp_z, x = tie(xy_stage(held), mlp_z, x)
        normed_one, start, qf, kf, onehot = x
        own = assemble(meta, quad, "assemble")
        s1, s2 = stack_pair(mlp_z)
        own, s1, s2 = tie(own, s1, s2)
        other, y1, x2 = px(own, 1), px(s1, 4), px(s2, 2)
        s_other = [px(s1, 1), px(s2, 1)]
        qkv = project(meta, normed_one, own, bias, 0, ())
        other, qkv = tie(other, qkv)
    else:
        qkv_all = lax.all_gather(attn_qkv, AXES, axis=1, tiled=True)
        out_all = lax.all_gather(attn_out, AXES, axis=0, tiled=True)
        mlp_all = lax.all_gather(mlp_weight, "dp", axis=1, tiled=True)
        mlp_all = lax.all_gather(mlp_all, "mp", axis=2, tiled=True)
        four_all = jnp.concatenate([qkv_all, out_all[None]])
        own = lax.dynamic_slice_in_dim(four_all, 384 * core, 384, 2)
        other = lax.dynamic_slice_in_dim(four_all, 384 * (1 - core), 384, 2)
        qkv = project(meta, normed_one, own, bias, 0, ())
    qkv = project(meta, normed_one, other, bias, 1, (qkv,))
    if fast:
        y1, x2, s_other, qkv = tie(y1, x2, s_other, qkv)
        x1, xy1, y2, xy2 = px(s1, 2), px(y1, 2), px(s2, 4), px(x2, 4)
    mixed, lse = attention_forward(meta, qf, kf, qkv)
    if fast:
        x1, xy1, y2, xy2, mixed = tie(x1, xy1, y2, xy2, mixed)
        one = [px(v, 1) for v in (x1, y1, xy1)]
        two = [px(v, 1) for v in (x2, y2, xy2)]
        mlp_pieces = [s1, x1, y1, xy1, s2, x2, y2, xy2, s_other[0], *one, s_other[1], *two]
    else:
        mlp_pieces = [mlp_all]
    middle, normed_two, out_weight = out_projection(meta, mixed, start, own, other, out_params)
    branch, grad_two, grad_up, own_mlp, other_mlp = mlp(meta, normed_two, cotangent, mlp_bias_up, mlp_pieces)
    if fast:
        other_mlp, grad_two, branch = tie(other_mlp, grad_two, branch)
        got_mlp = px(other_mlp, 1)
    turn_params = jnp.stack([norm_gain[1], mlp_bias_down])
    output, grad_middle, grad_mixed, own_out, other_out, sums_two = turn(
        meta, middle, branch, grad_two, cotangent, mixed, out_weight, turn_params
    )
    if fast:
        got_mlp, grad_mixed, other_out = tie(got_mlp, grad_mixed, other_out)
        send = [add_parts(own_mlp[c, 2:], got_mlp[c, 2:]).astype(B16) for c in range(2)]
        send, grad_mixed, other_out = tie(send, grad_mixed, other_out)
        got_1, got_2, got_out = px(send[0], 2), px(send[1], 4), px(other_out, 1)
    grads = attention_backward(meta, qf, kf, qkv, grad_mixed, mixed, lse)
    if fast:
        got_1, got_2, got_out, grads, grad_middle = tie(got_1, got_2, got_out, grads, grad_middle)
        plane = [
            add_parts(own_mlp[c, :2], got_mlp[c, :2]) + got.astype(F32) for c, got in enumerate((got_1, got_2))
        ]
        send, grads = tie([p[1].astype(B16) for p in plane], grads)
        got_1, got_2 = px(send[0], 4), px(send[1], 2)
    input_grad, packed = tail_step(
        meta, start, grad_middle, onehot, norm_gain[0:1], sums_two, grad_up, (own, other), grads
    )
    if fast:
        packed, grads, got_1, got_2 = tie(packed, grads, got_1, got_2)
        got_small = px(packed, 1)
        own_w, other_w = weight_grad(meta, normed_one, grads, "weight_grad_qkv")
        got_small, other_w = tie(got_small, other_w)
        got_w = px(other_w, 1)
        packed = pack_small(add_small(packed, got_small))
        got_small = px(packed, 2)
        got_w, got_small, packed = tie(got_w, got_small, packed)
        packed = pack_small(add_small(packed, got_small))
        got_small = px(packed, 4)
        col = [add_parts(plane[0][0], got_1), add_parts(plane[1][0], got_2)]
        send = jnp.stack([c[2:].astype(B16) for c in col])
        keep, *sends = gather_sums(own_w, got_w, own_out, got_out)
        send, sends, got_small, packed = tie(send, sends, got_small, packed)
        got_far = px(send, 16)
        moved = [px(x, 2 * i + 2) for i, x in enumerate(sends)]
        packed = pack_small(add_small(packed, got_small))
        got_small = px(packed, 8)
        moved, got_far, got_small, packed = tie(moved, got_far, got_small, packed)
        col_attn, *last = plane_sums(keep, moved)
        near = [add_parts(col[c][:2], got_far[c]) for c in range(2)]
        send = jnp.stack([x[1].astype(B16) for x in near])
        last, send = tie(last, send)
        last = [px(x, 8 * i + 8) for i, x in enumerate(last)]
        got_near = px(send, 8)
        small = exchange_small(pack_small(add_small(packed, got_small)), 16)
        mlp_grad = jnp.stack([x[0] for x in near]) + got_near.astype(F32)
        qkv_grad, out_grad = line_sums(col_attn, last)
    else:
        mlp_grad = own_mlp.transpose(2, 1, 3, 0, 4)
        mlp_grad = mlp_grad.reshape(2, 768, 3072)
        mlp_grad = lax.psum_scatter(mlp_grad, "dp", scatter_dimension=1, tiled=True)
        mlp_grad = lax.psum_scatter(mlp_grad, "mp", scatter_dimension=2, tiled=True).astype(F32)
        grad_out_weight = dotf(mixed, grad_middle.astype(B16), TN)
        grad_qkv = jnp.stack([dotf(normed_one, g, TN) for g in grads])
        qkv_grad = lax.psum_scatter(grad_qkv, AXES, scatter_dimension=1, tiled=True)
        out_grad = lax.psum_scatter(grad_out_weight, AXES, scatter_dimension=0, tiled=True)
        x = packed.astype(F32)
        small = lax.psum(jnp.concatenate([x[:64], x[64:80] + x[80:]]), AXES)
    return (
        output,
        input_grad,
        small[:NPROMPT],
        small[64:66],
        small[66:68],
        qkv_grad,
        small[68:71],
        out_grad,
        mlp_grad,
        small[72:76].reshape(-1),
        small[71],
    )


def solution(mesh):
    fast = dict(mesh.shape) == {"dp": 8, "mp": 4}
    return jax.shard_map(
        partial(local, fast),
        mesh=mesh,
        in_specs=(
            P(AXES, None),
            P(AXES, None),
            P(),
            P(AXES),
            P(AXES),
            P(),
            P(),
            P(None, AXES, None),
            P(),
            P(AXES, None),
            P(None, "dp", "mp"),
            P(),
            P(),
        ),
        out_specs=(
            P(AXES, None),
            P(AXES, None),
            P(),
            P(),
            P(),
            P(None, AXES, None),
            P(),
            P(AXES, None),
            P(None, "dp", "mp"),
            P(),
            P(),
        ),
        check_vma=False,
    )
```

```python
from functools import partial

import jax
import jax.numpy as jnp
from jax import lax
from jax.experimental import pallas as pl
from jax.experimental.pallas import tpu as pltpu
from jax.sharding import PartitionSpec as P

NPROMPT = 50
ROW = 1024
SPANS = (151, 247, 627)
EPS = 1e-06
HIGHEST = lax.Precision.HIGHEST
BIG = 1e30
B16 = jnp.bfloat16
F32 = jnp.float32
AXES = ("dp", "mp")
TILE = 256
STEP = 512
QROWS = 512
NT = (((1,), (1,)), ((), ()))
TN = (((0,), (0,)), ((), ()))
VMEM_LIMIT = 60 * 1024 * 1024


def layer_norm(value_list, gain_row, shift_row):
    centre = jnp.mean(value_list, axis=-1, keepdims=True)
    centred = value_list - centre
    spread = jnp.mean(centred * centred, axis=-1, keepdims=True)
    return centred * lax.rsqrt(spread + EPS) * gain_row + shift_row


def key_window(first, count):
    low, high = ROW, 0
    for span in SPANS:
        whole = ROW // span
        for row in (first, first + count - 1):
            seg = min(row // span, whole)
            low = min(low, seg * span)
            high = max(high, ROW if seg == whole else (seg + 1) * span)
    return low // 128 * 128, -(-high // 128) * 128


def dotf(a, b, dims=None):
    if dims is None:
        return jnp.dot(a, b, preferred_element_type=F32)
    return lax.dot_general(a, b, dims, preferred_element_type=F32)


def px(x, k):
    return lax.ppermute(x, AXES, [(i, i ^ k) for i in range(32)])


def tie(*trees):
    return lax.optimization_barrier(trees)


def stack_kernel(*refs):
    for i, ref in enumerate(refs[:-1]):
        refs[-1][i] = ref[...]


def stack(parts, name):
    vmem = pl.BlockSpec(memory_space=pltpu.VMEM)
    return pl.pallas_call(
        stack_kernel,
        name=name,
        out_shape=jax.ShapeDtypeStruct((len(parts),) + parts[0].shape, parts[0].dtype),
        in_specs=[vmem] * len(parts),
        out_specs=vmem,
    )(*parts)


def z_stage(piece):
    return stack([piece] + [px(piece, 8 * k) for k in range(1, 4)], "stack_z")


def stack_pair_kernel(*refs):
    for i, ref in enumerate(refs[:-2]):
        for c in range(2):
            refs[c - 2][i] = ref[c]


def stack_pair(parts):
    vmem = pl.BlockSpec(memory_space=pltpu.VMEM)
    shape = jax.ShapeDtypeStruct((len(parts),) + parts[0].shape[1:], parts[0].dtype)
    return pl.pallas_call(
        stack_pair_kernel,
        name="stack_pair",
        out_shape=(shape, shape),
        in_specs=[vmem] * len(parts),
        out_specs=(vmem, vmem),
    )(*parts)


def xy_stage(parts):
    return [parts] + [px(parts, 2 * k) for k in range(1, 4)]


def split_kernel(meta, qkv_ref, out_ref, mine_ref, theirs_ref):
    core = meta[0] % 2
    for ref, half in ((mine_ref, core), (theirs_ref, 1 - core)):
        cols = pl.ds(pl.multiple_of(384 * half, 128), 384)
        ref[0:3] = qkv_ref[:, :, cols]
        ref[3] = out_ref[:, cols]


def join_kernel(meta, mine_ref, got_ref, out_ref):
    for core in range(2):

        @pl.when(meta[0] % 2 == core)
        def _():
            out_ref[...] = jnp.concatenate([mine_ref[...], got_ref[...]][:: 1 - 2 * core], 1)


def pair_rows(meta, qkv, out):
    vmem = pl.BlockSpec(memory_space=pltpu.VMEM)
    smem = pl.BlockSpec(memory_space=pltpu.SMEM)
    half = jax.ShapeDtypeStruct((4, 24, 384), B16)
    mine, theirs = pl.pallas_call(
        split_kernel, name="split", out_shape=(half, half), in_specs=[smem, vmem, vmem], out_specs=(vmem, vmem)
    )(meta, qkv, out)
    return pl.pallas_call(
        join_kernel,
        name="join",
        out_shape=jax.ShapeDtypeStruct((4, 48, 384), B16),
        in_specs=[smem, vmem, vmem],
        out_specs=vmem,
    )(meta, mine, px(theirs, 1))


def assemble_kernel(meta, *refs):
    pieces, out, sems = refs[:4], refs[4], refs[5]
    copies = []
    for xy in range(4):
        for z in range(4):
            rows = pl.multiple_of(48 * jnp.bitwise_xor(meta[0] // 2, xy + 4 * z), 16)
            copies.append(
                pltpu.make_async_copy(pieces[xy].at[z], out.at[:, pl.ds(rows, 48), :], sems.at[4 * xy + z])
            )
    for copy in copies:
        copy.start()
    for copy in copies:
        copy.wait()


def assemble(meta, pieces, name):
    return pl.pallas_call(
        assemble_kernel,
        name=name,
        out_shape=jax.ShapeDtypeStruct((4, 768, 384), B16),
        in_specs=[pl.BlockSpec(memory_space=pltpu.SMEM)] + [pl.BlockSpec(memory_space=pl.ANY)] * 4,
        out_specs=pl.BlockSpec(memory_space=pltpu.VMEM),
        scratch_shapes=[pltpu.SemaphoreType.DMA((16,))],
    )(meta, *pieces)


def project_kernel(side, meta, x_ref, w_ref, b_ref, *refs):
    half = jnp.bitwise_xor(meta[0] % 2, side)
    cols = pl.ds(pl.multiple_of(384 * half, 128), 384)
    y = dotf(x_ref[...], w_ref[0]) + b_ref[pl.program_id(0), :, cols]
    refs[-1][...] = y.astype(B16)


def project(meta, x, weight, bias, side, held):
    rows = x.shape[0]
    vmem = pl.BlockSpec(memory_space=pltpu.VMEM)
    return pl.pallas_call(
        partial(project_kernel, side),
        name="project",
        grid=(3,),
        out_shape=jax.ShapeDtypeStruct((rows, 2304), B16),
        in_specs=[
            pl.BlockSpec(memory_space=pltpu.SMEM),
            vmem,
            pl.BlockSpec((1, 768, 384), lambda c: (c, 0, 0)),
            vmem,
        ]
        + [pl.BlockSpec(memory_space=pl.ANY)] * len(held),
        out_specs=pl.BlockSpec((rows, 384), lambda c: (0, 3 * side + c)),
        input_output_aliases={4 + i: i for i in range(len(held))},
        compiler_params=pltpu.CompilerParams(vmem_limit_bytes=VMEM_LIMIT),
    )(meta, x, weight, bias, *held)


def embed_kernel(tokens_ref, slots_ref, segs_ref, table_ref, p_ref, start_ref, normed_ref, hot_ref, qf_ref, kf_ref):
    lane = lax.broadcasted_iota(jnp.int32, (TILE, 128), 1)
    slots, segs = slots_ref[...], segs_ref[...]
    is_prompt = slots < NPROMPT
    hot = jnp.where((lane == slots) & is_prompt, 1.0, 0.0).astype(B16)
    hot_ref[...] = hot
    rows = None
    for part in three_parts(table_ref[...]):
        term = dotf(hot, part.astype(B16))
        rows = term if rows is None else rows + term
    start = jnp.where(is_prompt, rows, tokens_ref[...].astype(F32))
    start_ref[...] = start
    normed_ref[...] = (centred(start)[0] * p_ref[0:1] + p_ref[1:2]).astype(B16)
    spot = lane % 64
    same = (spot == segs) & (spot < 7)
    qf_ref[...] = jnp.where(same, 1.0, 0.0).astype(B16)
    kf = jnp.where(spot < 7, jnp.where(same, 0.0, -BIG), jnp.where(spot < 10, 1.0, 0.0))
    kf_ref[...] = kf.astype(B16)


def embed(tokens, slots, segs, table, params):
    rows = tokens.shape[0]

    def block(width):
        return pl.BlockSpec((TILE, width), lambda i: (i, 0))

    vmem = pl.BlockSpec(memory_space=pltpu.VMEM)
    lanes = jax.ShapeDtypeStruct((rows, 128), B16)
    return pl.pallas_call(
        embed_kernel,
        name="embed",
        grid=(rows // TILE,),
        in_specs=[block(768), block(1), block(1), vmem, vmem],
        out_specs=[block(768), block(768), block(128), block(128), block(128)],
        out_shape=(
            jax.ShapeDtypeStruct((rows, 768), F32),
            jax.ShapeDtypeStruct((rows, 768), B16),
            lanes,
            lanes,
            lanes,
        ),
    )(tokens, slots[:, None], segs[:, None], table, params)


def gather_sums_kernel(own_ref, got_ref, own_out_ref, got_out_ref, keep_ref, *sends):
    for k in range(4):
        for z in range(4):
            for m in range(4):
                if m < 3:
                    x = add_parts(own_ref[k, z, m], got_ref[k, z, m])
                else:
                    x = add_parts(own_out_ref[k, z, 0], got_out_ref[k, z, 0])
                if k:
                    sends[k - 1][z, m] = x.astype(B16)
                else:
                    keep_ref[z, m] = x


def gather_sums(own, got, own_out, got_out):
    vmem = pl.BlockSpec(memory_space=pltpu.VMEM)
    send = jax.ShapeDtypeStruct((4, 4, 24, 768), B16)
    return pl.pallas_call(
        gather_sums_kernel,
        name="gather_sums",
        in_specs=[vmem] * 4,
        out_specs=[vmem] * 4,
        out_shape=(jax.ShapeDtypeStruct((4, 4, 24, 768), F32), send, send, send),
        compiler_params=pltpu.CompilerParams(vmem_limit_bytes=VMEM_LIMIT),
    )(own, got, own_out, got_out)


def four(values):
    return (values[0] + values[1]) + (values[2] + values[3])


def plane_sums_kernel(keep_ref, *refs):
    moved, (col_ref, *sends) = refs[:3], refs[3:]
    for z in range(4):
        for m in range(4):
            x = four([keep_ref[z, m]] + [ref[z, m].astype(F32) for ref in moved])
            if z:
                sends[z - 1][m] = x.astype(B16)
            else:
                col_ref[m] = x


def plane_sums(keep, moved):
    vmem = pl.BlockSpec(memory_space=pltpu.VMEM)
    send = jax.ShapeDtypeStruct((4, 24, 768), B16)
    return pl.pallas_call(
        plane_sums_kernel,
        name="plane_sums",
        in_specs=[vmem] * 4,
        out_specs=[vmem] * 4,
        out_shape=(jax.ShapeDtypeStruct((4, 24, 768), F32), send, send, send),
        compiler_params=pltpu.CompilerParams(vmem_limit_bytes=VMEM_LIMIT),
    )(keep, *moved)


def line_sums_kernel(col_ref, *refs):
    last, (qkv_ref, out_ref) = refs[:3], refs[3:]
    for m in range(4):
        x = four([col_ref[m]] + [ref[m].astype(F32) for ref in last])
        if m < 3:
            qkv_ref[m] = x
        else:
            out_ref[...] = x


def line_sums(col, last):
    vmem = pl.BlockSpec(memory_space=pltpu.VMEM)
    return pl.pallas_call(
        line_sums_kernel,
        name="line_sums",
        in_specs=[vmem] * 4,
        out_specs=[vmem] * 2,
        out_shape=(jax.ShapeDtypeStruct((3, 24, 768), F32), jax.ShapeDtypeStruct((24, 768), F32)),
    )(col, *last)


def centred(x):
    mean = jnp.mean(x, axis=-1, keepdims=True)
    x = x - mean
    rate = lax.rsqrt(jnp.mean(x * x, axis=-1, keepdims=True) + EPS)
    return x * rate, rate


def out_kernel(meta, x_ref, start_ref, own_ref, other_ref, p_ref, middle_ref, normed_ref, w_ref):
    core = meta[0] % 2

    @pl.when(pl.program_id(0) == 0)
    def _():
        for ref, half in ((own_ref, core), (other_ref, 1 - core)):
            w_ref[:, pl.ds(pl.multiple_of(384 * half, 128), 384)] = ref[0]

    middle = start_ref[...] + dotf(x_ref[...], w_ref[...]) + p_ref[0:1]
    middle_ref[...] = middle
    normed_ref[...] = (centred(middle)[0] * p_ref[1:2] + p_ref[2:3]).astype(B16)


def out_projection(meta, mixed, start, own, other, params):
    rows = mixed.shape[0]
    block = pl.BlockSpec((STEP, 768), lambda i: (i, 0))
    vmem = pl.BlockSpec(memory_space=pltpu.VMEM)
    return pl.pallas_call(
        out_kernel,
        name="out_projection",
        grid=(rows // STEP,),
        in_specs=[pl.BlockSpec(memory_space=pltpu.SMEM), block, block]
        + [pl.BlockSpec((1, 768, 384), lambda i: (3, 0, 0))] * 2
        + [vmem],
        out_specs=[block, block, vmem],
        out_shape=(
            jax.ShapeDtypeStruct((rows, 768), F32),
            jax.ShapeDtypeStruct((rows, 768), B16),
            jax.ShapeDtypeStruct((768, 768), B16),
        ),
        compiler_params=pltpu.CompilerParams(vmem_limit_bytes=VMEM_LIMIT),
    )(meta, mixed, start, own, other, params)


def norm_backward(normal, rate, grad, gain):
    u = grad * gain
    return rate * (u - jnp.mean(u, axis=-1, keepdims=True) - normal * jnp.mean(u * normal, axis=-1, keepdims=True))


def row_sum(x):
    return jnp.sum(x, axis=0, keepdims=True)


def put_parts(meta, acc, own_ref, other_ref, m):
    chip, core = meta[0] // 2, meta[0] % 2
    for z in range(4):
        for xy in range(4):
            row = 48 * jnp.bitwise_xor(chip, xy + 4 * z)
            own_ref[xy, z, m] = acc[pl.ds(pl.multiple_of(row + 24 * core, 8), 24), :].astype(B16)
            other_ref[xy, z, m] = acc[pl.ds(pl.multiple_of(row + 24 * (1 - core), 8), 24), :].astype(B16)


def turn_kernel(
    meta, middle_ref, branch_ref, grad_ref, cot_ref, mixed_ref, w_ref, p_ref,
    output_ref, gmiddle_ref, gmixed_ref, own_ref, other_ref, sums_ref, acc,
):
    i = pl.program_id(0)

    @pl.when(i == 0)
    def _():
        sums_ref[...] = jnp.zeros_like(sums_ref)
        acc[...] = jnp.zeros_like(acc)

    middle, grad = middle_ref[...], grad_ref[...]
    cot = cot_ref[...].astype(F32)
    output_ref[...] = (middle + branch_ref[...] + p_ref[1:2]).astype(B16)
    normal, rate = centred(middle)
    gmiddle = cot + norm_backward(normal, rate, grad, p_ref[0:1])
    gmiddle_ref[...] = gmiddle
    low = gmiddle.astype(B16)
    for row, x in enumerate((normal * grad, grad, low.astype(F32), cot)):
        sums_ref[row : row + 1, :] += row_sum(x)
    gmixed_ref[...] = dotf(low, w_ref[...], NT).astype(B16)
    acc[...] += dotf(mixed_ref[...], low, TN)

    @pl.when(i == pl.num_programs(0) - 1)
    def _():
        put_parts(meta, acc, own_ref, other_ref, 0)


def turn(meta, middle, branch, grad, cot, mixed, weight, params):
    rows = middle.shape[0]
    block = pl.BlockSpec((STEP, 768), lambda i: (i, 0))
    vmem = pl.BlockSpec(memory_space=pltpu.VMEM)
    parts = jax.ShapeDtypeStruct((4, 4, 1, 24, 768), B16)
    return pl.pallas_call(
        turn_kernel,
        name="turn",
        grid=(rows // STEP,),
        in_specs=[pl.BlockSpec(memory_space=pltpu.SMEM)] + [block] * 5 + [vmem, vmem],
        out_specs=[block, block, block, vmem, vmem, vmem],
        out_shape=(
            jax.ShapeDtypeStruct((rows, 768), B16),
            jax.ShapeDtypeStruct((rows, 768), F32),
            jax.ShapeDtypeStruct((rows, 768), B16),
            parts,
            parts,
            jax.ShapeDtypeStruct((8, 768), F32),
        ),
        scratch_shapes=[pltpu.VMEM((768, 768), F32)],
        compiler_params=pltpu.CompilerParams(vmem_limit_bytes=VMEM_LIMIT),
    )(meta, middle, branch, grad, cot, mixed, weight, params)


def tail_kernel(meta, start_ref, gmiddle_ref, slots_ref, p_ref, turn_ref, up_ref, *refs):
    weights, grads = refs[:2], refs[2:5]
    input_ref, packed_ref, prompt_ref, sums_ref = refs[5:]
    core = meta[0] % 2

    @pl.when(pl.program_id(0) == 0)
    def _():
        prompt_ref[...] = jnp.zeros_like(prompt_ref)
        sums_ref[...] = jnp.zeros_like(sums_ref)

    total = None
    for c in range(3):
        for side in range(2):
            half = jnp.bitwise_xor(core, side)
            left = grads[c][:, pl.ds(pl.multiple_of(384 * half, 128), 384)]
            term = dotf(left, weights[side][c], NT)
            total = term if total is None else total + term
    normal, rate = centred(start_ref[...])
    rows = ((0, normal * total), (2, total), (4, grads[0][...].astype(F32)), (5, grads[2][...].astype(F32)))
    for row, x in rows:
        sums_ref[row : row + 1, :] += row_sum(x)
    gstart = gmiddle_ref[...] + norm_backward(normal, rate, total, p_ref[0:1])
    slots = slots_ref[...]
    is_prompt = jnp.sum(slots.astype(F32), axis=-1, keepdims=True) > 0.5
    input_ref[...] = jnp.where(is_prompt, 0.0, gstart)
    for part in three_parts(gstart):
        prompt_ref[...] += dotf(slots, part.astype(B16), TN)

    @pl.when(pl.program_id(0) == pl.num_programs(0) - 1)
    def _():
        for row, source in ((1, 0), (3, 1), (6, 2), (7, 3)):
            sums_ref[row : row + 1, :] = turn_ref[source : source + 1, :]
        for row in range(4):
            sums_ref[8 + row : 9 + row, :] = up_ref[row]
        packed_ref[0:64, :] = prompt_ref[0:64, :].astype(B16)
        high, low = split_rows(sums_ref[...])
        packed_ref[64:80, :] = high
        packed_ref[80:96, :] = low


def tail_step(meta, start, gmiddle, slots, params, sums_two, up, weights, grads):
    rows = start.shape[0]

    def block(width):
        return pl.BlockSpec((STEP, width), lambda i: (i, 0))

    vmem = pl.BlockSpec(memory_space=pltpu.VMEM)
    return pl.pallas_call(
        tail_kernel,
        name="tail_step",
        grid=(rows // STEP,),
        in_specs=[pl.BlockSpec(memory_space=pltpu.SMEM), block(768), block(768), block(128)]
        + [vmem] * 3
        + [pl.BlockSpec((3, 768, 384), lambda i: (0, 0, 0))] * 2
        + [block(768)] * 3,
        out_specs=[block(768), vmem],
        out_shape=(
            jax.ShapeDtypeStruct((rows, 768), F32),
            jax.ShapeDtypeStruct((96, 768), B16),
        ),
        scratch_shapes=[pltpu.VMEM((128, 768), F32), pltpu.VMEM((16, 768), F32)],
        compiler_params=pltpu.CompilerParams(vmem_limit_bytes=VMEM_LIMIT),
    )(meta, start, gmiddle, slots, params, sums_two, up, *weights, *grads)


def weight_grad_kernel(count, meta, left_ref, *refs):
    rights, own_ref, other_ref, acc = refs[:count], refs[count], refs[count + 1], refs[count + 2]
    for m in range(count):
        acc[...] = dotf(left_ref[...], rights[m][...], TN)
        put_parts(meta, acc, own_ref, other_ref, m)


def weight_grad(meta, left, rights, name):
    count, width = len(rights), rights[0].shape[1]
    shape = jax.ShapeDtypeStruct((4, 4, count, 24, width), B16)
    vmem = pl.BlockSpec(memory_space=pltpu.VMEM)
    return pl.pallas_call(
        partial(weight_grad_kernel, count),
        name=name,
        out_shape=(shape, shape),
        in_specs=[pl.BlockSpec(memory_space=pltpu.SMEM)] + [vmem] * (count + 1),
        out_specs=(vmem, vmem),
        scratch_shapes=[pltpu.VMEM((left.shape[1], width), F32)],
        compiler_params=pltpu.CompilerParams(vmem_limit_bytes=VMEM_LIMIT),
    )(meta, left, *rights)


def split_rows(rest):
    high = rest.astype(B16)
    return high, (rest - high.astype(F32)).astype(B16)


def add_small(x, y):
    x, y = x.astype(F32), y.astype(F32)
    return jnp.concatenate([x[:64] + y[:64], (x[64:80] + x[80:]) + (y[64:80] + y[80:])])


def pack_small(x):
    return jnp.concatenate([x[:64].astype(B16), *split_rows(x[64:])])


def exchange_small(x, k):
    return add_small(x, px(x, k))


def add_parts(own, got):
    return own.astype(F32) + got.astype(F32)


def three_parts(x):
    high = x.astype(B16).astype(F32)
    mid = (x - high).astype(B16).astype(F32)
    return high, mid, (x - high) - mid


def attention_forward_kernel(qf_ref, kf_ref, q_ref, k_ref, v_ref, mixed_ref, lse_ref):
    half = lax.broadcasted_iota(jnp.int32, (1, 128), 1) < 64
    q = q_ref[...] * jnp.asarray(0.125, B16)
    k, v = k_ref[...], v_ref[...]
    qf, kf = qf_ref[...], kf_ref[...]
    one = jnp.ones((), B16)
    sides = []
    for e in range(2):
        own = half if e == 0 else ~half
        sides.append((jnp.where(own, q, qf), jnp.where(own, k, kf), jnp.where(own, v, one)))
    for first in range(0, ROW, QROWS):
        low, high = key_window(first, QROWS)
        outs, peaks = [], []
        for qe, ke, ve in sides:
            s = dotf(qe[first : first + QROWS], ke[low:high], NT)
            peak = jnp.max(s, axis=-1, keepdims=True)
            p = jnp.exp(s - peak).astype(B16)
            outs.append(dotf(p, ve[low:high]))
            peaks.append(peak)
        data = jnp.where(half, outs[0], outs[1])
        total = pltpu.roll(jnp.where(half, outs[1], outs[0]), 64, 1)
        mixed_ref[first : first + QROWS, :] = (data / total).astype(B16)
        lse_ref[first : first + QROWS, :] = jnp.where(half, peaks[0], peaks[1]) + jnp.log(total)


def pair_specs(rows):
    full = pl.BlockSpec((ROW, 128), lambda r, s, p, meta: (r, 0))
    blocks = [pl.BlockSpec((ROW, 128), lambda r, s, p, meta, c=c: (r, 9 * s + 3 * c + p)) for c in range(3)]
    whole = pl.BlockSpec((ROW, 128), lambda r, s, p, meta: (r, 3 * jnp.bitwise_xor(meta[0] % 2, s) + p))
    return (rows // ROW, 2, 3), full, blocks, whole


def attention_forward(meta, qf, kf, qkv):
    rows = qkv.shape[0]
    grid, full, blocks, whole = pair_specs(rows)

    def kernel(meta, *refs):
        attention_forward_kernel(*refs)

    return pl.pallas_call(
        kernel,
        name="attention_forward",
        grid_spec=pltpu.PrefetchScalarGridSpec(
            num_scalar_prefetch=1, grid=grid, in_specs=[full, full] + blocks, out_specs=[whole, whole]
        ),
        out_shape=(
            jax.ShapeDtypeStruct((rows, 768), B16),
            jax.ShapeDtypeStruct((rows, 768), F32),
        ),
        compiler_params=pltpu.CompilerParams(vmem_limit_bytes=VMEM_LIMIT),
    )(meta, qf, kf, qkv, qkv, qkv)


def attention_backward_kernel(
    qf_ref, kf_ref, q_ref, k_ref, v_ref, g_ref, mixed_ref, lse_ref, dq_ref, dk_ref, dv_ref, dk_acc, dv_acc
):
    lane = lax.broadcasted_iota(jnp.int32, (1, 128), 1)
    half = lane < 64
    spot = lane % 64
    q = q_ref[...] * jnp.asarray(0.125, B16)
    k, v, g = k_ref[...], v_ref[...], g_ref[...]
    qf, kf = qf_ref[...].astype(F32), kf_ref[...]
    prod = g.astype(F32) * mixed_ref[...].astype(F32)
    d0 = jnp.sum(jnp.where(half, prod, 0.0), axis=-1, keepdims=True)
    d1 = jnp.sum(jnp.where(half, 0.0, prod), axis=-1, keepdims=True)
    delta = jnp.where(half, d1, d0)
    lse = pltpu.roll(lse_ref[...], 64, 1)

    def spread(base, x):
        a, b, c = three_parts(-x)
        return jnp.where(spot == 7, a, jnp.where(spot == 8, b, jnp.where(spot == 9, c, base))).astype(B16)

    q_extra = spread(qf, lse)
    g_extra = spread(jnp.zeros_like(qf), delta)
    v_extra = jnp.where((spot >= 7) & (spot <= 9), 1.0, 0.0).astype(B16)
    dk_acc[...] = jnp.zeros_like(dk_acc)
    dv_acc[...] = jnp.zeros_like(dv_acc)
    sides = []
    for e in range(2):
        own = half if e == 0 else ~half
        sides.append(
            (
                jnp.where(own, q, q_extra),
                jnp.where(own, k, kf),
                jnp.where(own, g, g_extra),
                jnp.where(own, v, v_extra),
            )
        )
    for first in range(0, ROW, TILE):
        low, high = key_window(first, TILE)
        dqs, dks, dvs = [], [], []
        for qe, ke, ge, ve in sides:
            s = dotf(qe[first : first + TILE], ke[low:high], NT)
            p = jnp.exp(s)
            d = dotf(ge[first : first + TILE], ve[low:high], NT)
            ds = (p * d).astype(B16)
            dqs.append(dotf(ds, k[low:high]))
            dks.append(dotf(ds, q[first : first + TILE], TN))
            dvs.append(dotf(p.astype(B16), g[first : first + TILE], TN))
        dq_ref[first : first + TILE, :] = (jnp.where(half, dqs[0], dqs[1]) * 0.125).astype(B16)
        dk_acc[low:high, :] += jnp.where(half, dks[0], dks[1])
        dv_acc[low:high, :] += jnp.where(half, dvs[0], dvs[1])
    dk_ref[...] = dk_acc[...].astype(B16)
    dv_ref[...] = dv_acc[...].astype(B16)


def attention_backward(meta, qf, kf, qkv, grad, mixed, lse):
    rows = qkv.shape[0]
    grid, full, blocks, whole = pair_specs(rows)
    shape = jax.ShapeDtypeStruct((rows, 768), B16)

    def kernel(meta, *refs):
        attention_backward_kernel(*refs)

    return pl.pallas_call(
        kernel,
        name="attention_backward",
        grid_spec=pltpu.PrefetchScalarGridSpec(
            num_scalar_prefetch=1,
            grid=grid,
            in_specs=[full, full] + blocks + [whole] * 3,
            out_specs=[whole] * 3,
            scratch_shapes=[pltpu.VMEM((ROW, 128), F32), pltpu.VMEM((ROW, 128), F32)],
        ),
        out_shape=(shape, shape, shape),
        compiler_params=pltpu.CompilerParams(vmem_limit_bytes=VMEM_LIMIT),
    )(meta, qf, kf, qkv, qkv, qkv, grad, mixed, lse)


SUB = 256
PER = 768 // SUB


def mlp_kernel(fast, *refs):
    meta, n_ref, c_ref, ct, b_ref = refs[:5]
    count = 16 if fast else 1
    pieces, refs = refs[5 : 5 + count], refs[5 + count :]
    branch_ref, gn_ref, db_ref, own_ref, other_ref = refs[:5]
    w, nt, dw, wsem, dsem = refs[5:]
    t = pl.program_id(0)
    jr, sub = t // PER, t % PER
    me_mp, me_dp = meta[0] % 4, meta[0] // 4

    def loads(j):
        if not fast:
            source = pieces[0].at[:, :, pl.ds(768 * j, 768)]
            return [pltpu.make_async_copy(source, w.at[j], wsem.at[j, 0, 0])]
        out = []
        for dr in range(8):
            rows = pl.multiple_of(96 * jnp.bitwise_xor(me_dp, dr), 32)
            for c in range(2):
                source = pieces[8 * (j & 1) + 4 * c + (j >> 1) + 2 * (dr & 1)].at[dr >> 1]
                out.append(pltpu.make_async_copy(source, w.at[j, c, pl.ds(rows, 96), :], wsem.at[j, dr, c]))
        return out

    def stores(j):
        if not fast:
            return [pltpu.make_async_copy(dw.at[j], own_ref.at[j], dsem.at[j, 0, 0])]
        out = []
        for dr in range(8):
            x, y = j >> 1, dr & 1
            for c, spot in enumerate((2 * x + y, 2 * y + x)):
                target = (other_ref if j & 1 else own_ref).at[c, spot, dr >> 1]
                out.append(pltpu.make_async_copy(dw.at[j, dr, c], target, dsem.at[j, dr, c]))
        return out

    @pl.when(t == 0)
    def _():
        for j in range(4):
            for copy in loads(j):
                copy.start()
        nt[...] = n_ref[...].T
        branch_ref[...] = jnp.zeros_like(branch_ref)
        gn_ref[...] = jnp.zeros_like(gn_ref)

    for j in range(4):

        @pl.when(t == PER * j)
        def _():
            for copy in loads(j):
                copy.wait()

    spot = jnp.bitwise_xor(me_mp, jr) if fast else jr
    cols = pl.ds(pl.multiple_of(sub * SUB, SUB), SUB)
    w1 = w[jr, 0, :, cols]
    w2 = w[jr, 1, :, cols]
    u = dotf(n_ref[...], w1) + b_ref[spot, :, cols]
    cdf = 0.5 * (1.0 + lax.erf(u * 0.7071067811865476))
    hidden = (u * cdf).astype(B16)
    slope = cdf + u * (0.3989422804014327 * jnp.exp(-0.5 * u * u))
    gb = (dotf(c_ref[...], w2) * slope).astype(B16)
    db_ref[spot, :, cols] = jnp.sum(gb.astype(F32), axis=0, keepdims=True)
    branch_ref[...] += dotf(hidden, w2, NT)
    gn_ref[...] += dotf(gb, w1, NT)
    dw1 = dotf(nt[...], gb).astype(B16)
    dw2 = dotf(ct[...], hidden).astype(B16)
    for a in range(8):
        dr = jnp.bitwise_xor(me_dp, a) if fast else a
        dw[jr, dr, 0, :, cols] = dw1[96 * a : 96 * a + 96]
        dw[jr, dr, 1, :, cols] = dw2[96 * a : 96 * a + 96]

    for j in range(4):

        @pl.when(t == PER * j + PER - 1)
        def _():
            for copy in stores(j):
                copy.start()

    @pl.when(t == 4 * PER - 1)
    def _():
        for j in range(4):
            for copy in stores(j):
                copy.wait()


def mlp(meta, normed, cot, cot_turned, bias, pieces):
    fast = len(pieces) == 16
    tokens = normed.shape[0]
    vmem = pl.BlockSpec(memory_space=pltpu.VMEM)
    anys = pl.BlockSpec(memory_space=pl.ANY)
    shape = jax.ShapeDtypeStruct((2, 4, 4, 96, 768) if fast else (4, 8, 2, 96, 768), B16)
    return pl.pallas_call(
        partial(mlp_kernel, fast),
        name="mlp",
        grid=(4 * PER,),
        in_specs=[pl.BlockSpec(memory_space=pltpu.SMEM)] + [vmem] * 4 + [anys] * len(pieces),
        out_specs=[vmem, vmem, vmem, anys, anys],
        out_shape=(
            jax.ShapeDtypeStruct((tokens, 768), F32),
            jax.ShapeDtypeStruct((tokens, 768), F32),
            jax.ShapeDtypeStruct((4, 1, 768), F32),
            shape,
            shape,
        ),
        scratch_shapes=[
            pltpu.VMEM((4, 2, 768, 768), B16),
            pltpu.VMEM((768, tokens), B16),
            pltpu.VMEM((4, 8, 2, 96, 768), B16),
            pltpu.SemaphoreType.DMA((4, 8, 2)),
            pltpu.SemaphoreType.DMA((4, 8, 2)),
        ],
        compiler_params=pltpu.CompilerParams(vmem_limit_bytes=VMEM_LIMIT),
    )(meta, normed, cot, cot_turned, bias.reshape(4, 1, 768), *pieces)


def local(
    fast,
    tokens,
    cotangent,
    prompts,
    segments,
    prompt_slot_index,
    norm_gain,
    norm_shift,
    attn_qkv,
    attn_bias,
    attn_out,
    mlp_weight,
    mlp_bias_up,
    mlp_bias_down,
):
    width = tokens.shape[1]
    device = lax.axis_index("dp") * lax.axis_size("mp") + lax.axis_index("mp")
    meta = jnp.reshape(device, (1,)).astype(jnp.int32)
    core = device % 2
    if fast:
        piece = pair_rows(meta, attn_qkv, attn_out)
        held = z_stage(piece)
        held, mlp_near, mlp_piece, tokens, prompts, segments, prompt_slot_index = tie(
            held, px(mlp_weight, 8), mlp_weight, tokens, prompts, segments, prompt_slot_index
        )
    table = jnp.concatenate([prompts, jnp.zeros((128 - NPROMPT, width), F32)], 0)
    start, normed_one, onehot, qf, kf = embed(
        tokens, prompt_slot_index, segments, table, jnp.stack([norm_gain[0], norm_shift[0]])
    )
    bias = jnp.stack([attn_bias[0], jnp.zeros_like(attn_bias[0]), attn_bias[1]])[:, None]
    out_params = jnp.stack([attn_bias[2], norm_gain[1], norm_shift[1]])
    turn_params = jnp.stack([norm_gain[1], mlp_bias_down])
    cot_turned = cotangent.T

    if fast:
        x = (normed_one, start, qf, kf, onehot, bias, out_params, turn_params, cot_turned)
        mlp_z = [mlp_piece, mlp_near] + [px(mlp_piece, 8 * k) for k in range(2, 4)]
        quad, mlp_z, x = tie(xy_stage(held), mlp_z, x)
        normed_one, start, qf, kf, onehot, bias, out_params, turn_params, cot_turned = x
        own = assemble(meta, quad, "assemble")
        s1, s2 = stack_pair(mlp_z)
        own, s1, s2 = tie(own, s1, s2)
        other, y1, x2 = px(own, 1), px(s1, 4), px(s2, 2)
        s_other = [px(s1, 1), px(s2, 1)]
        qkv = project(meta, normed_one, own, bias, 0, ())
        other, qkv = tie(other, qkv)
    else:
        qkv_all = lax.all_gather(attn_qkv, AXES, axis=1, tiled=True)
        out_all = lax.all_gather(attn_out, AXES, axis=0, tiled=True)
        mlp_all = lax.all_gather(mlp_weight, "dp", axis=1, tiled=True)
        mlp_all = lax.all_gather(mlp_all, "mp", axis=2, tiled=True)
        four_all = jnp.concatenate([qkv_all, out_all[None]])
        own = lax.dynamic_slice_in_dim(four_all, 384 * core, 384, 2)
        other = lax.dynamic_slice_in_dim(four_all, 384 * (1 - core), 384, 2)
        qkv = project(meta, normed_one, own, bias, 0, ())
    qkv = project(meta, normed_one, other, bias, 1, (qkv,))
    if fast:
        y1, x2, s_other, qkv = tie(y1, x2, s_other, qkv)
        x1, xy1, y2, xy2 = px(s1, 2), px(y1, 2), px(s2, 4), px(x2, 4)
    mixed, lse = attention_forward(meta, qf, kf, qkv)
    if fast:
        x1, xy1, y2, xy2, mixed = tie(x1, xy1, y2, xy2, mixed)
        one = [px(v, 1) for v in (x1, y1, xy1)]
        two = [px(v, 1) for v in (x2, y2, xy2)]
        mlp_pieces = [s1, x1, y1, xy1, s2, x2, y2, xy2, s_other[0], *one, s_other[1], *two]
    else:
        mlp_pieces = [mlp_all]
    middle, normed_two, out_weight = out_projection(meta, mixed, start, own, other, out_params)
    branch, grad_two, grad_up, own_mlp, other_mlp = mlp(
        meta, normed_two, cotangent, cot_turned, mlp_bias_up, mlp_pieces
    )
    if fast:
        other_mlp, grad_two, branch = tie(other_mlp, grad_two, branch)
        got_mlp = px(other_mlp, 1)
    output, grad_middle, grad_mixed, own_out, other_out, sums_two = turn(
        meta, middle, branch, grad_two, cotangent, mixed, out_weight, turn_params
    )
    if fast:
        got_mlp, grad_mixed, other_out = tie(got_mlp, grad_mixed, other_out)
        send = [add_parts(own_mlp[c, 2:], got_mlp[c, 2:]).astype(B16) for c in range(2)]
        send, grad_mixed, other_out = tie(send, grad_mixed, other_out)
        got_1, got_2, got_out = px(send[0], 2), px(send[1], 4), px(other_out, 1)
    grads = attention_backward(meta, qf, kf, qkv, grad_mixed, mixed, lse)
    if fast:
        got_1, got_2, got_out, grads, grad_middle = tie(got_1, got_2, got_out, grads, grad_middle)
        planes = (got_1, got_2)

        def plane(c, i):
            return add_parts(own_mlp[c, i], got_mlp[c, i]) + planes[c][i].astype(F32)

        send, grads = tie([plane(c, 1).astype(B16) for c in range(2)], grads)
        got_1, got_2 = px(send[0], 4), px(send[1], 2)
    input_grad, packed = tail_step(
        meta, start, grad_middle, onehot, norm_gain[0:1], sums_two, grad_up, (own, other), grads
    )
    if fast:
        packed, grads, got_1, got_2 = tie(packed, grads, got_1, got_2)
        got_small = px(packed, 1)
        own_w, other_w = weight_grad(meta, normed_one, grads, "weight_grad_qkv")
        got_small, other_w = tie(got_small, other_w)
        got_w = px(other_w, 1)
        packed = pack_small(add_small(packed, got_small))
        got_small = px(packed, 2)
        got_w, got_small, packed = tie(got_w, got_small, packed)
        packed = pack_small(add_small(packed, got_small))
        got_small = px(packed, 4)
        col = [add_parts(plane(0, 0), got_1), add_parts(plane(1, 0), got_2)]
        send = jnp.stack([c[2:].astype(B16) for c in col])
        keep, *sends = gather_sums(own_w, got_w, own_out, got_out)
        send, sends, got_small, packed = tie(send, sends, got_small, packed)
        got_far = px(send, 16)
        moved = [px(x, 2 * i + 2) for i, x in enumerate(sends)]
        packed = pack_small(add_small(packed, got_small))
        got_small = px(packed, 8)
        moved, got_far, got_small, packed = tie(moved, got_far, got_small, packed)
        col_attn, *last = plane_sums(keep, moved)
        near = [add_parts(col[c][:2], got_far[c]) for c in range(2)]
        send = jnp.stack([x[1].astype(B16) for x in near])
        last, send = tie(last, send)
        last = [px(x, 8 * i + 8) for i, x in enumerate(last)]
        got_near = px(send, 8)
        small = exchange_small(pack_small(add_small(packed, got_small)), 16)
        mlp_grad = jnp.stack([x[0] for x in near]) + got_near.astype(F32)
        qkv_grad, out_grad = line_sums(col_attn, last)
    else:
        mlp_grad = own_mlp.transpose(2, 1, 3, 0, 4)
        mlp_grad = mlp_grad.reshape(2, 768, 3072)
        mlp_grad = lax.psum_scatter(mlp_grad, "dp", scatter_dimension=1, tiled=True)
        mlp_grad = lax.psum_scatter(mlp_grad, "mp", scatter_dimension=2, tiled=True).astype(F32)
        grad_out_weight = dotf(mixed, grad_middle.astype(B16), TN)
        grad_qkv = jnp.stack([dotf(normed_one, g, TN) for g in grads])
        qkv_grad = lax.psum_scatter(grad_qkv, AXES, scatter_dimension=1, tiled=True)
        out_grad = lax.psum_scatter(grad_out_weight, AXES, scatter_dimension=0, tiled=True)
        x = packed.astype(F32)
        small = lax.psum(jnp.concatenate([x[:64], x[64:80] + x[80:]]), AXES)
    return (
        output,
        input_grad,
        small[:NPROMPT],
        small[64:66],
        small[66:68],
        qkv_grad,
        small[68:71],
        out_grad,
        mlp_grad,
        small[72:76].reshape(-1),
        small[71],
    )


def solution(mesh):
    fast = dict(mesh.shape) == {"dp": 8, "mp": 4}
    return jax.shard_map(
        partial(local, fast),
        mesh=mesh,
        in_specs=(
            P(AXES, None),
            P(AXES, None),
            P(),
            P(AXES),
            P(AXES),
            P(),
            P(),
            P(None, AXES, None),
            P(),
            P(AXES, None),
            P(None, "dp", "mp"),
            P(),
            P(),
        ),
        out_specs=(
            P(AXES, None),
            P(AXES, None),
            P(),
            P(),
            P(),
            P(None, AXES, None),
            P(),
            P(AXES, None),
            P(None, "dp", "mp"),
            P(),
            P(),
        ),
        check_vma=False,
    )
```

```python
from functools import partial

import jax
import jax.numpy as jnp
from jax import lax
from jax.experimental import pallas as pl
from jax.experimental.pallas import tpu as pltpu
from jax.sharding import PartitionSpec as P

NPROMPT = 50
ROW = 1024
SPANS = (151, 247, 627)
EPS = 1e-06
HIGHEST = lax.Precision.HIGHEST
BIG = 1e30
B16 = jnp.bfloat16
F32 = jnp.float32
AXES = ("dp", "mp")
TILE = 256
STEP = 512
QROWS = 512
NT = (((1,), (1,)), ((), ()))
TN = (((0,), (0,)), ((), ()))
VMEM_LIMIT = 60 * 1024 * 1024


def layer_norm(value_list, gain_row, shift_row):
    centre = jnp.mean(value_list, axis=-1, keepdims=True)
    centred = value_list - centre
    spread = jnp.mean(centred * centred, axis=-1, keepdims=True)
    return centred * lax.rsqrt(spread + EPS) * gain_row + shift_row


def key_window(first, count):
    low, high = ROW, 0
    for span in SPANS:
        whole = ROW // span
        for row in (first, first + count - 1):
            seg = min(row // span, whole)
            low = min(low, seg * span)
            high = max(high, ROW if seg == whole else (seg + 1) * span)
    return low // 128 * 128, -(-high // 128) * 128


def dotf(a, b, dims=None):
    if dims is None:
        return jnp.dot(a, b, preferred_element_type=F32)
    return lax.dot_general(a, b, dims, preferred_element_type=F32)


def px(x, k):
    return lax.ppermute(x, AXES, [(i, i ^ k) for i in range(32)])


def tie(*trees):
    return lax.optimization_barrier(trees)


def stack_kernel(*refs):
    for i, ref in enumerate(refs[:-1]):
        refs[-1][i] = ref[...]


def stack(parts, name):
    vmem = pl.BlockSpec(memory_space=pltpu.VMEM)
    return pl.pallas_call(
        stack_kernel,
        name=name,
        out_shape=jax.ShapeDtypeStruct((len(parts),) + parts[0].shape, parts[0].dtype),
        in_specs=[vmem] * len(parts),
        out_specs=vmem,
    )(*parts)


def z_stage(piece):
    return stack([piece] + [px(piece, 8 * k) for k in range(1, 4)], "stack_z")


def stack_pair_kernel(*refs):
    for i, ref in enumerate(refs[:-2]):
        for c in range(2):
            refs[c - 2][i] = ref[c]


def stack_pair(parts):
    vmem = pl.BlockSpec(memory_space=pltpu.VMEM)
    shape = jax.ShapeDtypeStruct((len(parts),) + parts[0].shape[1:], parts[0].dtype)
    return pl.pallas_call(
        stack_pair_kernel,
        name="stack_pair",
        out_shape=(shape, shape),
        in_specs=[vmem] * len(parts),
        out_specs=(vmem, vmem),
    )(*parts)


def xy_stage(parts):
    return [parts] + [px(parts, 2 * k) for k in range(1, 4)]


def split_kernel(meta, qkv_ref, out_ref, mine_ref, theirs_ref):
    core = meta[0] % 2
    for ref, half in ((mine_ref, core), (theirs_ref, 1 - core)):
        cols = pl.ds(pl.multiple_of(384 * half, 128), 384)
        ref[0:3] = qkv_ref[:, :, cols]
        ref[3] = out_ref[:, cols]


def join_kernel(meta, mine_ref, got_ref, out_ref):
    for core in range(2):

        @pl.when(meta[0] % 2 == core)
        def _():
            out_ref[...] = jnp.concatenate([mine_ref[...], got_ref[...]][:: 1 - 2 * core], 1)


def pair_rows(meta, qkv, out):
    vmem = pl.BlockSpec(memory_space=pltpu.VMEM)
    smem = pl.BlockSpec(memory_space=pltpu.SMEM)
    half = jax.ShapeDtypeStruct((4, 24, 384), B16)
    mine, theirs = pl.pallas_call(
        split_kernel, name="split", out_shape=(half, half), in_specs=[smem, vmem, vmem], out_specs=(vmem, vmem)
    )(meta, qkv, out)
    return pl.pallas_call(
        join_kernel,
        name="join",
        out_shape=jax.ShapeDtypeStruct((4, 48, 384), B16),
        in_specs=[smem, vmem, vmem],
        out_specs=vmem,
    )(meta, mine, px(theirs, 1))


def assemble_kernel(meta, *refs):
    pieces, out, sems = refs[:4], refs[4], refs[5]
    copies = []
    for xy in range(4):
        for z in range(4):
            rows = pl.multiple_of(48 * jnp.bitwise_xor(meta[0] // 2, xy + 4 * z), 16)
            copies.append(
                pltpu.make_async_copy(pieces[xy].at[z], out.at[:, pl.ds(rows, 48), :], sems.at[4 * xy + z])
            )
    for copy in copies:
        copy.start()
    for copy in copies:
        copy.wait()


def assemble(meta, pieces, name):
    return pl.pallas_call(
        assemble_kernel,
        name=name,
        out_shape=jax.ShapeDtypeStruct((4, 768, 384), B16),
        in_specs=[pl.BlockSpec(memory_space=pltpu.SMEM)] + [pl.BlockSpec(memory_space=pl.ANY)] * 4,
        out_specs=pl.BlockSpec(memory_space=pltpu.VMEM),
        scratch_shapes=[pltpu.SemaphoreType.DMA((16,))],
    )(meta, *pieces)


def project_kernel(side, meta, x_ref, w_ref, b_ref, *refs):
    half = jnp.bitwise_xor(meta[0] % 2, side)
    cols = pl.ds(pl.multiple_of(384 * half, 128), 384)
    y = dotf(x_ref[...], w_ref[0]) + b_ref[pl.program_id(0), :, cols]
    refs[-1][...] = y.astype(B16)


def project(meta, x, weight, bias, side, held):
    rows = x.shape[0]
    vmem = pl.BlockSpec(memory_space=pltpu.VMEM)
    return pl.pallas_call(
        partial(project_kernel, side),
        name="project",
        grid=(3,),
        out_shape=jax.ShapeDtypeStruct((rows, 2304), B16),
        in_specs=[
            pl.BlockSpec(memory_space=pltpu.SMEM),
            vmem,
            pl.BlockSpec((1, 768, 384), lambda c: (c, 0, 0)),
            vmem,
        ]
        + [pl.BlockSpec(memory_space=pl.ANY)] * len(held),
        out_specs=pl.BlockSpec((rows, 384), lambda c: (0, 3 * side + c)),
        input_output_aliases={4 + i: i for i in range(len(held))},
        compiler_params=pltpu.CompilerParams(vmem_limit_bytes=VMEM_LIMIT),
    )(meta, x, weight, bias, *held)


def embed_kernel(tokens_ref, slots_ref, segs_ref, table_ref, p_ref, start_ref, normed_ref, hot_ref, qf_ref, kf_ref):
    lane = lax.broadcasted_iota(jnp.int32, (TILE, 128), 1)
    slots, segs = slots_ref[...], segs_ref[...]
    is_prompt = slots < NPROMPT
    hot = jnp.where((lane == slots) & is_prompt, 1.0, 0.0).astype(B16)
    hot_ref[...] = hot
    rows = None
    for part in three_parts(table_ref[...]):
        term = dotf(hot, part.astype(B16))
        rows = term if rows is None else rows + term
    start = jnp.where(is_prompt, rows, tokens_ref[...].astype(F32))
    start_ref[...] = start
    normed_ref[...] = (centred(start)[0] * p_ref[0:1] + p_ref[1:2]).astype(B16)
    spot = lane % 64
    same = (spot == segs) & (spot < 7)
    qf_ref[...] = jnp.where(same, 1.0, 0.0).astype(B16)
    kf = jnp.where(spot < 7, jnp.where(same, 0.0, -BIG), jnp.where(spot < 10, 1.0, 0.0))
    kf_ref[...] = kf.astype(B16)


def embed(tokens, slots, segs, table, params):
    rows = tokens.shape[0]

    def block(width):
        return pl.BlockSpec((TILE, width), lambda i: (i, 0))

    vmem = pl.BlockSpec(memory_space=pltpu.VMEM)
    lanes = jax.ShapeDtypeStruct((rows, 128), B16)
    return pl.pallas_call(
        embed_kernel,
        name="embed",
        grid=(rows // TILE,),
        in_specs=[block(768), block(1), block(1), vmem, vmem],
        out_specs=[block(768), block(768), block(128), block(128), block(128)],
        out_shape=(
            jax.ShapeDtypeStruct((rows, 768), F32),
            jax.ShapeDtypeStruct((rows, 768), B16),
            lanes,
            lanes,
            lanes,
        ),
    )(tokens, slots[:, None], segs[:, None], table, params)


def gather_sums_kernel(own_ref, got_ref, own_out_ref, got_out_ref, keep_ref, *sends):
    for k in range(4):
        for z in range(4):
            for m in range(4):
                if m < 3:
                    x = add_parts(own_ref[k, z, m], got_ref[k, z, m])
                else:
                    x = add_parts(own_out_ref[k, z, 0], got_out_ref[k, z, 0])
                if k:
                    sends[k - 1][z, m] = x.astype(B16)
                else:
                    keep_ref[z, m] = x


def gather_sums(own, got, own_out, got_out):
    vmem = pl.BlockSpec(memory_space=pltpu.VMEM)
    send = jax.ShapeDtypeStruct((4, 4, 24, 768), B16)
    return pl.pallas_call(
        gather_sums_kernel,
        name="gather_sums",
        in_specs=[vmem] * 4,
        out_specs=[vmem] * 4,
        out_shape=(jax.ShapeDtypeStruct((4, 4, 24, 768), F32), send, send, send),
        compiler_params=pltpu.CompilerParams(vmem_limit_bytes=VMEM_LIMIT),
    )(own, got, own_out, got_out)


def four(values):
    return (values[0] + values[1]) + (values[2] + values[3])


def plane_sums_kernel(keep_ref, *refs):
    moved, (col_ref, *sends) = refs[:3], refs[3:]
    for z in range(4):
        for m in range(4):
            x = four([keep_ref[z, m]] + [ref[z, m].astype(F32) for ref in moved])
            if z:
                sends[z - 1][m] = x.astype(B16)
            else:
                col_ref[m] = x


def plane_sums(keep, moved):
    vmem = pl.BlockSpec(memory_space=pltpu.VMEM)
    send = jax.ShapeDtypeStruct((4, 24, 768), B16)
    return pl.pallas_call(
        plane_sums_kernel,
        name="plane_sums",
        in_specs=[vmem] * 4,
        out_specs=[vmem] * 4,
        out_shape=(jax.ShapeDtypeStruct((4, 24, 768), F32), send, send, send),
        compiler_params=pltpu.CompilerParams(vmem_limit_bytes=VMEM_LIMIT),
    )(keep, *moved)


def line_sums_kernel(col_ref, *refs):
    last, (qkv_ref, out_ref) = refs[:3], refs[3:]
    for m in range(4):
        x = four([col_ref[m]] + [ref[m].astype(F32) for ref in last])
        if m < 3:
            qkv_ref[m] = x
        else:
            out_ref[...] = x


def line_sums(col, last):
    vmem = pl.BlockSpec(memory_space=pltpu.VMEM)
    return pl.pallas_call(
        line_sums_kernel,
        name="line_sums",
        in_specs=[vmem] * 4,
        out_specs=[vmem] * 2,
        out_shape=(jax.ShapeDtypeStruct((3, 24, 768), F32), jax.ShapeDtypeStruct((24, 768), F32)),
    )(col, *last)


def centred(x):
    mean = jnp.mean(x, axis=-1, keepdims=True)
    x = x - mean
    rate = lax.rsqrt(jnp.mean(x * x, axis=-1, keepdims=True) + EPS)
    return x * rate, rate


def out_kernel(meta, x_ref, start_ref, own_ref, other_ref, p_ref, middle_ref, normed_ref, w_ref):
    core = meta[0] % 2

    @pl.when(pl.program_id(0) == 0)
    def _():
        for ref, half in ((own_ref, core), (other_ref, 1 - core)):
            w_ref[:, pl.ds(pl.multiple_of(384 * half, 128), 384)] = ref[0]

    middle = start_ref[...] + dotf(x_ref[...], w_ref[...]) + p_ref[0:1]
    middle_ref[...] = middle
    normed_ref[...] = (centred(middle)[0] * p_ref[1:2] + p_ref[2:3]).astype(B16)


def out_projection(meta, mixed, start, own, other, params):
    rows = mixed.shape[0]
    block = pl.BlockSpec((STEP, 768), lambda i: (i, 0))
    vmem = pl.BlockSpec(memory_space=pltpu.VMEM)
    return pl.pallas_call(
        out_kernel,
        name="out_projection",
        grid=(rows // STEP,),
        in_specs=[pl.BlockSpec(memory_space=pltpu.SMEM), block, block]
        + [pl.BlockSpec((1, 768, 384), lambda i: (3, 0, 0))] * 2
        + [vmem],
        out_specs=[block, block, vmem],
        out_shape=(
            jax.ShapeDtypeStruct((rows, 768), F32),
            jax.ShapeDtypeStruct((rows, 768), B16),
            jax.ShapeDtypeStruct((768, 768), B16),
        ),
        compiler_params=pltpu.CompilerParams(vmem_limit_bytes=VMEM_LIMIT),
    )(meta, mixed, start, own, other, params)


def norm_backward(normal, rate, grad, gain):
    u = grad * gain
    return rate * (u - jnp.mean(u, axis=-1, keepdims=True) - normal * jnp.mean(u * normal, axis=-1, keepdims=True))


def row_sum(x):
    return jnp.sum(x, axis=0, keepdims=True)


def put_parts(meta, acc, own_ref, other_ref, m):
    chip, core = meta[0] // 2, meta[0] % 2
    for z in range(4):
        for xy in range(4):
            row = 48 * jnp.bitwise_xor(chip, xy + 4 * z)
            own_ref[xy, z, m] = acc[pl.ds(pl.multiple_of(row + 24 * core, 8), 24), :].astype(B16)
            other_ref[xy, z, m] = acc[pl.ds(pl.multiple_of(row + 24 * (1 - core), 8), 24), :].astype(B16)


def turn_kernel(
    meta, middle_ref, branch_ref, grad_ref, cot_ref, mixed_ref, w_ref, p_ref,
    output_ref, gmiddle_ref, gmixed_ref, own_ref, other_ref, sums_ref, acc,
):
    i = pl.program_id(0)

    @pl.when(i == 0)
    def _():
        sums_ref[...] = jnp.zeros_like(sums_ref)
        acc[...] = jnp.zeros_like(acc)

    middle, grad = middle_ref[...], grad_ref[...]
    cot = cot_ref[...].astype(F32)
    output_ref[...] = (middle + branch_ref[...] + p_ref[1:2]).astype(B16)
    normal, rate = centred(middle)
    gmiddle = cot + norm_backward(normal, rate, grad, p_ref[0:1])
    gmiddle_ref[...] = gmiddle
    low = gmiddle.astype(B16)
    for row, x in enumerate((normal * grad, grad, low.astype(F32), cot)):
        sums_ref[row : row + 1, :] += row_sum(x)
    gmixed_ref[...] = dotf(low, w_ref[...], NT).astype(B16)
    acc[...] += dotf(mixed_ref[...], low, TN)

    @pl.when(i == pl.num_programs(0) - 1)
    def _():
        put_parts(meta, acc, own_ref, other_ref, 0)


def turn(meta, middle, branch, grad, cot, mixed, weight, params):
    rows = middle.shape[0]
    block = pl.BlockSpec((STEP, 768), lambda i: (i, 0))
    vmem = pl.BlockSpec(memory_space=pltpu.VMEM)
    parts = jax.ShapeDtypeStruct((4, 4, 1, 24, 768), B16)
    return pl.pallas_call(
        turn_kernel,
        name="turn",
        grid=(rows // STEP,),
        in_specs=[pl.BlockSpec(memory_space=pltpu.SMEM)] + [block] * 5 + [vmem, vmem],
        out_specs=[block, block, block, vmem, vmem, vmem],
        out_shape=(
            jax.ShapeDtypeStruct((rows, 768), B16),
            jax.ShapeDtypeStruct((rows, 768), F32),
            jax.ShapeDtypeStruct((rows, 768), B16),
            parts,
            parts,
            jax.ShapeDtypeStruct((8, 768), F32),
        ),
        scratch_shapes=[pltpu.VMEM((768, 768), F32)],
        compiler_params=pltpu.CompilerParams(vmem_limit_bytes=VMEM_LIMIT),
    )(meta, middle, branch, grad, cot, mixed, weight, params)


def tail_kernel(meta, start_ref, gmiddle_ref, slots_ref, p_ref, turn_ref, up_ref, *refs):
    weights, grads = refs[:2], refs[2:5]
    input_ref, packed_ref, prompt_ref, sums_ref = refs[5:]
    core = meta[0] % 2

    @pl.when(pl.program_id(0) == 0)
    def _():
        prompt_ref[...] = jnp.zeros_like(prompt_ref)
        sums_ref[...] = jnp.zeros_like(sums_ref)

    total = None
    for c in range(3):
        for side in range(2):
            half = jnp.bitwise_xor(core, side)
            left = grads[c][:, pl.ds(pl.multiple_of(384 * half, 128), 384)]
            term = dotf(left, weights[side][c], NT)
            total = term if total is None else total + term
    normal, rate = centred(start_ref[...])
    rows = ((0, normal * total), (2, total), (4, grads[0][...].astype(F32)), (5, grads[2][...].astype(F32)))
    for row, x in rows:
        sums_ref[row : row + 1, :] += row_sum(x)
    gstart = gmiddle_ref[...] + norm_backward(normal, rate, total, p_ref[0:1])
    slots = slots_ref[...]
    is_prompt = jnp.sum(slots.astype(F32), axis=-1, keepdims=True) > 0.5
    input_ref[...] = jnp.where(is_prompt, 0.0, gstart)
    for part in three_parts(gstart)[:2]:
        prompt_ref[...] += dotf(slots, part.astype(B16), TN)

    @pl.when(pl.program_id(0) == pl.num_programs(0) - 1)
    def _():
        for row, source in ((1, 0), (3, 1), (6, 2), (7, 3)):
            sums_ref[row : row + 1, :] = turn_ref[source : source + 1, :]
        for row in range(4):
            sums_ref[8 + row : 9 + row, :] = up_ref[row]
        packed_ref[0:64, :] = prompt_ref[0:64, :].astype(B16)
        high, low = split_rows(sums_ref[...])
        packed_ref[64:80, :] = high
        packed_ref[80:96, :] = low


def tail_step(meta, start, gmiddle, slots, params, sums_two, up, weights, grads):
    rows = start.shape[0]

    def block(width):
        return pl.BlockSpec((STEP, width), lambda i: (i, 0))

    vmem = pl.BlockSpec(memory_space=pltpu.VMEM)
    return pl.pallas_call(
        tail_kernel,
        name="tail_step",
        grid=(rows // STEP,),
        in_specs=[pl.BlockSpec(memory_space=pltpu.SMEM), block(768), block(768), block(128)]
        + [vmem] * 3
        + [pl.BlockSpec((3, 768, 384), lambda i: (0, 0, 0))] * 2
        + [block(768)] * 3,
        out_specs=[block(768), vmem],
        out_shape=(
            jax.ShapeDtypeStruct((rows, 768), F32),
            jax.ShapeDtypeStruct((96, 768), B16),
        ),
        scratch_shapes=[pltpu.VMEM((128, 768), F32), pltpu.VMEM((16, 768), F32)],
        compiler_params=pltpu.CompilerParams(vmem_limit_bytes=VMEM_LIMIT),
    )(meta, start, gmiddle, slots, params, sums_two, up, *weights, *grads)


def weight_grad_kernel(count, meta, left_ref, *refs):
    rights, own_ref, other_ref, acc = refs[:count], refs[count], refs[count + 1], refs[count + 2]
    for m in range(count):
        acc[...] = dotf(left_ref[...], rights[m][...], TN)
        put_parts(meta, acc, own_ref, other_ref, m)


def weight_grad(meta, left, rights, name):
    count, width = len(rights), rights[0].shape[1]
    shape = jax.ShapeDtypeStruct((4, 4, count, 24, width), B16)
    vmem = pl.BlockSpec(memory_space=pltpu.VMEM)
    return pl.pallas_call(
        partial(weight_grad_kernel, count),
        name=name,
        out_shape=(shape, shape),
        in_specs=[pl.BlockSpec(memory_space=pltpu.SMEM)] + [vmem] * (count + 1),
        out_specs=(vmem, vmem),
        scratch_shapes=[pltpu.VMEM((left.shape[1], width), F32)],
        compiler_params=pltpu.CompilerParams(vmem_limit_bytes=VMEM_LIMIT),
    )(meta, left, *rights)


def split_rows(rest):
    high = rest.astype(B16)
    return high, (rest - high.astype(F32)).astype(B16)


def add_small(x, y):
    x, y = x.astype(F32), y.astype(F32)
    return jnp.concatenate([x[:64] + y[:64], (x[64:80] + x[80:]) + (y[64:80] + y[80:])])


def pack_small(x):
    return jnp.concatenate([x[:64].astype(B16), *split_rows(x[64:])])


def exchange_small(x, k):
    return add_small(x, px(x, k))


def add_parts(own, got):
    return own.astype(F32) + got.astype(F32)


def three_parts(x):
    high = x.astype(B16).astype(F32)
    mid = (x - high).astype(B16).astype(F32)
    return high, mid, (x - high) - mid


def attention_forward_kernel(qf_ref, kf_ref, q_ref, k_ref, v_ref, mixed_ref, lse_ref):
    half = lax.broadcasted_iota(jnp.int32, (1, 128), 1) < 64
    q = q_ref[...] * jnp.asarray(0.125, B16)
    k, v = k_ref[...], v_ref[...]
    qf, kf = qf_ref[...], kf_ref[...]
    one = jnp.ones((), B16)
    sides = []
    for e in range(2):
        own = half if e == 0 else ~half
        sides.append((jnp.where(own, q, qf), jnp.where(own, k, kf), jnp.where(own, v, one)))
    for first in range(0, ROW, QROWS):
        low, high = key_window(first, QROWS)
        outs, peaks = [], []
        for qe, ke, ve in sides:
            s = dotf(qe[first : first + QROWS], ke[low:high], NT)
            peak = jnp.max(s, axis=-1, keepdims=True)
            p = jnp.exp(s - peak).astype(B16)
            outs.append(dotf(p, ve[low:high]))
            peaks.append(peak)
        data = jnp.where(half, outs[0], outs[1])
        total = pltpu.roll(jnp.where(half, outs[1], outs[0]), 64, 1)
        mixed_ref[first : first + QROWS, :] = (data / total).astype(B16)
        lse_ref[first : first + QROWS, :] = jnp.where(half, peaks[0], peaks[1]) + jnp.log(total)


def pair_specs(rows):
    full = pl.BlockSpec((ROW, 128), lambda r, s, p, meta: (r, 0))
    blocks = [pl.BlockSpec((ROW, 128), lambda r, s, p, meta, c=c: (r, 9 * s + 3 * c + p)) for c in range(3)]
    whole = pl.BlockSpec((ROW, 128), lambda r, s, p, meta: (r, 3 * jnp.bitwise_xor(meta[0] % 2, s) + p))
    return (rows // ROW, 2, 3), full, blocks, whole


def attention_forward(meta, qf, kf, qkv):
    rows = qkv.shape[0]
    grid, full, blocks, whole = pair_specs(rows)

    def kernel(meta, *refs):
        attention_forward_kernel(*refs)

    return pl.pallas_call(
        kernel,
        name="attention_forward",
        grid_spec=pltpu.PrefetchScalarGridSpec(
            num_scalar_prefetch=1, grid=grid, in_specs=[full, full] + blocks, out_specs=[whole, whole]
        ),
        out_shape=(
            jax.ShapeDtypeStruct((rows, 768), B16),
            jax.ShapeDtypeStruct((rows, 768), F32),
        ),
        compiler_params=pltpu.CompilerParams(vmem_limit_bytes=VMEM_LIMIT),
    )(meta, qf, kf, qkv, qkv, qkv)


def attention_backward_kernel(
    qf_ref, kf_ref, q_ref, k_ref, v_ref, g_ref, mixed_ref, lse_ref, dq_ref, dk_ref, dv_ref, dk_acc, dv_acc
):
    lane = lax.broadcasted_iota(jnp.int32, (1, 128), 1)
    half = lane < 64
    spot = lane % 64
    q = q_ref[...] * jnp.asarray(0.125, B16)
    k, v, g = k_ref[...], v_ref[...], g_ref[...]
    qf, kf = qf_ref[...].astype(F32), kf_ref[...]
    prod = g.astype(F32) * mixed_ref[...].astype(F32)
    d0 = jnp.sum(jnp.where(half, prod, 0.0), axis=-1, keepdims=True)
    d1 = jnp.sum(jnp.where(half, 0.0, prod), axis=-1, keepdims=True)
    delta = jnp.where(half, d1, d0)
    lse = pltpu.roll(lse_ref[...], 64, 1)

    def spread(base, x):
        a, b, c = three_parts(-x)
        return jnp.where(spot == 7, a, jnp.where(spot == 8, b, jnp.where(spot == 9, c, base))).astype(B16)

    q_extra = spread(qf, lse)
    g_extra = spread(jnp.zeros_like(qf), delta)
    v_extra = jnp.where((spot >= 7) & (spot <= 9), 1.0, 0.0).astype(B16)
    dk_acc[...] = jnp.zeros_like(dk_acc)
    dv_acc[...] = jnp.zeros_like(dv_acc)
    sides = []
    for e in range(2):
        own = half if e == 0 else ~half
        sides.append(
            (
                jnp.where(own, q, q_extra),
                jnp.where(own, k, kf),
                jnp.where(own, g, g_extra),
                jnp.where(own, v, v_extra),
            )
        )
    for first in range(0, ROW, TILE):
        low, high = key_window(first, TILE)
        dqs, dks, dvs = [], [], []
        for qe, ke, ge, ve in sides:
            s = dotf(qe[first : first + TILE], ke[low:high], NT)
            p = jnp.exp(s)
            d = dotf(ge[first : first + TILE], ve[low:high], NT)
            ds = (p * d).astype(B16)
            dqs.append(dotf(ds, k[low:high]))
            dks.append(dotf(ds, q[first : first + TILE], TN))
            dvs.append(dotf(p.astype(B16), g[first : first + TILE], TN))
        dq_ref[first : first + TILE, :] = (jnp.where(half, dqs[0], dqs[1]) * 0.125).astype(B16)
        dk_acc[low:high, :] += jnp.where(half, dks[0], dks[1])
        dv_acc[low:high, :] += jnp.where(half, dvs[0], dvs[1])
    dk_ref[...] = dk_acc[...].astype(B16)
    dv_ref[...] = dv_acc[...].astype(B16)


def attention_backward(meta, qf, kf, qkv, grad, mixed, lse):
    rows = qkv.shape[0]
    grid, full, blocks, whole = pair_specs(rows)
    shape = jax.ShapeDtypeStruct((rows, 768), B16)

    def kernel(meta, *refs):
        attention_backward_kernel(*refs)

    return pl.pallas_call(
        kernel,
        name="attention_backward",
        grid_spec=pltpu.PrefetchScalarGridSpec(
            num_scalar_prefetch=1,
            grid=grid,
            in_specs=[full, full] + blocks + [whole] * 3,
            out_specs=[whole] * 3,
            scratch_shapes=[pltpu.VMEM((ROW, 128), F32), pltpu.VMEM((ROW, 128), F32)],
        ),
        out_shape=(shape, shape, shape),
        compiler_params=pltpu.CompilerParams(vmem_limit_bytes=VMEM_LIMIT),
    )(meta, qf, kf, qkv, qkv, qkv, grad, mixed, lse)


SUB = 256
PER = 768 // SUB


def mlp_kernel(fast, *refs):
    meta, n_ref, c_ref, ct, b_ref = refs[:5]
    count = 16 if fast else 1
    pieces, refs = refs[5 : 5 + count], refs[5 + count :]
    branch_ref, gn_ref, db_ref, own_ref, other_ref = refs[:5]
    w, nt, dw, wsem, dsem = refs[5:]
    t = pl.program_id(0)
    jr, sub = t // PER, t % PER
    me_mp, me_dp = meta[0] % 4, meta[0] // 4

    def loads(j):
        if not fast:
            source = pieces[0].at[:, :, pl.ds(768 * j, 768)]
            return [pltpu.make_async_copy(source, w.at[j], wsem.at[j, 0, 0])]
        out = []
        for dr in range(8):
            rows = pl.multiple_of(96 * jnp.bitwise_xor(me_dp, dr), 32)
            for c in range(2):
                source = pieces[8 * (j & 1) + 4 * c + (j >> 1) + 2 * (dr & 1)].at[dr >> 1]
                out.append(pltpu.make_async_copy(source, w.at[j, c, pl.ds(rows, 96), :], wsem.at[j, dr, c]))
        return out

    def stores(j):
        if not fast:
            return [pltpu.make_async_copy(dw.at[j], own_ref.at[j], dsem.at[j, 0, 0])]
        out = []
        for dr in range(8):
            x, y = j >> 1, dr & 1
            for c, spot in enumerate((2 * x + y, 2 * y + x)):
                target = (other_ref if j & 1 else own_ref).at[c, spot, dr >> 1]
                out.append(pltpu.make_async_copy(dw.at[j, dr, c], target, dsem.at[j, dr, c]))
        return out

    @pl.when(t == 0)
    def _():
        for j in range(4):
            for copy in loads(j):
                copy.start()
        nt[...] = n_ref[...].T
        branch_ref[...] = jnp.zeros_like(branch_ref)
        gn_ref[...] = jnp.zeros_like(gn_ref)

    for j in range(4):

        @pl.when(t == PER * j)
        def _():
            for copy in loads(j):
                copy.wait()

    spot = jnp.bitwise_xor(me_mp, jr) if fast else jr
    cols = pl.ds(pl.multiple_of(sub * SUB, SUB), SUB)
    w1 = w[jr, 0, :, cols]
    w2 = w[jr, 1, :, cols]
    u = dotf(n_ref[...], w1) + b_ref[spot, :, cols]
    cdf = 0.5 * (1.0 + lax.erf(u * 0.7071067811865476))
    hidden = (u * cdf).astype(B16)
    slope = cdf + u * (0.3989422804014327 * jnp.exp(-0.5 * u * u))
    gb = (dotf(c_ref[...], w2) * slope).astype(B16)
    db_ref[spot, :, cols] = jnp.sum(gb.astype(F32), axis=0, keepdims=True)
    branch_ref[...] += dotf(hidden, w2, NT)
    gn_ref[...] += dotf(gb, w1, NT)
    dw1 = dotf(nt[...], gb).astype(B16)
    dw2 = dotf(ct[...], hidden).astype(B16)
    for a in range(8):
        dr = jnp.bitwise_xor(me_dp, a) if fast else a
        dw[jr, dr, 0, :, cols] = dw1[96 * a : 96 * a + 96]
        dw[jr, dr, 1, :, cols] = dw2[96 * a : 96 * a + 96]

    for j in range(4):

        @pl.when(t == PER * j + PER - 1)
        def _():
            for copy in stores(j):
                copy.start()

    @pl.when(t == 4 * PER - 1)
    def _():
        for j in range(4):
            for copy in stores(j):
                copy.wait()


def mlp(meta, normed, cot, cot_turned, bias, pieces):
    fast = len(pieces) == 16
    tokens = normed.shape[0]
    vmem = pl.BlockSpec(memory_space=pltpu.VMEM)
    anys = pl.BlockSpec(memory_space=pl.ANY)
    shape = jax.ShapeDtypeStruct((2, 4, 4, 96, 768) if fast else (4, 8, 2, 96, 768), B16)
    return pl.pallas_call(
        partial(mlp_kernel, fast),
        name="mlp",
        grid=(4 * PER,),
        in_specs=[pl.BlockSpec(memory_space=pltpu.SMEM)] + [vmem] * 4 + [anys] * len(pieces),
        out_specs=[vmem, vmem, vmem, anys, anys],
        out_shape=(
            jax.ShapeDtypeStruct((tokens, 768), F32),
            jax.ShapeDtypeStruct((tokens, 768), F32),
            jax.ShapeDtypeStruct((4, 1, 768), F32),
            shape,
            shape,
        ),
        scratch_shapes=[
            pltpu.VMEM((4, 2, 768, 768), B16),
            pltpu.VMEM((768, tokens), B16),
            pltpu.VMEM((4, 8, 2, 96, 768), B16),
            pltpu.SemaphoreType.DMA((4, 8, 2)),
            pltpu.SemaphoreType.DMA((4, 8, 2)),
        ],
        compiler_params=pltpu.CompilerParams(vmem_limit_bytes=VMEM_LIMIT),
    )(meta, normed, cot, cot_turned, bias.reshape(4, 1, 768), *pieces)


def local(
    fast,
    tokens,
    cotangent,
    prompts,
    segments,
    prompt_slot_index,
    norm_gain,
    norm_shift,
    attn_qkv,
    attn_bias,
    attn_out,
    mlp_weight,
    mlp_bias_up,
    mlp_bias_down,
):
    width = tokens.shape[1]
    device = lax.axis_index("dp") * lax.axis_size("mp") + lax.axis_index("mp")
    meta = jnp.reshape(device, (1,)).astype(jnp.int32)
    core = device % 2
    if fast:
        piece = pair_rows(meta, attn_qkv, attn_out)
        held = z_stage(piece)
        held, mlp_near, mlp_piece, tokens, prompts, segments, prompt_slot_index = tie(
            held, px(mlp_weight, 8), mlp_weight, tokens, prompts, segments, prompt_slot_index
        )
    table = jnp.concatenate([prompts, jnp.zeros((128 - NPROMPT, width), F32)], 0)
    start, normed_one, onehot, qf, kf = embed(
        tokens, prompt_slot_index, segments, table, jnp.stack([norm_gain[0], norm_shift[0]])
    )
    bias = jnp.stack([attn_bias[0], jnp.zeros_like(attn_bias[0]), attn_bias[1]])[:, None]
    out_params = jnp.stack([attn_bias[2], norm_gain[1], norm_shift[1]])
    turn_params = jnp.stack([norm_gain[1], mlp_bias_down])
    cot_turned = cotangent.T

    if fast:
        x = (normed_one, start, qf, kf, onehot, bias, out_params, turn_params, cot_turned)
        mlp_z = [mlp_piece, mlp_near] + [px(mlp_piece, 8 * k) for k in range(2, 4)]
        quad, mlp_z, x = tie(xy_stage(held), mlp_z, x)
        normed_one, start, qf, kf, onehot, bias, out_params, turn_params, cot_turned = x
        own = assemble(meta, quad, "assemble")
        s1, s2 = stack_pair(mlp_z)
        own, s1, s2 = tie(own, s1, s2)
        other, y1, x2 = px(own, 1), px(s1, 4), px(s2, 2)
        s_other = [px(s1, 1), px(s2, 1)]
        qkv = project(meta, normed_one, own, bias, 0, ())
        other, qkv = tie(other, qkv)
    else:
        qkv_all = lax.all_gather(attn_qkv, AXES, axis=1, tiled=True)
        out_all = lax.all_gather(attn_out, AXES, axis=0, tiled=True)
        mlp_all = lax.all_gather(mlp_weight, "dp", axis=1, tiled=True)
        mlp_all = lax.all_gather(mlp_all, "mp", axis=2, tiled=True)
        four_all = jnp.concatenate([qkv_all, out_all[None]])
        own = lax.dynamic_slice_in_dim(four_all, 384 * core, 384, 2)
        other = lax.dynamic_slice_in_dim(four_all, 384 * (1 - core), 384, 2)
        qkv = project(meta, normed_one, own, bias, 0, ())
    qkv = project(meta, normed_one, other, bias, 1, (qkv,))
    if fast:
        y1, x2, s_other, qkv = tie(y1, x2, s_other, qkv)
        x1, xy1, y2, xy2 = px(s1, 2), px(y1, 2), px(s2, 4), px(x2, 4)
    mixed, lse = attention_forward(meta, qf, kf, qkv)
    if fast:
        x1, xy1, y2, xy2, mixed = tie(x1, xy1, y2, xy2, mixed)
        one = [px(v, 1) for v in (x1, y1, xy1)]
        two = [px(v, 1) for v in (x2, y2, xy2)]
        mlp_pieces = [s1, x1, y1, xy1, s2, x2, y2, xy2, s_other[0], *one, s_other[1], *two]
    else:
        mlp_pieces = [mlp_all]
    middle, normed_two, out_weight = out_projection(meta, mixed, start, own, other, out_params)
    branch, grad_two, grad_up, own_mlp, other_mlp = mlp(
        meta, normed_two, cotangent, cot_turned, mlp_bias_up, mlp_pieces
    )
    if fast:
        other_mlp, grad_two, branch = tie(other_mlp, grad_two, branch)
        got_mlp = px(other_mlp, 1)
    output, grad_middle, grad_mixed, own_out, other_out, sums_two = turn(
        meta, middle, branch, grad_two, cotangent, mixed, out_weight, turn_params
    )
    if fast:
        got_mlp, grad_mixed, other_out = tie(got_mlp, grad_mixed, other_out)
        send = [add_parts(own_mlp[c, 2:], got_mlp[c, 2:]).astype(B16) for c in range(2)]
        send, grad_mixed, other_out = tie(send, grad_mixed, other_out)
        got_1, got_2, got_out = px(send[0], 2), px(send[1], 4), px(other_out, 1)
    grads = attention_backward(meta, qf, kf, qkv, grad_mixed, mixed, lse)
    if fast:
        got_1, got_2, got_out, grads, grad_middle = tie(got_1, got_2, got_out, grads, grad_middle)
        planes = (got_1, got_2)

        def plane(c, i):
            return add_parts(own_mlp[c, i], got_mlp[c, i]) + planes[c][i].astype(F32)

        send, grads = tie([plane(c, 1).astype(B16) for c in range(2)], grads)
        got_1, got_2 = px(send[0], 4), px(send[1], 2)
    input_grad, packed = tail_step(
        meta, start, grad_middle, onehot, norm_gain[0:1], sums_two, grad_up, (own, other), grads
    )
    if fast:
        packed, grads, got_1, got_2 = tie(packed, grads, got_1, got_2)
        got_small = px(packed, 1)
        own_w, other_w = weight_grad(meta, normed_one, grads, "weight_grad_qkv")
        got_small, other_w = tie(got_small, other_w)
        got_w = px(other_w, 1)
        packed = pack_small(add_small(packed, got_small))
        packed, got_1, got_2 = tie(packed, got_1, got_2)
        got_small = px(packed, 2)
        got_w, got_small, packed = tie(got_w, got_small, packed)
        packed = pack_small(add_small(packed, got_small))
        got_small = px(packed, 4)
        col = [add_parts(plane(0, 0), got_1), add_parts(plane(1, 0), got_2)]
        send = jnp.stack([c[2:].astype(B16) for c in col])
        keep, *sends = gather_sums(own_w, got_w, own_out, got_out)
        send, sends, got_small, packed = tie(send, sends, got_small, packed)
        got_far = px(send, 16)
        moved = [px(x, 2 * i + 2) for i, x in enumerate(sends)]
        packed = pack_small(add_small(packed, got_small))
        got_small = px(packed, 8)
        moved, got_far, got_small, packed = tie(moved, got_far, got_small, packed)
        col_attn, *last = plane_sums(keep, moved)
        near = [add_parts(col[c][:2], got_far[c]) for c in range(2)]
        send = jnp.stack([x[1].astype(B16) for x in near])
        last, send = tie(last, send)
        last = [px(x, 8 * i + 8) for i, x in enumerate(last)]
        got_near = px(send, 8)
        small = exchange_small(pack_small(add_small(packed, got_small)), 16)
        mlp_grad = jnp.stack([x[0] for x in near]) + got_near.astype(F32)
        qkv_grad, out_grad = line_sums(col_attn, last)
    else:
        mlp_grad = own_mlp.transpose(2, 1, 3, 0, 4)
        mlp_grad = mlp_grad.reshape(2, 768, 3072)
        mlp_grad = lax.psum_scatter(mlp_grad, "dp", scatter_dimension=1, tiled=True)
        mlp_grad = lax.psum_scatter(mlp_grad, "mp", scatter_dimension=2, tiled=True).astype(F32)
        grad_out_weight = dotf(mixed, grad_middle.astype(B16), TN)
        grad_qkv = jnp.stack([dotf(normed_one, g, TN) for g in grads])
        qkv_grad = lax.psum_scatter(grad_qkv, AXES, scatter_dimension=1, tiled=True)
        out_grad = lax.psum_scatter(grad_out_weight, AXES, scatter_dimension=0, tiled=True)
        x = packed.astype(F32)
        small = lax.psum(jnp.concatenate([x[:64], x[64:80] + x[80:]]), AXES)
    return (
        output,
        input_grad,
        small[:NPROMPT],
        small[64:66],
        small[66:68],
        qkv_grad,
        small[68:71],
        out_grad,
        mlp_grad,
        small[72:76].reshape(-1),
        small[71],
    )


def solution(mesh):
    fast = dict(mesh.shape) == {"dp": 8, "mp": 4}
    return jax.shard_map(
        partial(local, fast),
        mesh=mesh,
        in_specs=(
            P(AXES, None),
            P(AXES, None),
            P(),
            P(AXES),
            P(AXES),
            P(),
            P(),
            P(None, AXES, None),
            P(),
            P(AXES, None),
            P(None, "dp", "mp"),
            P(),
            P(),
        ),
        out_specs=(
            P(AXES, None),
            P(AXES, None),
            P(),
            P(),
            P(),
            P(None, AXES, None),
            P(),
            P(AXES, None),
            P(None, "dp", "mp"),
            P(),
            P(),
        ),
        check_vma=False,
    )
```

```python
from functools import partial

import jax
import jax.numpy as jnp
from jax import lax
from jax.experimental import pallas as pl
from jax.experimental.pallas import tpu as pltpu
from jax.sharding import PartitionSpec as P

NPROMPT = 50
ROW = 1024
SPANS = (151, 247, 627)
EPS = 1e-06
HIGHEST = lax.Precision.HIGHEST
BIG = 1e30
B16 = jnp.bfloat16
F32 = jnp.float32
AXES = ("dp", "mp")
TILE = 256
STEP = 512
QROWS = 512
NT = (((1,), (1,)), ((), ()))
TN = (((0,), (0,)), ((), ()))
VMEM_LIMIT = 60 * 1024 * 1024


def layer_norm(value_list, gain_row, shift_row):
    centre = jnp.mean(value_list, axis=-1, keepdims=True)
    centred = value_list - centre
    spread = jnp.mean(centred * centred, axis=-1, keepdims=True)
    return centred * lax.rsqrt(spread + EPS) * gain_row + shift_row


def key_window(first, count):
    low, high = ROW, 0
    for span in SPANS:
        whole = ROW // span
        for row in (first, first + count - 1):
            seg = min(row // span, whole)
            low = min(low, seg * span)
            high = max(high, ROW if seg == whole else (seg + 1) * span)
    return low // 128 * 128, -(-high // 128) * 128


def dotf(a, b, dims=None):
    if dims is None:
        return jnp.dot(a, b, preferred_element_type=F32)
    return lax.dot_general(a, b, dims, preferred_element_type=F32)


def px(x, k):
    return lax.ppermute(x, AXES, [(i, i ^ k) for i in range(32)])


def tie(*trees):
    return lax.optimization_barrier(trees)


def stack_kernel(*refs):
    for i, ref in enumerate(refs[:-1]):
        refs[-1][i] = ref[...]


def stack(parts, name):
    vmem = pl.BlockSpec(memory_space=pltpu.VMEM)
    return pl.pallas_call(
        stack_kernel,
        name=name,
        out_shape=jax.ShapeDtypeStruct((len(parts),) + parts[0].shape, parts[0].dtype),
        in_specs=[vmem] * len(parts),
        out_specs=vmem,
    )(*parts)


def z_stage(piece):
    return stack([piece] + [px(piece, 8 * k) for k in range(1, 4)], "stack_z")


def stack_pair_kernel(*refs):
    for i, ref in enumerate(refs[:-2]):
        for c in range(2):
            refs[c - 2][i] = ref[c]


def stack_pair(parts):
    vmem = pl.BlockSpec(memory_space=pltpu.VMEM)
    shape = jax.ShapeDtypeStruct((len(parts),) + parts[0].shape[1:], parts[0].dtype)
    return pl.pallas_call(
        stack_pair_kernel,
        name="stack_pair",
        out_shape=(shape, shape),
        in_specs=[vmem] * len(parts),
        out_specs=(vmem, vmem),
    )(*parts)


def xy_stage(parts):
    return [parts] + [px(parts, 2 * k) for k in range(1, 4)]


def split_kernel(meta, qkv_ref, out_ref, mine_ref, theirs_ref):
    core = meta[0] % 2
    for ref, half in ((mine_ref, core), (theirs_ref, 1 - core)):
        cols = pl.ds(pl.multiple_of(384 * half, 128), 384)
        ref[0:3] = qkv_ref[:, :, cols]
        ref[3] = out_ref[:, cols]


def join_kernel(meta, mine_ref, got_ref, out_ref):
    for core in range(2):

        @pl.when(meta[0] % 2 == core)
        def _():
            out_ref[...] = jnp.concatenate([mine_ref[...], got_ref[...]][:: 1 - 2 * core], 1)


def pair_rows(meta, qkv, out):
    vmem = pl.BlockSpec(memory_space=pltpu.VMEM)
    smem = pl.BlockSpec(memory_space=pltpu.SMEM)
    half = jax.ShapeDtypeStruct((4, 24, 384), B16)
    mine, theirs = pl.pallas_call(
        split_kernel, name="split", out_shape=(half, half), in_specs=[smem, vmem, vmem], out_specs=(vmem, vmem)
    )(meta, qkv, out)
    return pl.pallas_call(
        join_kernel,
        name="join",
        out_shape=jax.ShapeDtypeStruct((4, 48, 384), B16),
        in_specs=[smem, vmem, vmem],
        out_specs=vmem,
    )(meta, mine, px(theirs, 1))


def assemble_kernel(meta, *refs):
    pieces, out, sems = refs[:4], refs[4], refs[5]
    copies = []
    for xy in range(4):
        for z in range(4):
            rows = pl.multiple_of(48 * jnp.bitwise_xor(meta[0] // 2, xy + 4 * z), 16)
            copies.append(
                pltpu.make_async_copy(pieces[xy].at[z], out.at[:, pl.ds(rows, 48), :], sems.at[4 * xy + z])
            )
    for copy in copies:
        copy.start()
    for copy in copies:
        copy.wait()


def assemble(meta, pieces, name):
    return pl.pallas_call(
        assemble_kernel,
        name=name,
        out_shape=jax.ShapeDtypeStruct((4, 768, 384), B16),
        in_specs=[pl.BlockSpec(memory_space=pltpu.SMEM)] + [pl.BlockSpec(memory_space=pl.ANY)] * 4,
        out_specs=pl.BlockSpec(memory_space=pltpu.VMEM),
        scratch_shapes=[pltpu.SemaphoreType.DMA((16,))],
    )(meta, *pieces)


def project_kernel(side, meta, x_ref, w_ref, b_ref, *refs):
    half = jnp.bitwise_xor(meta[0] % 2, side)
    cols = pl.ds(pl.multiple_of(384 * half, 128), 384)
    y = dotf(x_ref[...], w_ref[0]) + b_ref[pl.program_id(0), :, cols]
    refs[-1][...] = y.astype(B16)


def project(meta, x, weight, bias, side, held):
    rows = x.shape[0]
    vmem = pl.BlockSpec(memory_space=pltpu.VMEM)
    return pl.pallas_call(
        partial(project_kernel, side),
        name="project",
        grid=(3,),
        out_shape=jax.ShapeDtypeStruct((rows, 2304), B16),
        in_specs=[
            pl.BlockSpec(memory_space=pltpu.SMEM),
            vmem,
            pl.BlockSpec((1, 768, 384), lambda c: (c, 0, 0)),
            vmem,
        ]
        + [pl.BlockSpec(memory_space=pl.ANY)] * len(held),
        out_specs=pl.BlockSpec((rows, 384), lambda c: (0, 3 * side + c)),
        input_output_aliases={4 + i: i for i in range(len(held))},
        compiler_params=pltpu.CompilerParams(vmem_limit_bytes=VMEM_LIMIT),
    )(meta, x, weight, bias, *held)


def embed_kernel(tokens_ref, slots_ref, segs_ref, table_ref, p_ref, start_ref, normed_ref, hot_ref, qf_ref, kf_ref):
    lane = lax.broadcasted_iota(jnp.int32, (TILE, 128), 1)
    slots, segs = slots_ref[...], segs_ref[...]
    is_prompt = slots < NPROMPT
    hot = jnp.where((lane == slots) & is_prompt, 1.0, 0.0).astype(B16)
    hot_ref[...] = hot
    rows = None
    for part in three_parts(table_ref[...]):
        term = dotf(hot, part.astype(B16))
        rows = term if rows is None else rows + term
    start = jnp.where(is_prompt, rows, tokens_ref[...].astype(F32))
    start_ref[...] = start
    normed_ref[...] = (centred(start)[0] * p_ref[0:1] + p_ref[1:2]).astype(B16)
    spot = lane % 64
    same = (spot == segs) & (spot < 7)
    qf_ref[...] = jnp.where(same, 1.0, 0.0).astype(B16)
    kf = jnp.where(spot < 7, jnp.where(same, 0.0, -BIG), jnp.where(spot < 10, 1.0, 0.0))
    kf_ref[...] = kf.astype(B16)


def embed(tokens, slots, segs, table, params):
    rows = tokens.shape[0]

    def block(width):
        return pl.BlockSpec((TILE, width), lambda i: (i, 0))

    vmem = pl.BlockSpec(memory_space=pltpu.VMEM)
    lanes = jax.ShapeDtypeStruct((rows, 128), B16)
    return pl.pallas_call(
        embed_kernel,
        name="embed",
        grid=(rows // TILE,),
        in_specs=[block(768), block(1), block(1), vmem, vmem],
        out_specs=[block(768), block(768), block(128), block(128), block(128)],
        out_shape=(
            jax.ShapeDtypeStruct((rows, 768), F32),
            jax.ShapeDtypeStruct((rows, 768), B16),
            lanes,
            lanes,
            lanes,
        ),
    )(tokens, slots[:, None], segs[:, None], table, params)


def gather_sums_kernel(own_ref, got_ref, own_out_ref, got_out_ref, keep_ref, *sends):
    for k in range(4):
        for z in range(4):
            for m in range(4):
                if m < 3:
                    x = add_parts(own_ref[k, z, m], got_ref[k, z, m])
                else:
                    x = add_parts(own_out_ref[k, z, 0], got_out_ref[k, z, 0])
                if k:
                    sends[k - 1][z, m] = x.astype(B16)
                else:
                    keep_ref[z, m] = x


def gather_sums(own, got, own_out, got_out):
    vmem = pl.BlockSpec(memory_space=pltpu.VMEM)
    send = jax.ShapeDtypeStruct((4, 4, 24, 768), B16)
    return pl.pallas_call(
        gather_sums_kernel,
        name="gather_sums",
        in_specs=[vmem] * 4,
        out_specs=[vmem] * 4,
        out_shape=(jax.ShapeDtypeStruct((4, 4, 24, 768), F32), send, send, send),
        compiler_params=pltpu.CompilerParams(vmem_limit_bytes=VMEM_LIMIT),
    )(own, got, own_out, got_out)


def four(values):
    return (values[0] + values[1]) + (values[2] + values[3])


def plane_sums_kernel(keep_ref, *refs):
    moved, (col_ref, *sends) = refs[:3], refs[3:]
    for z in range(4):
        for m in range(4):
            x = four([keep_ref[z, m]] + [ref[z, m].astype(F32) for ref in moved])
            if z:
                sends[z - 1][m] = x.astype(B16)
            else:
                col_ref[m] = x


def plane_sums(keep, moved):
    vmem = pl.BlockSpec(memory_space=pltpu.VMEM)
    send = jax.ShapeDtypeStruct((4, 24, 768), B16)
    return pl.pallas_call(
        plane_sums_kernel,
        name="plane_sums",
        in_specs=[vmem] * 4,
        out_specs=[vmem] * 4,
        out_shape=(jax.ShapeDtypeStruct((4, 24, 768), F32), send, send, send),
        compiler_params=pltpu.CompilerParams(vmem_limit_bytes=VMEM_LIMIT),
    )(keep, *moved)


def line_sums_kernel(col_ref, *refs):
    last, (qkv_ref, out_ref) = refs[:3], refs[3:]
    for m in range(4):
        x = four([col_ref[m]] + [ref[m].astype(F32) for ref in last])
        if m < 3:
            qkv_ref[m] = x
        else:
            out_ref[...] = x


def line_sums(col, last):
    vmem = pl.BlockSpec(memory_space=pltpu.VMEM)
    return pl.pallas_call(
        line_sums_kernel,
        name="line_sums",
        in_specs=[vmem] * 4,
        out_specs=[vmem] * 2,
        out_shape=(jax.ShapeDtypeStruct((3, 24, 768), F32), jax.ShapeDtypeStruct((24, 768), F32)),
    )(col, *last)


def centred(x):
    mean = jnp.mean(x, axis=-1, keepdims=True)
    x = x - mean
    rate = lax.rsqrt(jnp.mean(x * x, axis=-1, keepdims=True) + EPS)
    return x * rate, rate


def out_kernel(meta, x_ref, start_ref, own_ref, other_ref, p_ref, middle_ref, normed_ref, w_ref):
    core = meta[0] % 2

    @pl.when(pl.program_id(0) == 0)
    def _():
        for ref, half in ((own_ref, core), (other_ref, 1 - core)):
            w_ref[:, pl.ds(pl.multiple_of(384 * half, 128), 384)] = ref[0]

    middle = start_ref[...] + dotf(x_ref[...], w_ref[...]) + p_ref[0:1]
    middle_ref[...] = middle
    normed_ref[...] = (centred(middle)[0] * p_ref[1:2] + p_ref[2:3]).astype(B16)


def out_projection(meta, mixed, start, own, other, params):
    rows = mixed.shape[0]
    block = pl.BlockSpec((STEP, 768), lambda i: (i, 0))
    vmem = pl.BlockSpec(memory_space=pltpu.VMEM)
    return pl.pallas_call(
        out_kernel,
        name="out_projection",
        grid=(rows // STEP,),
        in_specs=[pl.BlockSpec(memory_space=pltpu.SMEM), block, block]
        + [pl.BlockSpec((1, 768, 384), lambda i: (3, 0, 0))] * 2
        + [vmem],
        out_specs=[block, block, vmem],
        out_shape=(
            jax.ShapeDtypeStruct((rows, 768), F32),
            jax.ShapeDtypeStruct((rows, 768), B16),
            jax.ShapeDtypeStruct((768, 768), B16),
        ),
        compiler_params=pltpu.CompilerParams(vmem_limit_bytes=VMEM_LIMIT),
    )(meta, mixed, start, own, other, params)


def norm_backward(normal, rate, grad, gain):
    u = grad * gain
    return rate * (u - jnp.mean(u, axis=-1, keepdims=True) - normal * jnp.mean(u * normal, axis=-1, keepdims=True))


def row_sum(x):
    return jnp.sum(x, axis=0, keepdims=True)


def put_parts(meta, acc, own_ref, other_ref, m):
    chip, core = meta[0] // 2, meta[0] % 2
    for z in range(4):
        for xy in range(4):
            row = 48 * jnp.bitwise_xor(chip, xy + 4 * z)
            own_ref[xy, z, m] = acc[pl.ds(pl.multiple_of(row + 24 * core, 8), 24), :].astype(B16)
            other_ref[xy, z, m] = acc[pl.ds(pl.multiple_of(row + 24 * (1 - core), 8), 24), :].astype(B16)


def turn_kernel(
    meta, middle_ref, branch_ref, grad_ref, cot_ref, mixed_ref, w_ref, p_ref,
    output_ref, gmiddle_ref, gmixed_ref, own_ref, other_ref, sums_ref, acc,
):
    i = pl.program_id(0)

    @pl.when(i == 0)
    def _():
        sums_ref[...] = jnp.zeros_like(sums_ref)
        acc[...] = jnp.zeros_like(acc)

    middle, grad = middle_ref[...], grad_ref[...]
    cot = cot_ref[...].astype(F32)
    output_ref[...] = (middle + branch_ref[...] + p_ref[1:2]).astype(B16)
    normal, rate = centred(middle)
    gmiddle = cot + norm_backward(normal, rate, grad, p_ref[0:1])
    gmiddle_ref[...] = gmiddle
    low = gmiddle.astype(B16)
    for row, x in enumerate((normal * grad, grad, low.astype(F32), cot)):
        sums_ref[row : row + 1, :] += row_sum(x)
    gmixed_ref[...] = dotf(low, w_ref[...], NT).astype(B16)
    acc[...] += dotf(mixed_ref[...], low, TN)

    @pl.when(i == pl.num_programs(0) - 1)
    def _():
        put_parts(meta, acc, own_ref, other_ref, 0)


def turn(meta, middle, branch, grad, cot, mixed, weight, params):
    rows = middle.shape[0]
    block = pl.BlockSpec((STEP, 768), lambda i: (i, 0))
    vmem = pl.BlockSpec(memory_space=pltpu.VMEM)
    parts = jax.ShapeDtypeStruct((4, 4, 1, 24, 768), B16)
    return pl.pallas_call(
        turn_kernel,
        name="turn",
        grid=(rows // STEP,),
        in_specs=[pl.BlockSpec(memory_space=pltpu.SMEM)] + [block] * 5 + [vmem, vmem],
        out_specs=[block, block, block, vmem, vmem, vmem],
        out_shape=(
            jax.ShapeDtypeStruct((rows, 768), B16),
            jax.ShapeDtypeStruct((rows, 768), F32),
            jax.ShapeDtypeStruct((rows, 768), B16),
            parts,
            parts,
            jax.ShapeDtypeStruct((8, 768), F32),
        ),
        scratch_shapes=[pltpu.VMEM((768, 768), F32)],
        compiler_params=pltpu.CompilerParams(vmem_limit_bytes=VMEM_LIMIT),
    )(meta, middle, branch, grad, cot, mixed, weight, params)


def tail_kernel(meta, start_ref, gmiddle_ref, slots_ref, p_ref, turn_ref, up_ref, *refs):
    weights, grads = refs[:2], refs[2:5]
    input_ref, packed_ref, prompt_ref, sums_ref = refs[5:]
    core = meta[0] % 2

    @pl.when(pl.program_id(0) == 0)
    def _():
        prompt_ref[...] = jnp.zeros_like(prompt_ref)
        sums_ref[...] = jnp.zeros_like(sums_ref)

    total = None
    for c in range(3):
        for side in range(2):
            half = jnp.bitwise_xor(core, side)
            left = grads[c][:, pl.ds(pl.multiple_of(384 * half, 128), 384)]
            term = dotf(left, weights[side][c], NT)
            total = term if total is None else total + term
    normal, rate = centred(start_ref[...])
    rows = ((0, normal * total), (2, total), (4, grads[0][...].astype(F32)), (5, grads[2][...].astype(F32)))
    for row, x in rows:
        sums_ref[row : row + 1, :] += row_sum(x)
    gstart = gmiddle_ref[...] + norm_backward(normal, rate, total, p_ref[0:1])
    slots = slots_ref[...]
    is_prompt = jnp.sum(slots.astype(F32), axis=-1, keepdims=True) > 0.5
    input_ref[...] = jnp.where(is_prompt, 0.0, gstart)
    for part in three_parts(gstart)[:2]:
        prompt_ref[...] += dotf(slots, part.astype(B16), TN)

    @pl.when(pl.program_id(0) == pl.num_programs(0) - 1)
    def _():
        for row, source in ((1, 0), (3, 1), (6, 2), (7, 3)):
            sums_ref[row : row + 1, :] = turn_ref[source : source + 1, :]
        for row in range(4):
            sums_ref[8 + row : 9 + row, :] = up_ref[row]
        packed_ref[0:64, :] = prompt_ref[0:64, :].astype(B16)
        high, low = split_rows(sums_ref[...])
        packed_ref[64:80, :] = high
        packed_ref[80:96, :] = low


def tail_step(meta, start, gmiddle, slots, params, sums_two, up, weights, grads):
    rows = start.shape[0]

    def block(width):
        return pl.BlockSpec((STEP, width), lambda i: (i, 0))

    vmem = pl.BlockSpec(memory_space=pltpu.VMEM)
    return pl.pallas_call(
        tail_kernel,
        name="tail_step",
        grid=(rows // STEP,),
        in_specs=[pl.BlockSpec(memory_space=pltpu.SMEM), block(768), block(768), block(128)]
        + [vmem] * 3
        + [pl.BlockSpec((3, 768, 384), lambda i: (0, 0, 0))] * 2
        + [block(768)] * 3,
        out_specs=[block(768), vmem],
        out_shape=(
            jax.ShapeDtypeStruct((rows, 768), F32),
            jax.ShapeDtypeStruct((96, 768), B16),
        ),
        scratch_shapes=[pltpu.VMEM((128, 768), F32), pltpu.VMEM((16, 768), F32)],
        compiler_params=pltpu.CompilerParams(vmem_limit_bytes=VMEM_LIMIT),
    )(meta, start, gmiddle, slots, params, sums_two, up, *weights, *grads)


def weight_grad_kernel(count, meta, left_ref, *refs):
    rights, own_ref, other_ref, acc = refs[:count], refs[count], refs[count + 1], refs[count + 2]
    for m in range(count):
        acc[...] = dotf(left_ref[...], rights[m][...], TN)
        put_parts(meta, acc, own_ref, other_ref, m)


def weight_grad(meta, left, rights, name):
    count, width = len(rights), rights[0].shape[1]
    shape = jax.ShapeDtypeStruct((4, 4, count, 24, width), B16)
    vmem = pl.BlockSpec(memory_space=pltpu.VMEM)
    return pl.pallas_call(
        partial(weight_grad_kernel, count),
        name=name,
        out_shape=(shape, shape),
        in_specs=[pl.BlockSpec(memory_space=pltpu.SMEM)] + [vmem] * (count + 1),
        out_specs=(vmem, vmem),
        scratch_shapes=[pltpu.VMEM((left.shape[1], width), F32)],
        compiler_params=pltpu.CompilerParams(vmem_limit_bytes=VMEM_LIMIT),
    )(meta, left, *rights)


def split_rows(rest):
    high = rest.astype(B16)
    return high, (rest - high.astype(F32)).astype(B16)


def add_small(x, y):
    x, y = x.astype(F32), y.astype(F32)
    return jnp.concatenate([x[:64] + y[:64], (x[64:80] + x[80:]) + (y[64:80] + y[80:])])


def pack_small(x):
    return jnp.concatenate([x[:64].astype(B16), *split_rows(x[64:])])


def exchange_small(x, k):
    return add_small(x, px(x, k))


def add_parts(own, got):
    return own.astype(F32) + got.astype(F32)


def three_parts(x):
    high = x.astype(B16).astype(F32)
    mid = (x - high).astype(B16).astype(F32)
    return high, mid, (x - high) - mid


def attention_forward_kernel(qf_ref, kf_ref, q_ref, k_ref, v_ref, mixed_ref, lse_ref):
    half = lax.broadcasted_iota(jnp.int32, (1, 128), 1) < 64
    q = q_ref[...] * jnp.asarray(0.125, B16)
    k, v = k_ref[...], v_ref[...]
    qf, kf = qf_ref[...], kf_ref[...]
    one = jnp.ones((), B16)
    sides = []
    for e in range(2):
        own = half if e == 0 else ~half
        sides.append((jnp.where(own, q, qf), jnp.where(own, k, kf), jnp.where(own, v, one)))
    for first in range(0, ROW, QROWS):
        low, high = key_window(first, QROWS)
        outs, peaks = [], []
        for qe, ke, ve in sides:
            s = dotf(qe[first : first + QROWS], ke[low:high], NT)
            peak = jnp.max(s, axis=-1, keepdims=True)
            p = jnp.exp(s - peak).astype(B16)
            outs.append(dotf(p, ve[low:high]))
            peaks.append(peak)
        data = jnp.where(half, outs[0], outs[1])
        total = pltpu.roll(jnp.where(half, outs[1], outs[0]), 64, 1)
        mixed_ref[first : first + QROWS, :] = (data / total).astype(B16)
        lse_ref[first : first + QROWS, :] = jnp.where(half, peaks[0], peaks[1]) + jnp.log(total)


def pair_specs(rows):
    full = pl.BlockSpec((ROW, 128), lambda r, s, p, meta: (r, 0))
    blocks = [pl.BlockSpec((ROW, 128), lambda r, s, p, meta, c=c: (r, 9 * s + 3 * c + p)) for c in range(3)]
    whole = pl.BlockSpec((ROW, 128), lambda r, s, p, meta: (r, 3 * jnp.bitwise_xor(meta[0] % 2, s) + p))
    return (rows // ROW, 2, 3), full, blocks, whole


def attention_forward(meta, qf, kf, qkv):
    rows = qkv.shape[0]
    grid, full, blocks, whole = pair_specs(rows)

    def kernel(meta, *refs):
        attention_forward_kernel(*refs)

    return pl.pallas_call(
        kernel,
        name="attention_forward",
        grid_spec=pltpu.PrefetchScalarGridSpec(
            num_scalar_prefetch=1, grid=grid, in_specs=[full, full] + blocks, out_specs=[whole, whole]
        ),
        out_shape=(
            jax.ShapeDtypeStruct((rows, 768), B16),
            jax.ShapeDtypeStruct((rows, 768), F32),
        ),
        compiler_params=pltpu.CompilerParams(vmem_limit_bytes=VMEM_LIMIT),
    )(meta, qf, kf, qkv, qkv, qkv)


def attention_backward_kernel(
    qf_ref, kf_ref, q_ref, k_ref, v_ref, g_ref, mixed_ref, lse_ref, dq_ref, dk_ref, dv_ref, dk_acc, dv_acc
):
    lane = lax.broadcasted_iota(jnp.int32, (1, 128), 1)
    half = lane < 64
    spot = lane % 64
    q = q_ref[...] * jnp.asarray(0.125, B16)
    k, v, g = k_ref[...], v_ref[...], g_ref[...]
    qf, kf = qf_ref[...].astype(F32), kf_ref[...]
    prod = g.astype(F32) * mixed_ref[...].astype(F32)
    d0 = jnp.sum(jnp.where(half, prod, 0.0), axis=-1, keepdims=True)
    d1 = jnp.sum(jnp.where(half, 0.0, prod), axis=-1, keepdims=True)
    delta = jnp.where(half, d1, d0)
    lse = pltpu.roll(lse_ref[...], 64, 1)

    def spread(base, x):
        a, b, c = three_parts(-x)
        return jnp.where(spot == 7, a, jnp.where(spot == 8, b, jnp.where(spot == 9, c, base))).astype(B16)

    q_extra = spread(qf, lse)
    g_extra = spread(jnp.zeros_like(qf), delta)
    v_extra = jnp.where((spot >= 7) & (spot <= 9), 1.0, 0.0).astype(B16)
    dk_acc[...] = jnp.zeros_like(dk_acc)
    dv_acc[...] = jnp.zeros_like(dv_acc)
    sides = []
    for e in range(2):
        own = half if e == 0 else ~half
        sides.append(
            (
                jnp.where(own, q, q_extra),
                jnp.where(own, k, kf),
                jnp.where(own, g, g_extra),
                jnp.where(own, v, v_extra),
            )
        )
    for first in range(0, ROW, TILE):
        low, high = key_window(first, TILE)
        dqs, dks, dvs = [], [], []
        for qe, ke, ge, ve in sides:
            s = dotf(qe[first : first + TILE], ke[low:high], NT)
            p = jnp.exp(s)
            d = dotf(ge[first : first + TILE], ve[low:high], NT)
            ds = (p * d).astype(B16)
            dqs.append(dotf(ds, k[low:high]))
            dks.append(dotf(ds, q[first : first + TILE], TN))
            dvs.append(dotf(p.astype(B16), g[first : first + TILE], TN))
        dq_ref[first : first + TILE, :] = (jnp.where(half, dqs[0], dqs[1]) * 0.125).astype(B16)
        dk_acc[low:high, :] += jnp.where(half, dks[0], dks[1])
        dv_acc[low:high, :] += jnp.where(half, dvs[0], dvs[1])
    dk_ref[...] = dk_acc[...].astype(B16)
    dv_ref[...] = dv_acc[...].astype(B16)


def attention_backward(meta, qf, kf, qkv, grad, mixed, lse):
    rows = qkv.shape[0]
    grid, full, blocks, whole = pair_specs(rows)
    shape = jax.ShapeDtypeStruct((rows, 768), B16)

    def kernel(meta, *refs):
        attention_backward_kernel(*refs)

    return pl.pallas_call(
        kernel,
        name="attention_backward",
        grid_spec=pltpu.PrefetchScalarGridSpec(
            num_scalar_prefetch=1,
            grid=grid,
            in_specs=[full, full] + blocks + [whole] * 3,
            out_specs=[whole] * 3,
            scratch_shapes=[pltpu.VMEM((ROW, 128), F32), pltpu.VMEM((ROW, 128), F32)],
        ),
        out_shape=(shape, shape, shape),
        compiler_params=pltpu.CompilerParams(vmem_limit_bytes=VMEM_LIMIT),
    )(meta, qf, kf, qkv, qkv, qkv, grad, mixed, lse)


SUB = 256
PER = 768 // SUB


def mlp_kernel(fast, *refs):
    meta, n_ref, c_ref, ct, b_ref = refs[:5]
    count = 16 if fast else 1
    pieces, refs = refs[5 : 5 + count], refs[5 + count :]
    branch_ref, gn_ref, db_ref, own_ref, other_ref = refs[:5]
    w, nt, dw, wsem, dsem = refs[5:]
    t = pl.program_id(0)
    jr, sub = t // PER, t % PER
    me_mp, me_dp = meta[0] % 4, meta[0] // 4

    def loads(j):
        if not fast:
            source = pieces[0].at[:, :, pl.ds(768 * j, 768)]
            return [pltpu.make_async_copy(source, w.at[j], wsem.at[j, 0, 0])]
        out = []
        for dr in range(8):
            rows = pl.multiple_of(96 * jnp.bitwise_xor(me_dp, dr), 32)
            for c in range(2):
                source = pieces[8 * (j & 1) + 4 * c + (j >> 1) + 2 * (dr & 1)].at[dr >> 1]
                out.append(pltpu.make_async_copy(source, w.at[j, c, pl.ds(rows, 96), :], wsem.at[j, dr, c]))
        return out

    def stores(j):
        if not fast:
            return [pltpu.make_async_copy(dw.at[j], own_ref.at[j], dsem.at[j, 0, 0])]
        out = []
        for dr in range(8):
            x, y = j >> 1, dr & 1
            for c, spot in enumerate((2 * x + y, 2 * y + x)):
                target = (other_ref if j & 1 else own_ref).at[c, spot, dr >> 1]
                out.append(pltpu.make_async_copy(dw.at[j, dr, c], target, dsem.at[j, dr, c]))
        return out

    @pl.when(t == 0)
    def _():
        for j in range(4):
            for copy in loads(j):
                copy.start()
        nt[...] = n_ref[...].T
        branch_ref[...] = jnp.zeros_like(branch_ref)
        gn_ref[...] = jnp.zeros_like(gn_ref)

    for j in range(4):

        @pl.when(t == PER * j)
        def _():
            for copy in loads(j):
                copy.wait()

    spot = jnp.bitwise_xor(me_mp, jr) if fast else jr
    cols = pl.ds(pl.multiple_of(sub * SUB, SUB), SUB)
    w1 = w[jr, 0, :, cols]
    w2 = w[jr, 1, :, cols]
    u = dotf(n_ref[...], w1) + b_ref[spot, :, cols]
    cdf = 0.5 * (1.0 + lax.erf(u * 0.7071067811865476))
    hidden = (u * cdf).astype(B16)
    slope = cdf + u * (0.3989422804014327 * jnp.exp(-0.5 * u * u))
    gb = (dotf(c_ref[...], w2) * slope).astype(B16)
    db_ref[spot, :, cols] = jnp.sum(gb.astype(F32), axis=0, keepdims=True)
    branch_ref[...] += dotf(hidden, w2, NT)
    gn_ref[...] += dotf(gb, w1, NT)
    dw1 = dotf(nt[...], gb).astype(B16)
    dw2 = dotf(ct[...], hidden).astype(B16)
    for a in range(8):
        dr = jnp.bitwise_xor(me_dp, a) if fast else a
        dw[jr, dr, 0, :, cols] = dw1[96 * a : 96 * a + 96]
        dw[jr, dr, 1, :, cols] = dw2[96 * a : 96 * a + 96]

    for j in range(4):

        @pl.when(t == PER * j + PER - 1)
        def _():
            for copy in stores(j):
                copy.start()

    @pl.when(t == 4 * PER - 1)
    def _():
        for j in range(4):
            for copy in stores(j):
                copy.wait()


def mlp(meta, normed, cot, cot_turned, bias, pieces):
    fast = len(pieces) == 16
    tokens = normed.shape[0]
    vmem = pl.BlockSpec(memory_space=pltpu.VMEM)
    anys = pl.BlockSpec(memory_space=pl.ANY)
    shape = jax.ShapeDtypeStruct((2, 4, 4, 96, 768) if fast else (4, 8, 2, 96, 768), B16)
    return pl.pallas_call(
        partial(mlp_kernel, fast),
        name="mlp",
        grid=(4 * PER,),
        in_specs=[pl.BlockSpec(memory_space=pltpu.SMEM)] + [vmem] * 4 + [anys] * len(pieces),
        out_specs=[vmem, vmem, vmem, anys, anys],
        out_shape=(
            jax.ShapeDtypeStruct((tokens, 768), F32),
            jax.ShapeDtypeStruct((tokens, 768), F32),
            jax.ShapeDtypeStruct((4, 1, 768), F32),
            shape,
            shape,
        ),
        scratch_shapes=[
            pltpu.VMEM((4, 2, 768, 768), B16),
            pltpu.VMEM((768, tokens), B16),
            pltpu.VMEM((4, 8, 2, 96, 768), B16),
            pltpu.SemaphoreType.DMA((4, 8, 2)),
            pltpu.SemaphoreType.DMA((4, 8, 2)),
        ],
        compiler_params=pltpu.CompilerParams(vmem_limit_bytes=VMEM_LIMIT),
    )(meta, normed, cot, cot_turned, bias.reshape(4, 1, 768), *pieces)


def local(
    fast,
    tokens,
    cotangent,
    prompts,
    segments,
    prompt_slot_index,
    norm_gain,
    norm_shift,
    attn_qkv,
    attn_bias,
    attn_out,
    mlp_weight,
    mlp_bias_up,
    mlp_bias_down,
):
    width = tokens.shape[1]
    device = lax.axis_index("dp") * lax.axis_size("mp") + lax.axis_index("mp")
    meta = jnp.reshape(device, (1,)).astype(jnp.int32)
    core = device % 2
    if fast:
        piece = pair_rows(meta, attn_qkv, attn_out)
        held = z_stage(piece)
        held, mlp_near, mlp_piece, tokens, prompts, segments, prompt_slot_index = tie(
            held, px(mlp_weight, 8), mlp_weight, tokens, prompts, segments, prompt_slot_index
        )
    table = jnp.concatenate([prompts, jnp.zeros((128 - NPROMPT, width), F32)], 0)
    start, normed_one, onehot, qf, kf = embed(
        tokens, prompt_slot_index, segments, table, jnp.stack([norm_gain[0], norm_shift[0]])
    )
    bias = jnp.stack([attn_bias[0], jnp.zeros_like(attn_bias[0]), attn_bias[1]])[:, None]
    out_params = jnp.stack([attn_bias[2], norm_gain[1], norm_shift[1]])
    turn_params = jnp.stack([norm_gain[1], mlp_bias_down])
    cot_turned = cotangent.T

    if fast:
        x = (normed_one, start, qf, kf, onehot, bias, out_params, turn_params, cot_turned)
        mlp_z = [mlp_piece, mlp_near] + [px(mlp_piece, 8 * k) for k in range(2, 4)]
        quad, mlp_z, x = tie(xy_stage(held), mlp_z, x)
        normed_one, start, qf, kf, onehot, bias, out_params, turn_params, cot_turned = x
        own = assemble(meta, quad, "assemble")
        s1, s2 = stack_pair(mlp_z)
        own, s1, s2 = tie(own, s1, s2)
        other, y1, x2 = px(own, 1), px(s1, 4), px(s2, 2)
        s_other = [px(s1, 1), px(s2, 1)]
        qkv = project(meta, normed_one, own, bias, 0, ())
        other, qkv = tie(other, qkv)
    else:
        qkv_all = lax.all_gather(attn_qkv, AXES, axis=1, tiled=True)
        out_all = lax.all_gather(attn_out, AXES, axis=0, tiled=True)
        mlp_all = lax.all_gather(mlp_weight, "dp", axis=1, tiled=True)
        mlp_all = lax.all_gather(mlp_all, "mp", axis=2, tiled=True)
        four_all = jnp.concatenate([qkv_all, out_all[None]])
        own = lax.dynamic_slice_in_dim(four_all, 384 * core, 384, 2)
        other = lax.dynamic_slice_in_dim(four_all, 384 * (1 - core), 384, 2)
        qkv = project(meta, normed_one, own, bias, 0, ())
    qkv = project(meta, normed_one, other, bias, 1, (qkv,))
    if fast:
        y1, x2, s_other, qkv = tie(y1, x2, s_other, qkv)
        x1, xy1, y2, xy2 = px(s1, 2), px(y1, 2), px(s2, 4), px(x2, 4)
    mixed, lse = attention_forward(meta, qf, kf, qkv)
    if fast:
        x1, xy1, y2, xy2, mixed = tie(x1, xy1, y2, xy2, mixed)
        one = [px(v, 1) for v in (x1, y1, xy1)]
        two = [px(v, 1) for v in (x2, y2, xy2)]
        mlp_pieces = [s1, x1, y1, xy1, s2, x2, y2, xy2, s_other[0], *one, s_other[1], *two]
    else:
        mlp_pieces = [mlp_all]
    middle, normed_two, out_weight = out_projection(meta, mixed, start, own, other, out_params)
    branch, grad_two, grad_up, own_mlp, other_mlp = mlp(
        meta, normed_two, cotangent, cot_turned, mlp_bias_up, mlp_pieces
    )
    if fast:
        other_mlp, grad_two, branch = tie(other_mlp, grad_two, branch)
        got_mlp = px(other_mlp, 1)
    output, grad_middle, grad_mixed, own_out, other_out, sums_two = turn(
        meta, middle, branch, grad_two, cotangent, mixed, out_weight, turn_params
    )
    if fast:
        got_mlp, grad_mixed, other_out = tie(got_mlp, grad_mixed, other_out)
        send = [add_parts(own_mlp[c, 2:], got_mlp[c, 2:]).astype(B16) for c in range(2)]
        send, grad_mixed, other_out = tie(send, grad_mixed, other_out)
        got_1, got_2, got_out = px(send[0], 2), px(send[1], 4), px(other_out, 1)
    grads = attention_backward(meta, qf, kf, qkv, grad_mixed, mixed, lse)
    if fast:
        got_1, got_2, got_out, grads, grad_middle = tie(got_1, got_2, got_out, grads, grad_middle)
        planes = (got_1, got_2)

        def plane(c, i):
            return add_parts(own_mlp[c, i], got_mlp[c, i]) + planes[c][i].astype(F32)

        send, grads = tie([plane(c, 1).astype(B16) for c in range(2)], grads)
        got_1, got_2 = px(send[0], 4), px(send[1], 2)
    input_grad, packed = tail_step(
        meta, start, grad_middle, onehot, norm_gain[0:1], sums_two, grad_up, (own, other), grads
    )
    if fast:
        packed, grads, got_1, got_2 = tie(packed, grads, got_1, got_2)
        got_small = px(packed, 1)
        own_w, other_w = weight_grad(meta, normed_one, grads, "weight_grad_qkv")
        got_small, other_w = tie(got_small, other_w)
        got_w = px(other_w, 1)
        packed = pack_small(add_small(packed, got_small))
        packed, got_1, got_2 = tie(packed, got_1, got_2)
        got_small = px(packed, 2)
        got_w, got_small, packed = tie(got_w, got_small, packed)
        packed = pack_small(add_small(packed, got_small))
        got_small = px(packed, 4)
        col = [add_parts(plane(0, 0), got_1), add_parts(plane(1, 0), got_2)]
        send = jnp.stack([c[2:].astype(B16) for c in col])
        keep, *sends = gather_sums(own_w, got_w, own_out, got_out)
        send, sends, got_small, packed = tie(send, sends, got_small, packed)
        got_far = px(send, 16)
        moved = [px(x, 2 * i + 2) for i, x in enumerate(sends)]
        packed = pack_small(add_small(packed, got_small))
        got_small = px(packed, 8)
        moved, got_far, got_small, packed = tie(moved, got_far, got_small, packed)
        near = [add_parts(col[c][:2], got_far[c]) for c in range(2)]
        moved, send = tie(moved, jnp.stack([x[1].astype(B16) for x in near]))
        col_attn, *last = plane_sums(keep, moved)
        last = [px(x, 8 * i + 8) for i, x in enumerate(last)]
        got_near = px(send, 8)
        small = exchange_small(pack_small(add_small(packed, got_small)), 16)
        mlp_grad = jnp.stack([x[0] for x in near]) + got_near.astype(F32)
        qkv_grad, out_grad = line_sums(col_attn, last)
    else:
        mlp_grad = own_mlp.transpose(2, 1, 3, 0, 4)
        mlp_grad = mlp_grad.reshape(2, 768, 3072)
        mlp_grad = lax.psum_scatter(mlp_grad, "dp", scatter_dimension=1, tiled=True)
        mlp_grad = lax.psum_scatter(mlp_grad, "mp", scatter_dimension=2, tiled=True).astype(F32)
        grad_out_weight = dotf(mixed, grad_middle.astype(B16), TN)
        grad_qkv = jnp.stack([dotf(normed_one, g, TN) for g in grads])
        qkv_grad = lax.psum_scatter(grad_qkv, AXES, scatter_dimension=1, tiled=True)
        out_grad = lax.psum_scatter(grad_out_weight, AXES, scatter_dimension=0, tiled=True)
        x = packed.astype(F32)
        small = lax.psum(jnp.concatenate([x[:64], x[64:80] + x[80:]]), AXES)
    return (
        output,
        input_grad,
        small[:NPROMPT],
        small[64:66],
        small[66:68],
        qkv_grad,
        small[68:71],
        out_grad,
        mlp_grad,
        small[72:76].reshape(-1),
        small[71],
    )


def solution(mesh):
    fast = dict(mesh.shape) == {"dp": 8, "mp": 4}
    return jax.shard_map(
        partial(local, fast),
        mesh=mesh,
        in_specs=(
            P(AXES, None),
            P(AXES, None),
            P(),
            P(AXES),
            P(AXES),
            P(),
            P(),
            P(None, AXES, None),
            P(),
            P(AXES, None),
            P(None, "dp", "mp"),
            P(),
            P(),
        ),
        out_specs=(
            P(AXES, None),
            P(AXES, None),
            P(),
            P(),
            P(),
            P(None, AXES, None),
            P(),
            P(AXES, None),
            P(None, "dp", "mp"),
            P(),
            P(),
        ),
        check_vma=False,
    )
```
